512 devices in a mesh: gx: 4 (over y_hi), gy: 16 (over z, y_lo), gz: 8 (over x, core).
Axes of the slice: x: 4, y: 8 (y_hi: 4, y_lo: 2; y = y_hi * 2 + y_lo), z: 8, core: 2. Of those that a mesh axis runs over, the one named last changes fastest.
Arguments:
- nodal_scalar_values: float32 [3, 32, 128, 16384], P(None, 'gx', 'gy', 'gz'), may hold values from -6 to 6
- geometry: float32 [6, 4, 16, 2048], P(None, 'gx', 'gy', 'gz'), may hold values from -1.2 to 4, as said below
Outputs:
- assembled: float32 [3, 32, 128, 16384], P(None, 'gx', 'gy', 'gz')
The draws below stay inside these ranges and needn't reach their ends.
Inputs may be any that keep to these rules, and one draw needn't show every extreme that they name: `geometry`: G00, G11 and G22 are positive; each off-diagonal factor is at most 0.3 times the root of the product of its two diagonal factors in magnitude.
All inputs are finite; a program needn't handle non-finite values.
Results may differ from the reference program's by a relative error of at most 0.00007.
Values sent between devices are 32-bit elements; how exact they have to be, the bound alone decides.
No kernel may reach another device: no remote copies, remote signals or barrier semaphores. Data moves between devices by JAX's collectives and lax.ppermute only.
A program may use at most 64 MiB of HBM per device.

```python
import math
import jax
import jax.numpy as jnp
import numpy as np
from jax import lax

COMPONENTS = 3
ELEMENTS_FIRST = 4
ELEMENTS_SECOND = 16
ELEMENTS_THIRD = 2048


def draw_geometry(key, part):
    element_grid_shape = (ELEMENTS_FIRST, ELEMENTS_SECOND, ELEMENTS_THIRD)
    key_list = jax.random.split(key, 2)
    diagonal = jnp.exp(jax.random.uniform(key_list[0], (3,) + element_grid_shape, jnp.float32, math.log(0.5), math.log(2.0)))
    coupling = jax.random.uniform(key_list[1], (3,) + element_grid_shape, jnp.float32, -0.3, 0.3)
    cross_xy = coupling[0] * jnp.sqrt(diagonal[0] * diagonal[1])
    cross_xz = coupling[1] * jnp.sqrt(diagonal[0] * diagonal[2])
    cross_yz = coupling[2] * jnp.sqrt(diagonal[1] * diagonal[2])
    return jnp.stack([diagonal[0], diagonal[1], diagonal[2], cross_xy, cross_xz, cross_yz]).astype(jnp.float32)


def level_of(own_key, extent, cuts, low, high):
    factor_of, own = 1.0, jax.random.fold_in(own_key, 6)
    for axis_at, blocks in cuts:
        steps = jnp.exp(jax.random.uniform(jax.random.fold_in(own, axis_at), (blocks,), jnp.float32, low / len(cuts), high / len(cuts)))
        factor_of = factor_of * jnp.repeat(steps, extent[axis_at] // blocks).reshape([-1 if axis == axis_at else 1 for axis in range(len(extent))])
    return factor_of


def gaussian(key, shape, scale, most, pieces=(), held_as=jnp.bfloat16):
    level = level_of(key, shape, pieces, -0.22, 0.18) if pieces else 1.0
    entries = jax.random.normal(key, shape, jnp.float32) * scale * level
    return jnp.minimum(jnp.maximum(entries, -most), most).astype(held_as)


def setup_inputs(seed: int = 0) -> dict:
    key_of = jax.random.split(jax.random.key(seed), 3)
    return {
        "nodal_scalar_values": gaussian(key_of[0], (COMPONENTS, 8 * ELEMENTS_FIRST, 8 * ELEMENTS_SECOND, 8 * ELEMENTS_THIRD), 1.0, 6.0, ((1, 4), (2, 16), (3, 8)), jnp.float32),
        "geometry": draw_geometry(jax.random.fold_in(key_of[2], 71), 0),
    }


interior_points = [-0.8717401485096066, -0.5917001814331423, -0.2092992179024789, 0.2092992179024789, 0.5917001814331423, 0.8717401485096066]


def legendre_seven(point):
    previous = 1.0
    current = point
    for order in range(1, 7):
        following = ((2 * order + 1) * point * current - order * previous) / (order + 1)
        previous = current
        current = following
    return current


def gll_tables():
    degree = 7
    points = [-1.0] + interior_points + [1.0]
    values = [legendre_seven(point) for point in points]
    node_count = degree + 1
    weights = np.array([2.0 / (degree * (degree + 1) * value * value) for value in values])
    derivative = np.zeros((node_count, node_count))
    for row_index in range(node_count):
        for col_index in range(node_count):
            if row_index != col_index:
                derivative[row_index, col_index] = values[row_index] / (values[col_index] * (points[row_index] - points[col_index]))
    derivative[0, 0] = -degree * (degree + 1) / 4.0
    derivative[node_count - 1, node_count - 1] = degree * (degree + 1) / 4.0
    return derivative, weights


def apply_axis(field_in, matrix, direction):
    length = field_in.shape[direction]
    block_size = math.gcd(length, 128)
    big_table = jnp.kron(jnp.eye(block_size // 8, dtype=jnp.float32), matrix)
    dim_list = list(field_in.shape)
    folded_shape = dim_list[:direction] + [length // block_size, block_size] + dim_list[direction + 1:]
    folded_field = field_in.reshape(folded_shape)
    patterns = ["nbyz,ab->nayz", "xnbz,ab->xnaz", "xynb,ab->xyna"]
    result = jnp.einsum(patterns[direction], folded_field, big_table, precision=lax.Precision.HIGHEST)
    return result.reshape(field_in.shape)


def expand(field_component, target):
    elem_x, elem_y, elem_z = field_component.shape
    spread = jnp.broadcast_to(field_component[:, None, :, None, :, None], (elem_x, 8, elem_y, 8, elem_z, 8))
    return spread.reshape(target)


def stiffness(field_in, geometry):
    derivative, weights = gll_tables()
    matrix = jnp.asarray(derivative, jnp.float32)
    weight_row = jnp.asarray(weights, jnp.float32)
    size_x, size_y, size_z = field_in.shape
    weight_x = jnp.tile(weight_row, size_x // 8)
    weight_y = jnp.tile(weight_row, size_y // 8)
    weight_z = jnp.tile(weight_row, size_z // 8)
    node_weight = weight_x[:, None, None] * weight_y[None, :, None] * weight_z[None, None, :]
    grad_x = apply_axis(field_in, matrix, 0)
    grad_y = apply_axis(field_in, matrix, 1)
    grad_z = apply_axis(field_in, matrix, 2)
    factors = [expand(geometry[index], field_in.shape) for index in range(6)]
    flux_x = node_weight * (factors[0] * grad_x + factors[3] * grad_y + factors[4] * grad_z)
    flux_y = node_weight * (factors[3] * grad_x + factors[1] * grad_y + factors[5] * grad_z)
    flux_z = node_weight * (factors[4] * grad_x + factors[5] * grad_y + factors[2] * grad_z)
    transposed = matrix.T
    return apply_axis(flux_x, transposed, 0) + apply_axis(flux_y, transposed, 1) + apply_axis(flux_z, transposed, 2)


def combine(middle, below_plane, above_plane, direction):
    length = middle.shape[direction]
    from_above = jnp.concatenate([lax.slice_in_dim(middle, 1, length, axis=direction), above_plane], axis=direction)
    from_below = jnp.concatenate([below_plane, lax.slice_in_dim(middle, 0, length - 1, axis=direction)], axis=direction)
    position = lax.broadcasted_iota(jnp.int32, middle.shape, direction) % 8
    return middle + jnp.where(position == 7, from_above, 0.0) + jnp.where(position == 0, from_below, 0.0)


def single_component(field_values, geometry):
    total_x, total_y, total_z = field_values.shape
    zblock = math.gcd(total_z, 1024)
    block_count = total_z // zblock
    field_blocks = jnp.moveaxis(field_values.reshape(total_x, total_y, block_count, zblock), 2, 0)
    geometries = jnp.moveaxis(geometry.reshape(6, geometry.shape[1], geometry.shape[2], block_count, zblock // 8), 3, 0)
    local_terms = lax.map(lambda operands: stiffness(operands[0], operands[1]), (field_blocks, geometries))
    local_terms = jnp.moveaxis(local_terms, 0, 2).reshape(field_values.shape)
    summed = local_terms
    for direction in range(3):
        plane_extents = list(summed.shape)
        plane_extents[direction] = 1
        zero_plane = jnp.zeros(plane_extents, jnp.float32)
        summed = combine(summed, zero_plane, zero_plane, direction)
    return summed


def reference(nodal_scalar_values, geometry):
    return jnp.stack([single_component(nodal_scalar_values[component], geometry) for component in range(COMPONENTS)])
```

```python
import functools

import jax
import jax.numpy as jnp
import numpy as np
from jax import lax
from jax.experimental import pallas as pl
from jax.experimental.pallas import tpu as pltpu
from jax.sharding import PartitionSpec as P

interior_points = [
    -0.8717401485096066,
    -0.5917001814331423,
    -0.2092992179024789,
    0.2092992179024789,
    0.5917001814331423,
    0.8717401485096066,
]
LANES = 128
BLOCK = 256
F32 = jnp.float32
BF16 = jnp.bfloat16


def legendre_seven(point):
    previous = 1.0
    current = point
    for order in range(1, 7):
        following = ((2 * order + 1) * point * current - order * previous) / (order + 1)
        previous = current
        current = following
    return current


def gll_tables():
    degree = 7
    points = [-1.0] + interior_points + [1.0]
    values = [legendre_seven(point) for point in points]
    node_count = degree + 1
    weights = np.array([2.0 / (degree * (degree + 1) * value * value) for value in values])
    derivative = np.zeros((node_count, node_count))
    for row_index in range(node_count):
        for col_index in range(node_count):
            if row_index != col_index:
                derivative[row_index, col_index] = values[row_index] / (
                    values[col_index] * (points[row_index] - points[col_index])
                )
    derivative[0, 0] = -degree * (degree + 1) / 4.0
    derivative[node_count - 1, node_count - 1] = degree * (degree + 1) / 4.0
    return (derivative.astype(np.float32).astype(np.float64), weights)


def split_table(table):
    high = np.asarray(table, np.float32).astype(jnp.bfloat16)
    low = (np.asarray(table, np.float64) - high.astype(np.float64)).astype(jnp.bfloat16)
    return high, low


def tables():
    derivative, weights = gll_tables()
    eye = np.eye(8)
    grads = np.concatenate([np.kron(derivative, eye), np.kron(eye, derivative)], 0)
    high, low = split_table(grads)
    grad_xy = np.concatenate([high, high, low], 1)
    plane = np.kron(weights, weights)
    back_x = np.kron((derivative * weights[:, None]).T, np.diag(weights))
    back_y = np.kron(np.diag(weights), (derivative * weights[:, None]).T)
    high, low = split_table(np.concatenate([back_x, back_y], 1))
    back_xy = np.concatenate([high, high, low], 1)
    many = np.eye(BLOCK // 8)
    grad_z = np.concatenate(split_table(np.kron(many, derivative.T)), 0)
    back_z = np.concatenate(split_table(np.kron(many, derivative)), 0)
    spread = np.kron(np.eye(LANES)[:, : BLOCK // 8], np.ones((1, 8))).astype(jnp.bfloat16)
    weight_z = np.tile(weights, BLOCK // 8)[None].astype(np.float32)
    plane = np.tile(plane[:, None], (1, BLOCK)).astype(np.float32)
    return grad_xy, back_xy, grad_z, back_z, spread, weight_z, plane


def split(values):
    high = values.astype(BF16)
    return high, (values - high.astype(F32)).astype(BF16)


def dot(left, right):
    return jnp.dot(left, right, preferred_element_type=F32)


def lane_iota():
    return lax.broadcasted_iota(jnp.int32, (8, LANES), 1)


def stiffness_kernel(
    u_ref, geo_ref, gxy_ref, bxy_ref, gz_ref, bz_ref, spread_ref, wz_ref, plane_ref,
    out_ref, xa_ref, xb_ref, yf_ref, za_ref, zb_ref, geo_scr,
):
    components = u_ref.shape[0]
    length = u_ref.shape[3]
    blocks = length // BLOCK
    tiles = length // LANES
    per_block = BLOCK // 8
    geo = jnp.concatenate([geo_ref[...], jnp.zeros((2, geo_ref.shape[1]), F32)], 0)
    rows = []
    for block in range(blocks):
        start = block * per_block
        tile = geo[:, start // LANES * LANES : start // LANES * LANES + LANES]
        shift = start % LANES
        rows.append(pltpu.roll(tile, LANES - shift, 1) if shift else tile)
    stacked = jnp.concatenate(rows, 0)
    first, rest = split(stacked)
    rest = stacked - first.astype(F32)
    second = rest.astype(BF16)
    third = (rest - second.astype(F32)).astype(BF16)
    spread = spread_ref[...]
    expanded = dot(first, spread) + dot(second, spread) + dot(third, spread)
    geo_scr[...] = expanded * wz_ref[...]

    def body(block, carry):
        start = pl.multiple_of(block * BLOCK, BLOCK)
        where = pl.ds(start, BLOCK)
        field = jnp.concatenate(
            [u_ref[c, :, :, where].reshape(64, BLOCK) for c in range(components)], 0
        )
        high, low = split(field)
        grad_z = (
            dot(high, gz_ref[:BLOCK]) + dot(low, gz_ref[:BLOCK]) + dot(high, gz_ref[BLOCK:])
        )
        factor = geo_scr[pl.ds(pl.multiple_of(block * 8, 8), 8), :]
        g = [factor[k : k + 1] for k in range(6)]
        fluxes = []
        sums = []
        for c in range(components):
            mine = slice(64 * c, 64 * c + 64)
            stack = jnp.concatenate([high[mine], low[mine], high[mine]], 0)
            both = dot(gxy_ref[...], stack)
            gx, gy, gz = both[:64], both[64:], grad_z[mine]
            fx = g[0] * gx + g[3] * gy + g[4] * gz
            fy = g[3] * gx + g[1] * gy + g[5] * gz
            fz = g[4] * gx + g[5] * gy + g[2] * gz
            fluxes.append(fz * plane_ref[...])
            fh, fl = split(jnp.concatenate([fx, fy], 0))
            sums.append(dot(bxy_ref[...], jnp.concatenate([fh, fl, fh], 0)))
        fh, fl = split(jnp.concatenate(fluxes, 0))
        back = dot(fh, bz_ref[:BLOCK]) + dot(fl, bz_ref[:BLOCK]) + dot(fh, bz_ref[BLOCK:])
        for c in range(components):
            total = sums[c] + back[64 * c : 64 * c + 64]
            out_ref[c, :, :, where] = total.reshape(8, 8, BLOCK)
        return carry

    lax.fori_loop(0, blocks, body, 0)

    position = lax.broadcasted_iota(jnp.int32, (8, length), 1)
    last = (position % 8 == 7) & (position != length - 1)
    initial = (position % 8 == 0) & (position != 0)
    for c in range(components):
        for x in range(8):
            row = out_ref[c, x]
            after = pltpu.roll(row, length - 1, 1)
            before = pltpu.roll(row, 1, 1)
            out_ref[c, x] = (
                row + jnp.where(last, after, 0.0) + jnp.where(initial, before, 0.0)
            )

    even_x = lax.rem(lax.axis_index("gx"), 2) == 0
    even_z = lax.rem(lax.axis_index("gz"), 2) == 0
    for c in range(components):
        for t in range(tiles):
            where = slice(t * LANES, t * LANES + LANES)
            first_plane = out_ref[c, 0, :, where]
            last_plane = out_ref[c, 7, :, where]
            xa_ref[c * tiles + t] = jnp.where(even_x, last_plane, first_plane)
            xb_ref[c * tiles + t] = jnp.where(even_x, first_plane, last_plane)
        for y, k in ((0, 0), (7, 1)):
            for x in range(8):
                yf_ref[k, c, x : x + 1, :] = out_ref[c, x, y : y + 1, :]
    lane = lane_iota()
    low_plane = jnp.zeros((8, LANES), F32)
    high_plane = jnp.zeros((8, LANES), F32)
    for c in range(components):
        for x in range(8):
            slot = 8 * c + x
            begin = out_ref[c, x, :, :LANES]
            end = out_ref[c, x, :, length - LANES :]
            begin = pltpu.roll(begin, slot, 1) if slot else begin
            end = pltpu.roll(end, slot + 1, 1)
            low_plane = jnp.where(lane == slot, begin, low_plane)
            high_plane = jnp.where(lane == slot, end, high_plane)
    za_ref[...] = jnp.where(even_z, high_plane, low_plane)
    zb_ref[...] = jnp.where(even_z, low_plane, high_plane)


def z_halo(za_ref, zb_ref):
    even_z = lax.rem(lax.axis_index("gz"), 2) == 0
    first, second = za_ref[...], zb_ref[...]
    return jnp.where(even_z, second, first), jnp.where(even_z, first, second)


def at_lane(packed, slot, lane_to):
    lane = lane_iota()
    shift = (lane_to - slot) % LANES
    moved = pltpu.roll(packed, shift, 1) if shift else packed
    return jnp.where(lane == lane_to, moved, 0.0)


def x_face_kernel(xa_ref, xb_ref, za_ref, zb_ref, outa_ref, outb_ref):
    tiles = 16
    components = xa_ref.shape[0] // tiles
    even_x = lax.rem(lax.axis_index("gx"), 2) == 0
    low, high = z_halo(za_ref, zb_ref)
    outa_ref[...] = xa_ref[...]
    outb_ref[...] = xb_ref[...]
    for c in range(components):
        for t, packed, lane_to in ((0, low, 0), (tiles - 1, high, LANES - 1)):
            first = at_lane(packed, 8 * c, lane_to)
            last = at_lane(packed, 8 * c + 7, lane_to)
            spot = c * tiles + t
            outa_ref[spot] = xa_ref[spot] + jnp.where(even_x, last, first)
            outb_ref[spot] = xb_ref[spot] + jnp.where(even_x, first, last)


def y_face_kernel(yf_ref, xa_ref, xb_ref, za_ref, zb_ref, outa_ref, outb_ref):
    tiles = 16
    components = yf_ref.shape[1]
    even_x = lax.rem(lax.axis_index("gx"), 2) == 0
    even_y = lax.rem(lax.axis_index("gy"), 2) == 0
    low, high = z_halo(za_ref, zb_ref)
    sublane = lax.broadcasted_iota(jnp.int32, (8, LANES), 0)
    lane = lane_iota()
    for c in range(components):
        halos = {}
        for t, packed, lane_to in ((0, low, 0), (tiles - 1, high, LANES - 1)):
            pieces = [jnp.zeros((8, LANES), F32)] * 2
            for k, y in ((0, 0), (1, 7)):
                for x in range(8):
                    slot = 8 * c + x
                    shift = (lane_to - slot) % LANES
                    moved = pltpu.roll(packed, shift, 1) if shift else packed
                    moved = jnp.broadcast_to(moved[y : y + 1], (8, LANES))
                    pieces[k] = jnp.where((lane == lane_to) & (sublane == x), moved, pieces[k])
            halos[t] = pieces
        for t in range(tiles):
            spot = c * tiles + t
            where = slice(t * LANES, t * LANES + LANES)
            ra, rb = xa_ref[spot], xb_ref[spot]
            below = jnp.where(even_x, rb, ra)
            above = jnp.where(even_x, ra, rb)
            sides = []
            for k, y in ((0, 0), (1, 7)):
                value = yf_ref[k, c, :, where]
                value = value + jnp.where(sublane == 0, jnp.broadcast_to(below[y : y + 1], (8, LANES)), 0.0)
                value = value + jnp.where(sublane == 7, jnp.broadcast_to(above[y : y + 1], (8, LANES)), 0.0)
                if t in halos:
                    value = value + halos[t][k]
                sides.append(value)
            outa_ref[spot] = jnp.where(even_y, sides[1], sides[0])
            outb_ref[spot] = jnp.where(even_y, sides[0], sides[1])


def final_kernel(local_ref, xa_ref, xb_ref, ya_ref, yb_ref, za_ref, zb_ref, out_ref):
    tiles = 16
    components = local_ref.shape[0]
    even_x = lax.rem(lax.axis_index("gx"), 2) == 0
    even_y = lax.rem(lax.axis_index("gy"), 2) == 0
    low, high = z_halo(za_ref, zb_ref)
    sublane = lax.broadcasted_iota(jnp.int32, (8, LANES), 0)
    for c in range(components):
        for t in range(tiles):
            spot = c * tiles + t
            where = slice(t * LANES, t * LANES + LANES)
            ra, rb = xa_ref[spot], xb_ref[spot]
            below = jnp.where(even_x, rb, ra)
            above = jnp.where(even_x, ra, rb)
            ya, yb = ya_ref[spot], yb_ref[spot]
            front = jnp.where(even_y, yb, ya)
            behind = jnp.where(even_y, ya, yb)
            for x in range(8):
                value = local_ref[c, x, :, where]
                if x == 0:
                    value = value + below
                if x == 7:
                    value = value + above
                value = value + jnp.where(
                    sublane == 0, jnp.broadcast_to(front[x : x + 1], (8, LANES)), 0.0
                )
                value = value + jnp.where(
                    sublane == 7, jnp.broadcast_to(behind[x : x + 1], (8, LANES)), 0.0
                )
                if t == 0:
                    value = value + at_lane(low, 8 * c + x, 0)
                if t == tiles - 1:
                    value = value + at_lane(high, 8 * c + x, LANES - 1)
                out_ref[c, x, :, where] = value


def pair_exchange(first, second, axis):
    count = lax.axis_size(axis)

    def pairs(start):
        found = []
        for i in range(start, count - 1, 2):
            found += [(i, i + 1), (i + 1, i)]
        return found

    return lax.ppermute(first, axis, pairs(0)), lax.ppermute(second, axis, pairs(1))


def call(kernel, outs, scratch=(), flops=1000000):
    return pl.pallas_call(
        kernel,
        out_shape=[jax.ShapeDtypeStruct(shape, F32) for shape in outs],
        scratch_shapes=list(scratch),
        compiler_params=pltpu.CompilerParams(vmem_limit_bytes=24 * 1024 * 1024),
        cost_estimate=pl.CostEstimate(flops=flops, bytes_accessed=1000000, transcendentals=0),
    )


def local(nodal, geometry):
    components, _, _, length = nodal.shape
    tiles = length // LANES
    geo = geometry.reshape(6, length // 8)
    face = (components * tiles, 8, LANES)
    tile = (8, LANES)
    result, xa, xb, yf, za, zb = call(
        stiffness_kernel,
        [nodal.shape, face, face, (2, components, 8, length), tile, tile],
        [pltpu.VMEM((8 * length // BLOCK, BLOCK), F32)],
    )(nodal, geo, *[jnp.asarray(table) for table in tables()])
    za, zb = pair_exchange(za, zb, "gz")
    xa, xb = call(x_face_kernel, [face, face])(xa, xb, za, zb)
    xa, xb = pair_exchange(xa, xb, "gx")
    ya, yb = call(y_face_kernel, [face, face])(yf, xa, xb, za, zb)
    ya, yb = pair_exchange(ya, yb, "gy")
    (result,) = call(final_kernel, [nodal.shape])(result, xa, xb, ya, yb, za, zb)
    return result


def solution(mesh):
    return jax.shard_map(
        local,
        mesh=mesh,
        in_specs=(P(None, "gx", "gy", "gz"), P(None, "gx", "gy", "gz")),
        out_specs=P(None, "gx", "gy", "gz"),
        check_vma=False,
    )
```

```python
import functools

import jax
import jax.numpy as jnp
import numpy as np
from jax import lax
from jax.experimental import pallas as pl
from jax.experimental.pallas import tpu as pltpu
from jax.sharding import PartitionSpec as P

interior_points = [
    -0.8717401485096066,
    -0.5917001814331423,
    -0.2092992179024789,
    0.2092992179024789,
    0.5917001814331423,
    0.8717401485096066,
]
LANES = 128
BLOCK = 256
F32 = jnp.float32
BF16 = jnp.bfloat16


def legendre_seven(point):
    previous = 1.0
    current = point
    for order in range(1, 7):
        following = ((2 * order + 1) * point * current - order * previous) / (order + 1)
        previous = current
        current = following
    return current


def gll_tables():
    degree = 7
    points = [-1.0] + interior_points + [1.0]
    values = [legendre_seven(point) for point in points]
    node_count = degree + 1
    weights = np.array([2.0 / (degree * (degree + 1) * value * value) for value in values])
    derivative = np.zeros((node_count, node_count))
    for row_index in range(node_count):
        for col_index in range(node_count):
            if row_index != col_index:
                derivative[row_index, col_index] = values[row_index] / (
                    values[col_index] * (points[row_index] - points[col_index])
                )
    derivative[0, 0] = -degree * (degree + 1) / 4.0
    derivative[node_count - 1, node_count - 1] = degree * (degree + 1) / 4.0
    return (derivative.astype(np.float32).astype(np.float64), weights)


def split_table(table):
    high = np.asarray(table, np.float32).astype(jnp.bfloat16)
    low = (np.asarray(table, np.float64) - high.astype(np.float64)).astype(jnp.bfloat16)
    return high, low


def tables():
    derivative, weights = gll_tables()
    eye = np.eye(8)
    grads = np.concatenate([np.kron(derivative, eye), np.kron(eye, derivative)], 0)
    high, low = split_table(grads)
    grad_xy = np.concatenate([high, high, low], 1)
    plane = np.kron(weights, weights)
    back_x = np.kron((derivative * weights[:, None]).T, np.diag(weights))
    back_y = np.kron(np.diag(weights), (derivative * weights[:, None]).T)
    high, low = split_table(np.concatenate([back_x, back_y], 1))
    back_xy = np.concatenate([high, high, low], 1)
    many = np.eye(BLOCK // 8)
    grad_z = np.concatenate(split_table(np.kron(many, derivative.T)), 0)
    back_z = np.concatenate(split_table(np.kron(many, derivative)), 0)
    spread = np.kron(np.eye(LANES)[:, : BLOCK // 8], np.ones((1, 8))).astype(jnp.bfloat16)
    weight_z = np.tile(weights, BLOCK // 8)[None].astype(np.float32)
    plane = np.tile(plane[:, None], (1, BLOCK)).astype(np.float32)
    return grad_xy, back_xy, grad_z, back_z, spread, weight_z, plane


def split(values):
    high = values.astype(BF16)
    return high, (values - high.astype(F32)).astype(BF16)


def dot(left, right):
    return jnp.dot(left, right, preferred_element_type=F32)


def lane_iota():
    return lax.broadcasted_iota(jnp.int32, (8, LANES), 1)


def stiffness_kernel(
    u_hbm, geo_hbm, gxy_hbm, bxy_hbm, gz_hbm, bz_hbm, spread_hbm, wz_hbm, plane_hbm,
    out_ref, xa_ref, xb_ref, ia_ref, ib_ref, ea_ref, eb_ref, za_ref, zb_ref,
    u_ref, geo_ref, gxy_ref, bxy_ref, gz_ref, bz_ref, spread_ref, wz_ref, plane_ref,
    geo_scr, sems,
):
    components = u_ref.shape[0]
    length = u_ref.shape[3]
    blocks = length // BLOCK
    tiles = length // LANES
    per_block = BLOCK // 8
    copies = []
    sources = (geo_hbm, spread_hbm, wz_hbm, gz_hbm, gxy_hbm, plane_hbm, bxy_hbm, bz_hbm)
    targets = (geo_ref, spread_ref, wz_ref, gz_ref, gxy_ref, plane_ref, bxy_ref, bz_ref)
    for k, (source, target) in enumerate(zip(sources, targets)):
        copies.append(pltpu.make_async_copy(source, target, sems.at[blocks + k]))
        copies[-1].start()

    def piece(block):
        where = pl.ds(pl.multiple_of(block * BLOCK, BLOCK), BLOCK)
        return pltpu.make_async_copy(
            u_hbm.at[:, :, :, where], u_ref.at[:, :, :, where], sems.at[block]
        )

    for block in range(blocks):
        piece(block).start()
    for copy in copies:
        copy.wait()
    geo = jnp.concatenate(
        [geo_ref[k, 0] for k in range(6)] + [jnp.zeros((2, length // 8), F32)], 0
    )
    rows = []
    for block in range(blocks):
        start = block * per_block
        tile = geo[:, start // LANES * LANES : start // LANES * LANES + LANES]
        shift = start % LANES
        rows.append(pltpu.roll(tile, LANES - shift, 1) if shift else tile)
    stacked = jnp.concatenate(rows, 0)
    first = stacked.astype(BF16)
    rest = stacked - first.astype(F32)
    second = rest.astype(BF16)
    third = (rest - second.astype(F32)).astype(BF16)
    spread = spread_ref[...]
    expanded = dot(first, spread) + dot(second, spread) + dot(third, spread)
    geo_scr[...] = expanded * wz_ref[...]

    def body(block, carry):
        piece(block).wait()
        where = pl.ds(pl.multiple_of(block * BLOCK, BLOCK), BLOCK)
        field = jnp.concatenate(
            [u_ref[c, :, :, where].reshape(64, BLOCK) for c in range(components)], 0
        )
        high, low = split(field)
        grad_z = (
            dot(high, gz_ref[:BLOCK]) + dot(low, gz_ref[:BLOCK]) + dot(high, gz_ref[BLOCK:])
        )
        factor = geo_scr[pl.ds(pl.multiple_of(block * 8, 8), 8), :]
        g = [factor[k : k + 1] for k in range(6)]
        fluxes = []
        sums = []
        for c in range(components):
            mine = slice(64 * c, 64 * c + 64)
            stack = jnp.concatenate([high[mine], low[mine], high[mine]], 0)
            both = dot(gxy_ref[...], stack)
            gx, gy, gz = both[:64], both[64:], grad_z[mine]
            fx = g[0] * gx + g[3] * gy + g[4] * gz
            fy = g[3] * gx + g[1] * gy + g[5] * gz
            fz = g[4] * gx + g[5] * gy + g[2] * gz
            fluxes.append(fz * plane_ref[...])
            fh, fl = split(jnp.concatenate([fx, fy], 0))
            sums.append(dot(bxy_ref[...], jnp.concatenate([fh, fl, fh], 0)))
        fh, fl = split(jnp.concatenate(fluxes, 0))
        back = dot(fh, bz_ref[:BLOCK]) + dot(fl, bz_ref[:BLOCK]) + dot(fh, bz_ref[BLOCK:])
        for c in range(components):
            total = sums[c] + back[64 * c : 64 * c + 64]
            out_ref[c, :, :, where] = total.reshape(8, 8, BLOCK)
        return carry

    lax.fori_loop(0, blocks, body, 0)

    position = lax.broadcasted_iota(jnp.int32, (8, length), 1)
    last = (position % 8 == 7) & (position != length - 1)
    initial = (position % 8 == 0) & (position != 0)
    for c in range(components):
        for x in range(8):
            row = out_ref[c, x]
            after = pltpu.roll(row, length - 1, 1)
            before = pltpu.roll(row, 1, 1)
            out_ref[c, x] = (
                row + jnp.where(last, after, 0.0) + jnp.where(initial, before, 0.0)
            )

    even_x = lax.rem(lax.axis_index("gx"), 2) == 0
    even_y = lax.rem(lax.axis_index("gy"), 2) == 0
    even_z = lax.rem(lax.axis_index("gz"), 2) == 0
    for c in range(components):
        for t in range(tiles):
            where = slice(t * LANES, t * LANES + LANES)
            first_plane = out_ref[c, 0, :, where]
            last_plane = out_ref[c, 7, :, where]
            xa_ref[c * tiles + t] = jnp.where(even_x, last_plane, first_plane)
            xb_ref[c * tiles + t] = jnp.where(even_x, first_plane, last_plane)
            for x in range(8):
                first_row = out_ref[c, x, 0:1, where]
                last_row = out_ref[c, x, 7:8, where]
                row_a = jnp.where(even_y, last_row, first_row)
                row_b = jnp.where(even_y, first_row, last_row)
                if x in (0, 7):
                    spot = 6 * t + 2 * c + x // 7
                    ea_ref[spot : spot + 1] = row_a
                    eb_ref[spot : spot + 1] = row_b
                else:
                    spot = 18 * t + 6 * c + x - 1
                    ia_ref[spot : spot + 1] = row_a
                    ib_ref[spot : spot + 1] = row_b
    lane = lane_iota()
    low_plane = jnp.zeros((8, LANES), F32)
    high_plane = jnp.zeros((8, LANES), F32)
    for c in range(components):
        for x in range(8):
            slot = 8 * c + x
            begin = out_ref[c, x, :, :LANES]
            end = out_ref[c, x, :, length - LANES :]
            begin = pltpu.roll(begin, slot, 1) if slot else begin
            end = pltpu.roll(end, slot + 1, 1)
            low_plane = jnp.where(lane == slot, begin, low_plane)
            high_plane = jnp.where(lane == slot, end, high_plane)
    za_ref[...] = jnp.where(even_z, high_plane, low_plane)
    zb_ref[...] = jnp.where(even_z, low_plane, high_plane)


def ordered(even, first, second):
    return jnp.where(even, second, first), jnp.where(even, first, second)


def parities():
    return [lax.rem(lax.axis_index(axis), 2) == 0 for axis in ("gx", "gy", "gz")]


def at_lane(packed, slot, lane_to):
    shift = (lane_to - slot) % LANES
    moved = pltpu.roll(packed, shift, 1) if shift else packed
    return jnp.where(lane_iota() == lane_to, moved, 0.0)


def x_sides(xa_ref, xb_ref, spot, c, t, even_x, halos):
    below, above = ordered(even_x, xa_ref[spot], xb_ref[spot])
    if t in halos:
        lane_to, mine, lower, upper = halos[t]
        below = below + at_lane(lower, 8 * c + 7, lane_to) + at_lane(mine, 8 * c, lane_to)
        above = above + at_lane(upper, 8 * c, lane_to) + at_lane(mine, 8 * c + 7, lane_to)
    return below, above


def halo_table(za_ref, zb_ref, na_ref, nb_ref, tiles, even_x, even_z):
    low, high = ordered(even_z, za_ref[...], zb_ref[...])
    low_a, high_a = ordered(even_z, na_ref[0], na_ref[1])
    low_b, high_b = ordered(even_z, nb_ref[0], nb_ref[1])
    lower_low, upper_low = ordered(even_x, low_a, low_b)
    lower_high, upper_high = ordered(even_x, high_a, high_b)
    return {
        0: (0, low, lower_low, upper_low),
        tiles - 1: (LANES - 1, high, lower_high, upper_high),
    }


def edge_kernel(
    ea_ref, eb_ref, xa_ref, xb_ref, za_ref, zb_ref, na_ref, nb_ref, outa_ref, outb_ref
):
    tiles = ea_ref.shape[0] // 6
    components = xa_ref.shape[0] // tiles
    even_x, even_y, even_z = parities()
    halos = halo_table(za_ref, zb_ref, na_ref, nb_ref, tiles, even_x, even_z)
    for c in range(components):
        for t in range(tiles):
            sides = x_sides(xa_ref, xb_ref, c * tiles + t, c, t, even_x, halos)
            for k in range(2):
                spot = 6 * t + 2 * c + k
                at = slice(spot, spot + 1)
                first, last = sides[k][0:1], sides[k][7:8]
                outa_ref[at] = ea_ref[at] + jnp.where(even_y, last, first)
                outb_ref[at] = eb_ref[at] + jnp.where(even_y, first, last)
    base = 6 * tiles
    for out in (outa_ref, outb_ref):
        out[base : base + 8] = za_ref[...]
        out[base + 8 : base + 16] = zb_ref[...]


def final_kernel(
    local_ref, xa_ref, xb_ref, ia_ref, ib_ref, ea_ref, eb_ref,
    za_ref, zb_ref, na_ref, nb_ref, out_hbm, out_ref, sems,
):
    components = local_ref.shape[0]
    tiles = local_ref.shape[3] // LANES
    even_x, even_y, even_z = parities()
    halos = halo_table(za_ref, zb_ref, na_ref, nb_ref, tiles, even_x, even_z)
    sublane = lax.broadcasted_iota(jnp.int32, (8, LANES), 0)
    base = 6 * tiles
    far = {}
    for t, half in ((0, 0), (tiles - 1, 1)):
        per_side = []
        for ref in (ea_ref, eb_ref):
            pair = ordered(even_z, ref[base : base + 8], ref[base + 8 : base + 16])
            per_side.append(pair[half])
        far[t] = ordered(even_y, *per_side)
    copies = []
    for c in range(components):
        for t in range(tiles):
            where = slice(t * LANES, t * LANES + LANES)
            below, above = x_sides(xa_ref, xb_ref, c * tiles + t, c, t, even_x, halos)
            inner = slice(18 * t + 6 * c, 18 * t + 6 * c + 6)
            outer = slice(6 * t + 2 * c, 6 * t + 2 * c + 2)
            front_in, behind_in = ordered(even_y, ia_ref[inner], ib_ref[inner])
            front_out, behind_out = ordered(even_y, ea_ref[outer], eb_ref[outer])
            for x in range(8):
                value = local_ref[c, x, :, where]
                if x in (0, 7):
                    value = value + (above if x else below)
                    k = x // 7
                    front, behind = front_out[k : k + 1], behind_out[k : k + 1]
                else:
                    front, behind = front_in[x - 1 : x], behind_in[x - 1 : x]
                front = jnp.broadcast_to(front, (8, LANES))
                behind = jnp.broadcast_to(behind, (8, LANES))
                if t in halos and x not in (0, 7):
                    lane_to, mine, _, _ = halos[t]
                    value = value + at_lane(mine, 8 * c + x, lane_to)
                    near, away = far[t]
                    near = at_lane(near, 8 * c + x, lane_to)[7:8]
                    away = at_lane(away, 8 * c + x, lane_to)[0:1]
                    front = front + jnp.broadcast_to(near, (8, LANES))
                    behind = behind + jnp.broadcast_to(away, (8, LANES))
                value = value + jnp.where(sublane == 0, front, 0.0)
                value = value + jnp.where(sublane == 7, behind, 0.0)
                out_ref[c, x, :, where] = value
        copies.append(pltpu.make_async_copy(out_ref.at[c], out_hbm.at[c], sems.at[c]))
        copies[-1].start()
    for copy in copies:
        copy.wait()


def pair_exchange(first, second, axis):
    count = lax.axis_size(axis)

    def pairs(start):
        found = []
        for i in range(start, count - 1, 2):
            found += [(i, i + 1), (i + 1, i)]
        return found

    return lax.ppermute(first, axis, pairs(0)), lax.ppermute(second, axis, pairs(1))


def call(kernel, outs, scratch=(), flops=1000000, **specs):
    return pl.pallas_call(
        kernel,
        out_shape=[jax.ShapeDtypeStruct(shape, F32) for shape in outs],
        scratch_shapes=list(scratch),
        compiler_params=pltpu.CompilerParams(vmem_limit_bytes=24 * 1024 * 1024),
        cost_estimate=pl.CostEstimate(flops=flops, bytes_accessed=1000000, transcendentals=0),
        **specs,
    )


def local(nodal, geometry):
    components, _, _, length = nodal.shape
    tiles = length // LANES
    blocks = length // BLOCK
    face = (components * tiles, 8, LANES)
    inner = (components * tiles * 6, LANES)
    edge = (components * tiles * 2, LANES)
    tile = (8, LANES)
    constants = [jnp.asarray(table) for table in tables()]
    order = [0, 1, 2, 3, 4, 5, 6]
    operands = [nodal, geometry] + [constants[k] for k in order]
    hbm = pl.BlockSpec(memory_space=pltpu.HBM)
    result, xa, xb, ia, ib, ea, eb, za, zb = call(
        stiffness_kernel,
        [nodal.shape, face, face, inner, inner, edge, edge, tile, tile],
        [pltpu.VMEM(operand.shape, operand.dtype) for operand in operands]
        + [
            pltpu.VMEM((8 * blocks, BLOCK), F32),
            pltpu.SemaphoreType.DMA((blocks + len(constants) + 1,)),
        ],
        in_specs=[hbm] * len(operands),
    )(*operands)
    xa, xb = pair_exchange(xa, xb, "gx")
    za, zb = pair_exchange(za, zb, "gz")
    ia, ib = pair_exchange(ia, ib, "gy")
    halo = jnp.stack([za, zb])
    na, nb = pair_exchange(halo, halo, "gx")
    longer = (edge[0] + 16, LANES)
    ea, eb = call(edge_kernel, [longer, longer])(ea, eb, xa, xb, za, zb, na, nb)
    ea, eb = pair_exchange(ea, eb, "gy")
    (result,) = call(
        final_kernel,
        [nodal.shape],
        [pltpu.VMEM(nodal.shape, F32), pltpu.SemaphoreType.DMA((components,))],
        out_specs=[hbm],
    )(result, xa, xb, ia, ib, ea, eb, za, zb, na, nb)
    return result


def solution(mesh):
    return jax.shard_map(
        local,
        mesh=mesh,
        in_specs=(P(None, "gx", "gy", "gz"), P(None, "gx", "gy", "gz")),
        out_specs=P(None, "gx", "gy", "gz"),
        check_vma=False,
    )
```

```python
import functools

import jax
import jax.numpy as jnp
import numpy as np
from jax import lax
from jax.experimental import pallas as pl
from jax.experimental.pallas import tpu as pltpu
from jax.sharding import PartitionSpec as P

interior_points = [
    -0.8717401485096066,
    -0.5917001814331423,
    -0.2092992179024789,
    0.2092992179024789,
    0.5917001814331423,
    0.8717401485096066,
]
LANES = 128
BLOCK = 256
F32 = jnp.float32
BF16 = jnp.bfloat16


def legendre_seven(point):
    previous = 1.0
    current = point
    for order in range(1, 7):
        following = ((2 * order + 1) * point * current - order * previous) / (order + 1)
        previous = current
        current = following
    return current


def gll_tables():
    degree = 7
    points = [-1.0] + interior_points + [1.0]
    values = [legendre_seven(point) for point in points]
    node_count = degree + 1
    weights = np.array([2.0 / (degree * (degree + 1) * value * value) for value in values])
    derivative = np.zeros((node_count, node_count))
    for row_index in range(node_count):
        for col_index in range(node_count):
            if row_index != col_index:
                derivative[row_index, col_index] = values[row_index] / (
                    values[col_index] * (points[row_index] - points[col_index])
                )
    derivative[0, 0] = -degree * (degree + 1) / 4.0
    derivative[node_count - 1, node_count - 1] = degree * (degree + 1) / 4.0
    return (derivative.astype(np.float32).astype(np.float64), weights)


def split_table(table):
    high = np.asarray(table, np.float32).astype(jnp.bfloat16)
    low = (np.asarray(table, np.float64) - high.astype(np.float64)).astype(jnp.bfloat16)
    return high, low


def tables():
    derivative, weights = gll_tables()
    eye = np.eye(8)
    zero = np.zeros((64, 64))

    def doubled(table):
        high, low = split_table(table)
        top = np.concatenate([high, high], 1)
        return np.concatenate([top, np.concatenate([low, zero.astype(low.dtype)], 1)], 0)

    grad_y = doubled(np.kron(eye, derivative))
    back = (derivative * weights[:, None]).T
    back_y = doubled(np.kron(np.diag(weights), back))
    many = np.eye(BLOCK // 8)
    grad_z = np.concatenate(split_table(np.kron(many, derivative.T)), 0)
    back_z = np.concatenate(split_table(np.kron(many, derivative)), 0)
    spread = np.kron(np.eye(LANES)[:, : BLOCK // 8], np.ones((1, 8))).astype(jnp.bfloat16)
    weight_z = np.tile(weights, BLOCK // 8)[None].astype(np.float32)
    plane = np.tile(np.kron(weights, weights)[:, None], (1, BLOCK)).astype(np.float32)
    return grad_y, back_y, grad_z, back_z, spread, weight_z, plane


def x_matrices():
    derivative, weights = gll_tables()
    scaled = (derivative * weights[:, None]).T / weights[:, None]
    return derivative, scaled


def split(values):
    high = values.astype(BF16)
    return high, (values - high.astype(F32)).astype(BF16)


def dot(left, right):
    return jnp.dot(left, right, preferred_element_type=F32)


def lane_iota():
    return lax.broadcasted_iota(jnp.int32, (8, LANES), 1)


def along_x(planes, matrix):
    even = [planes[b] + planes[7 - b] for b in range(4)]
    odd = [planes[b] - planes[7 - b] for b in range(4)]
    result = [None] * 8
    for a in range(4):
        first = second = None
        for b in range(4):
            p = float((matrix[a, b] + matrix[a, 7 - b]) / 2)
            q = float((matrix[a, b] - matrix[a, 7 - b]) / 2)
            first = even[b] * p if first is None else first + even[b] * p
            second = odd[b] * q if second is None else second + odd[b] * q
        result[a] = second + first
        result[7 - a] = second - first
    return result


def operator_block(field, factor, gy_ref, by_ref, gz_ref, bz_ref, plane):
    forward, backward = x_matrices()
    count = field.shape[0] // 64
    high, low = split(field)
    grad_z = dot(high, gz_ref[:BLOCK]) + dot(low, gz_ref[:BLOCK]) + dot(high, gz_ref[BLOCK:])
    g = [factor[k : k + 1] for k in range(6)]
    fluxes = []
    along_y = []
    sums = []
    for c in range(count):
        mine = slice(64 * c, 64 * c + 64)
        both = dot(gy_ref[...], jnp.concatenate([high[mine], low[mine]], 0))
        gy = both[:64] + both[64:]
        gz = grad_z[mine]
        gx = along_x([field[64 * c + 8 * x : 64 * c + 8 * x + 8] for x in range(8)], forward)
        gx = jnp.concatenate(gx, 0)
        fx = g[0] * gx + g[3] * gy + g[4] * gz
        fy = g[3] * gx + g[1] * gy + g[5] * gz
        fz = g[4] * gx + g[5] * gy + g[2] * gz
        fluxes.append(fz)
        fh, fl = split(fy)
        both = dot(by_ref[...], jnp.concatenate([fh, fl], 0))
        along_y.append(both[:64] + both[64:])
        sums.append(jnp.concatenate(along_x([fx[8 * x : 8 * x + 8] for x in range(8)], backward), 0))
    fh, fl = split(jnp.concatenate(fluxes, 0))
    back = dot(fh, bz_ref[:BLOCK]) + dot(fl, bz_ref[:BLOCK]) + dot(fh, bz_ref[BLOCK:])
    return [
        along_y[c] + plane * (sums[c] + back[64 * c : 64 * c + 64]) for c in range(count)
    ]


def spread_rows(rows, spread, weight):
    first = rows.astype(BF16)
    rest = rows - first.astype(F32)
    second = rest.astype(BF16)
    third = (rest - second.astype(F32)).astype(BF16)
    return (dot(first, spread) + dot(second, spread) + dot(third, spread)) * weight


def load_kernel(
    u_hbm, geo_hbm, gy_hbm, by_hbm, gz_hbm, bz_hbm, spread_hbm, wz_hbm, plane_hbm,
    u_ref, factor_ref, gy_ref, by_ref, gz_ref, bz_ref, plane_ref, za_ref, zb_ref,
    geo_ref, spread_ref, wz_ref, sems,
):
    components = u_ref.shape[0]
    length = u_ref.shape[3]
    blocks = length // BLOCK
    per_block = BLOCK // 8
    copies = []
    ends = (pl.ds(0, LANES), pl.ds(length - LANES, LANES))
    middle = pl.ds(LANES, length - 2 * LANES)
    pairs = [(geo_hbm, geo_ref), (spread_hbm, spread_ref), (wz_hbm, wz_ref)]
    pairs += [(u_hbm.at[:, :, :, where], u_ref.at[:, :, :, where]) for where in ends]
    pairs += [(gz_hbm, gz_ref), (gy_hbm, gy_ref), (by_hbm, by_ref), (bz_hbm, bz_ref)]
    pairs += [(plane_hbm, plane_ref)]
    pairs += [(u_hbm.at[c, :, :, middle], u_ref.at[c, :, :, middle]) for c in range(components)]
    for k, (source, target) in enumerate(pairs):
        copies.append(pltpu.make_async_copy(source, target, sems.at[k]))
        copies[-1].start()
    for copy in copies[:3]:
        copy.wait()
    geo = jnp.concatenate(
        [geo_ref[k, 0] for k in range(6)] + [jnp.zeros((2, length // 8), F32)], 0
    )
    rows = []
    for block in range(blocks):
        start = block * per_block
        tile = geo[:, start // LANES * LANES : start // LANES * LANES + LANES]
        shift = start % LANES
        rows.append(pltpu.roll(tile, LANES - shift, 1) if shift else tile)
    expanded = spread_rows(jnp.concatenate(rows, 0), spread_ref[...], wz_ref[...])
    factor_ref[...] = expanded
    for copy in copies[3:10]:
        copy.wait()
    factor = jnp.concatenate([expanded[:8, :LANES], expanded[8 * blocks - 8 :, LANES:]], 1)
    sides = []
    for c in range(components):
        sides.append(jnp.concatenate([u_ref[c, :, :, where].reshape(64, LANES) for where in ends], 1))
    totals = operator_block(
        jnp.concatenate(sides, 0), factor, gy_ref, by_ref, gz_ref, bz_ref, plane_ref[...]
    )
    even_z = lax.rem(lax.axis_index("gz"), 2) == 0
    lane = lane_iota()
    low_plane = jnp.zeros((8, LANES), F32)
    high_plane = jnp.zeros((8, LANES), F32)
    for c in range(components):
        for x in range(8):
            slot = 8 * c + x
            begin = totals[c][8 * x : 8 * x + 8, :LANES]
            end = totals[c][8 * x : 8 * x + 8, LANES:]
            begin = pltpu.roll(begin, slot, 1) if slot else begin
            end = pltpu.roll(end, slot + 1, 1)
            low_plane = jnp.where(lane == slot, begin, low_plane)
            high_plane = jnp.where(lane == slot, end, high_plane)
    za_ref[...] = jnp.where(even_z, high_plane, low_plane)
    zb_ref[...] = jnp.where(even_z, low_plane, high_plane)
    for copy in copies[10:]:
        copy.wait()


def stiffness_kernel(
    u_ref, factor_ref, gy_ref, by_ref, gz_ref, bz_ref, plane_ref, za_ref, zb_ref,
    out_ref, xa_ref, xb_ref, ia_ref, ea_ref, yb_ref,
):
    components = u_ref.shape[0]
    length = u_ref.shape[3]
    blocks = length // BLOCK
    tiles = length // LANES

    def body(block, carry):
        where = pl.ds(pl.multiple_of(block * BLOCK, BLOCK), BLOCK)
        field = jnp.concatenate(
            [u_ref[c, :, :, where].reshape(64, BLOCK) for c in range(components)], 0
        )
        factor = factor_ref[pl.ds(pl.multiple_of(block * 8, 8), 8), :]
        totals = operator_block(field, factor, gy_ref, by_ref, gz_ref, bz_ref, plane_ref[...])
        for c in range(components):
            out_ref[c, :, :, where] = totals[c].reshape(8, 8, BLOCK)
        return carry

    lax.fori_loop(0, blocks, body, 0)

    even_x, even_y, even_z = parities()
    low, high = ordered(even_z, za_ref[...], zb_ref[...])
    position = lax.broadcasted_iota(jnp.int32, (8, length), 1)
    last = (position % 8 == 7) & (position != length - 1)
    initial = (position % 8 == 0) & (position != 0)
    for c in range(components):
        for x in range(8):
            row = out_ref[c, x]
            after = pltpu.roll(row, length - 1, 1)
            before = pltpu.roll(row, 1, 1)
            row = row + jnp.where(last, after, 0.0) + jnp.where(initial, before, 0.0)
            slot = 8 * c + x
            out_ref[c, x] = row
            out_ref[c, x, :, :LANES] = row[:, :LANES] + at_lane(low, slot, 0)
            out_ref[c, x, :, length - LANES :] = row[:, length - LANES :] + at_lane(
                high, slot, LANES - 1
            )

    for c in range(components):
        for t in range(tiles):
            where = slice(t * LANES, t * LANES + LANES)
            spot = c * tiles + t
            first_plane = out_ref[c, 0, :, where]
            last_plane = out_ref[c, 7, :, where]
            xa_ref[spot] = jnp.where(even_x, last_plane, first_plane)
            xb_ref[spot] = jnp.where(even_x, first_plane, last_plane)
            for x in range(8):
                first_row = out_ref[c, x, 0:1, where]
                last_row = out_ref[c, x, 7:8, where]
                row_a = jnp.where(even_y, last_row, first_row)
                yb_ref[spot, x : x + 1] = jnp.where(even_y, first_row, last_row)
                if x in (0, 7):
                    at = 6 * t + 2 * c + x // 7
                    ea_ref[at : at + 1] = row_a
                else:
                    at = 18 * t + 6 * c + x - 1
                    ia_ref[at : at + 1] = row_a


def ordered(even, first, second):
    return jnp.where(even, second, first), jnp.where(even, first, second)


def parities():
    return [lax.rem(lax.axis_index(axis), 2) == 0 for axis in ("gx", "gy", "gz")]


def at_lane(packed, slot, lane_to):
    shift = (lane_to - slot) % LANES
    moved = pltpu.roll(packed, shift, 1) if shift else packed
    return jnp.where(lane_iota() == lane_to, moved, 0.0)


def edge_kernel(ea_ref, yb_ref, xa_ref, xb_ref, outa_ref, outb_ref):
    tiles = ea_ref.shape[0] // 6
    components = xa_ref.shape[0] // tiles
    even_x, even_y, _ = parities()
    for c in range(components):
        for t in range(tiles):
            spot = c * tiles + t
            sides = ordered(even_x, xa_ref[spot], xb_ref[spot])
            outb_ref[spot] = yb_ref[spot]
            for k in range(2):
                at = 6 * t + 2 * c + k
                at = slice(at, at + 1)
                first, last = sides[k][0:1], sides[k][7:8]
                outa_ref[at] = ea_ref[at] + jnp.where(even_y, last, first)
                x = slice(7 * k, 7 * k + 1)
                outb_ref[spot, x] = yb_ref[spot, x] + jnp.where(even_y, first, last)


def final_kernel(
    local_ref, xa_ref, xb_ref, ia_ref, ea_ref, yb_ref, out_hbm, out_ref, sems
):
    components = local_ref.shape[0]
    tiles = local_ref.shape[3] // LANES
    even_x, even_y, _ = parities()
    sublane = lax.broadcasted_iota(jnp.int32, (8, LANES), 0)
    row_a = jnp.where(even_y, 7, 0)
    row_b = 7 - row_a
    is_a, is_b = sublane == row_a, sublane == row_b
    copies = []
    for c in range(components):
        for t in range(tiles):
            where = slice(t * LANES, t * LANES + LANES)
            spot = c * tiles + t
            below, above = ordered(even_x, xa_ref[spot], xb_ref[spot])
            for x in range(8):
                value = local_ref[c, x, :, where]
                if x in (0, 7):
                    value = value + (above if x else below)
                    at = 6 * t + 2 * c + x // 7
                    line = ea_ref[at : at + 1]
                else:
                    at = 18 * t + 6 * c + x - 1
                    line = ia_ref[at : at + 1]
                other = yb_ref[spot, x : x + 1]
                line = jnp.broadcast_to(line, (8, LANES))
                other = jnp.broadcast_to(other, (8, LANES))
                change = jnp.where(is_a, line, jnp.where(is_b, other, 0.0))
                out_ref[c, x, :, where] = value + change
        copies.append(pltpu.make_async_copy(out_ref.at[c], out_hbm.at[c], sems.at[c]))
        copies[-1].start()
    for copy in copies:
        copy.wait()


def pairs_from(start, count):
    found = []
    for i in range(start, count - 1, 2):
        found += [(i, i + 1), (i + 1, i)]
    return found


def exchange(array, axis, start):
    return lax.ppermute(array, axis, pairs_from(start, lax.axis_size(axis)))


def call(kernel, outs, scratch=(), flops=1000000, **specs):
    shapes = [out if hasattr(out, "dtype") else jax.ShapeDtypeStruct(out, F32) for out in outs]
    return pl.pallas_call(
        kernel,
        out_shape=shapes,
        scratch_shapes=list(scratch),
        compiler_params=pltpu.CompilerParams(vmem_limit_bytes=24 * 1024 * 1024),
        cost_estimate=pl.CostEstimate(flops=flops, bytes_accessed=1000000, transcendentals=0),
        **specs,
    )


def local(nodal, geometry):
    components, _, _, length = nodal.shape
    tiles = length // LANES
    blocks = length // BLOCK
    face = (components * tiles, 8, LANES)
    inner = (components * tiles * 6, LANES)
    edge = (components * tiles * 2, LANES)
    tile = (8, LANES)
    constants = [jnp.asarray(table) for table in tables()]
    operands = [
        pltpu.with_memory_space_constraint(operand, pltpu.HBM)
        for operand in [nodal, geometry] + constants
    ]
    hbm = pl.BlockSpec(memory_space=pltpu.HBM)
    kept = [jax.ShapeDtypeStruct(constants[k].shape, constants[k].dtype) for k in (0, 1, 2, 3, 6)]
    loaded = call(
        load_kernel,
        [nodal.shape, (8 * blocks, BLOCK)] + kept + [tile, tile],
        [pltpu.VMEM(operands[k].shape, operands[k].dtype) for k in (1, 6, 7)]
        + [pltpu.SemaphoreType.DMA((10 + components,))],
        in_specs=[hbm] * len(operands),
    )(*operands)
    za = exchange(loaded[-2], "gz", 0)
    zb = exchange(loaded[-1], "gz", 1)
    result, xa, xb, ia, ea, yb = call(
        stiffness_kernel, [nodal.shape, face, face, inner, edge, face]
    )(*loaded[:-2], za, zb)
    xa = exchange(xa, "gx", 0)
    xb = exchange(xb, "gx", 1)
    ia = exchange(ia, "gy", 0)
    ea, yb = call(edge_kernel, [edge, face])(ea, yb, xa, xb)
    yb = exchange(yb, "gy", 1)
    ea = exchange(ea, "gy", 0)
    (result,) = call(
        final_kernel,
        [nodal.shape],
        [pltpu.VMEM(nodal.shape, F32), pltpu.SemaphoreType.DMA((components,))],
        out_specs=[hbm],
    )(result, xa, xb, ia, ea, yb)
    return result


def solution(mesh):
    return jax.shard_map(
        local,
        mesh=mesh,
        in_specs=(P(None, "gx", "gy", "gz"), P(None, "gx", "gy", "gz")),
        out_specs=P(None, "gx", "gy", "gz"),
        check_vma=False,
    )
```

```python
import functools

import jax
import jax.numpy as jnp
import numpy as np
from jax import lax
from jax.experimental import pallas as pl
from jax.experimental.pallas import tpu as pltpu
from jax.sharding import PartitionSpec as P

interior_points = [
    -0.8717401485096066,
    -0.5917001814331423,
    -0.2092992179024789,
    0.2092992179024789,
    0.5917001814331423,
    0.8717401485096066,
]
LANES = 128
BLOCK = 256
F32 = jnp.float32
BF16 = jnp.bfloat16


def legendre_seven(point):
    previous = 1.0
    current = point
    for order in range(1, 7):
        following = ((2 * order + 1) * point * current - order * previous) / (order + 1)
        previous = current
        current = following
    return current


def gll_tables():
    degree = 7
    points = [-1.0] + interior_points + [1.0]
    values = [legendre_seven(point) for point in points]
    node_count = degree + 1
    weights = np.array([2.0 / (degree * (degree + 1) * value * value) for value in values])
    derivative = np.zeros((node_count, node_count))
    for row_index in range(node_count):
        for col_index in range(node_count):
            if row_index != col_index:
                derivative[row_index, col_index] = values[row_index] / (
                    values[col_index] * (points[row_index] - points[col_index])
                )
    derivative[0, 0] = -degree * (degree + 1) / 4.0
    derivative[node_count - 1, node_count - 1] = degree * (degree + 1) / 4.0
    return (derivative.astype(np.float32).astype(np.float64), weights)


def split_table(table):
    high = np.asarray(table, np.float32).astype(jnp.bfloat16)
    low = (np.asarray(table, np.float64) - high.astype(np.float64)).astype(jnp.bfloat16)
    return high, low


def tables():
    derivative, weights = gll_tables()
    eye = np.eye(8)
    zero = np.zeros((64, 64))

    def doubled(table):
        high, low = split_table(table)
        top = np.concatenate([high, high], 1)
        return np.concatenate([top, np.concatenate([low, zero.astype(low.dtype)], 1)], 0)

    high, low = split_table(np.concatenate([np.kron(derivative, eye), np.kron(eye, derivative)], 0))
    grad_y = np.concatenate([high, high, low], 1)
    back = (derivative * weights[:, None]).T
    high, low = split_table(np.concatenate([np.kron(back, np.diag(weights)), np.kron(np.diag(weights), back)], 1))
    back_y = np.concatenate([high, high, low], 1)
    many = np.eye(BLOCK // 8)
    grad_z = np.concatenate(split_table(np.kron(many, derivative.T)), 0)
    back_z = np.concatenate(split_table(np.kron(many, derivative)), 0)
    spread = np.kron(np.eye(LANES)[:, : BLOCK // 8], np.ones((1, 8))).astype(jnp.bfloat16)
    weight_z = np.tile(weights, BLOCK // 8)[None].astype(np.float32)
    plane = np.tile(np.kron(weights, weights)[:, None], (1, BLOCK)).astype(np.float32)
    return grad_y, back_y, grad_z, back_z, spread, weight_z, plane


def x_matrices():
    derivative, weights = gll_tables()
    scaled = (derivative * weights[:, None]).T / weights[:, None]
    return derivative, scaled


def split(values):
    high = values.astype(BF16)
    return high, (values - high.astype(F32)).astype(BF16)


def dot(left, right):
    return jnp.dot(left, right, preferred_element_type=F32)


def lane_iota():
    return lax.broadcasted_iota(jnp.int32, (8, LANES), 1)


def along_x(planes, matrix):
    even = [planes[b] + planes[7 - b] for b in range(4)]
    odd = [planes[b] - planes[7 - b] for b in range(4)]
    result = [None] * 8
    for a in range(4):
        first = second = None
        for b in range(4):
            p = float((matrix[a, b] + matrix[a, 7 - b]) / 2)
            q = float((matrix[a, b] - matrix[a, 7 - b]) / 2)
            first = even[b] * p if first is None else first + even[b] * p
            second = odd[b] * q if second is None else second + odd[b] * q
        result[a] = second + first
        result[7 - a] = second - first
    return result


def operator_block(field, factor, gy_ref, by_ref, gz_ref, bz_ref, plane):
    forward, backward = x_matrices()
    count = field.shape[0] // 64
    high, low = split(field)
    grad_z = dot(high, gz_ref[:BLOCK]) + dot(low, gz_ref[:BLOCK]) + dot(high, gz_ref[BLOCK:])
    g = [factor[k : k + 1] for k in range(6)]
    fluxes = []
    along_y = []
    sums = []
    for c in range(count):
        mine = slice(64 * c, 64 * c + 64)
        both = dot(gy_ref[...], jnp.concatenate([high[mine], low[mine], high[mine]], 0))
        gx, gy = both[:64], both[64:]
        gz = grad_z[mine]
        fx = g[0] * gx + g[3] * gy + g[4] * gz
        fy = g[3] * gx + g[1] * gy + g[5] * gz
        fz = g[4] * gx + g[5] * gy + g[2] * gz
        fluxes.append(fz)
        fh, fl = split(jnp.concatenate([fx, fy], 0))
        along_y.append(dot(by_ref[...], jnp.concatenate([fh, fl, fh], 0)))
    fh, fl = split(jnp.concatenate(fluxes, 0))
    back = dot(fh, bz_ref[:BLOCK]) + dot(fl, bz_ref[:BLOCK]) + dot(fh, bz_ref[BLOCK:])
    return [
        along_y[c] + plane * back[64 * c : 64 * c + 64] for c in range(count)
    ]


def spread_rows(rows, spread, weight):
    first = rows.astype(BF16)
    rest = rows - first.astype(F32)
    second = rest.astype(BF16)
    third = (rest - second.astype(F32)).astype(BF16)
    return (dot(first, spread) + dot(second, spread) + dot(third, spread)) * weight


def load_kernel(
    u_hbm, geo_hbm, gy_hbm, by_hbm, gz_hbm, bz_hbm, spread_hbm, wz_hbm, plane_hbm,
    u_ref, factor_ref, gy_ref, by_ref, gz_ref, bz_ref, plane_ref, za_ref, zb_ref,
    geo_ref, spread_ref, wz_ref, sems,
):
    components = u_ref.shape[0]
    length = u_ref.shape[3]
    blocks = length // BLOCK
    per_block = BLOCK // 8
    copies = []
    ends = (pl.ds(0, LANES), pl.ds(length - LANES, LANES))
    middle = pl.ds(LANES, length - 2 * LANES)
    pairs = [(geo_hbm, geo_ref), (spread_hbm, spread_ref), (wz_hbm, wz_ref)]
    pairs += [(u_hbm.at[:, :, :, where], u_ref.at[:, :, :, where]) for where in ends]
    pairs += [(gz_hbm, gz_ref), (gy_hbm, gy_ref), (by_hbm, by_ref), (bz_hbm, bz_ref)]
    pairs += [(plane_hbm, plane_ref)]
    pairs += [(u_hbm.at[c, :, :, middle], u_ref.at[c, :, :, middle]) for c in range(components)]
    for k, (source, target) in enumerate(pairs):
        copies.append(pltpu.make_async_copy(source, target, sems.at[k]))
        copies[-1].start()
    for copy in copies[:3]:
        copy.wait()
    geo = jnp.concatenate(
        [geo_ref[k, 0] for k in range(6)] + [jnp.zeros((2, length // 8), F32)], 0
    )
    rows = []
    for block in range(blocks):
        start = block * per_block
        tile = geo[:, start // LANES * LANES : start // LANES * LANES + LANES]
        shift = start % LANES
        rows.append(pltpu.roll(tile, LANES - shift, 1) if shift else tile)
    expanded = spread_rows(jnp.concatenate(rows, 0), spread_ref[...], wz_ref[...])
    factor_ref[...] = expanded
    for copy in copies[3:10]:
        copy.wait()
    factor = jnp.concatenate([expanded[:8, :LANES], expanded[8 * blocks - 8 :, LANES:]], 1)
    sides = []
    for c in range(components):
        sides.append(jnp.concatenate([u_ref[c, :, :, where].reshape(64, LANES) for where in ends], 1))
    totals = operator_block(
        jnp.concatenate(sides, 0), factor, gy_ref, by_ref, gz_ref, bz_ref, plane_ref[...]
    )
    even_z = lax.rem(lax.axis_index("gz"), 2) == 0
    lane = lane_iota()
    low_plane = jnp.zeros((8, LANES), F32)
    high_plane = jnp.zeros((8, LANES), F32)
    for c in range(components):
        for x in range(8):
            slot = 8 * c + x
            begin = totals[c][8 * x : 8 * x + 8, :LANES]
            end = totals[c][8 * x : 8 * x + 8, LANES:]
            begin = pltpu.roll(begin, slot, 1) if slot else begin
            end = pltpu.roll(end, slot + 1, 1)
            low_plane = jnp.where(lane == slot, begin, low_plane)
            high_plane = jnp.where(lane == slot, end, high_plane)
    za_ref[...] = jnp.where(even_z, high_plane, low_plane)
    zb_ref[...] = jnp.where(even_z, low_plane, high_plane)
    for copy in copies[10:]:
        copy.wait()


def stiffness_kernel(
    u_ref, factor_ref, gy_ref, by_ref, gz_ref, bz_ref, plane_ref, za_ref, zb_ref,
    out_ref, xa_ref, xb_ref, ia_ref, ea_ref, yb_ref,
):
    components = u_ref.shape[0]
    length = u_ref.shape[3]
    blocks = length // BLOCK
    tiles = length // LANES

    def body(block, carry):
        where = pl.ds(pl.multiple_of(block * BLOCK, BLOCK), BLOCK)
        field = jnp.concatenate(
            [u_ref[c, :, :, where].reshape(64, BLOCK) for c in range(components)], 0
        )
        factor = factor_ref[pl.ds(pl.multiple_of(block * 8, 8), 8), :]
        totals = operator_block(field, factor, gy_ref, by_ref, gz_ref, bz_ref, plane_ref[...])
        for c in range(components):
            out_ref[c, :, :, where] = totals[c].reshape(8, 8, BLOCK)
        return carry

    lax.fori_loop(0, blocks, body, 0, unroll=8)

    even_x, even_y, even_z = parities()
    low, high = ordered(even_z, za_ref[...], zb_ref[...])
    position = lax.broadcasted_iota(jnp.int32, (8, length), 1)
    last = (position % 8 == 7) & (position != length - 1)
    initial = (position % 8 == 0) & (position != 0)
    for c in range(components):
        for x in range(8):
            row = out_ref[c, x]
            after = pltpu.roll(row, length - 1, 1)
            before = pltpu.roll(row, 1, 1)
            row = row + jnp.where(last, after, 0.0) + jnp.where(initial, before, 0.0)
            slot = 8 * c + x
            out_ref[c, x] = row
            out_ref[c, x, :, :LANES] = row[:, :LANES] + at_lane(low, slot, 0)
            out_ref[c, x, :, length - LANES :] = row[:, length - LANES :] + at_lane(
                high, slot, LANES - 1
            )

    for c in range(components):
        for t in range(tiles):
            where = slice(t * LANES, t * LANES + LANES)
            spot = c * tiles + t
            first_plane = out_ref[c, 0, :, where]
            last_plane = out_ref[c, 7, :, where]
            xa_ref[spot] = jnp.where(even_x, last_plane, first_plane)
            xb_ref[spot] = jnp.where(even_x, first_plane, last_plane)
            for x in range(8):
                first_row = out_ref[c, x, 0:1, where]
                last_row = out_ref[c, x, 7:8, where]
                row_a = jnp.where(even_y, last_row, first_row)
                yb_ref[spot, x : x + 1] = jnp.where(even_y, first_row, last_row)
                if x in (0, 7):
                    at = 6 * t + 2 * c + x // 7
                    ea_ref[at : at + 1] = row_a
                else:
                    at = 18 * t + 6 * c + x - 1
                    ia_ref[at : at + 1] = row_a


def ordered(even, first, second):
    return jnp.where(even, second, first), jnp.where(even, first, second)


def parities():
    return [lax.rem(lax.axis_index(axis), 2) == 0 for axis in ("gx", "gy", "gz")]


def at_lane(packed, slot, lane_to):
    shift = (lane_to - slot) % LANES
    moved = pltpu.roll(packed, shift, 1) if shift else packed
    return jnp.where(lane_iota() == lane_to, moved, 0.0)


def edge_kernel(ea_ref, yb_ref, xa_ref, xb_ref, outa_ref, outb_ref):
    tiles = ea_ref.shape[0] // 6
    components = xa_ref.shape[0] // tiles
    even_x, even_y, _ = parities()
    for c in range(components):
        for t in range(tiles):
            spot = c * tiles + t
            sides = ordered(even_x, xa_ref[spot], xb_ref[spot])
            outb_ref[spot] = yb_ref[spot]
            for k in range(2):
                at = 6 * t + 2 * c + k
                at = slice(at, at + 1)
                first, last = sides[k][0:1], sides[k][7:8]
                outa_ref[at] = ea_ref[at] + jnp.where(even_y, last, first)
                x = slice(7 * k, 7 * k + 1)
                outb_ref[spot, x] = yb_ref[spot, x] + jnp.where(even_y, first, last)


def final_kernel(
    local_ref, xa_ref, xb_ref, ia_ref, ea_ref, yb_ref, out_hbm, out_ref, sems
):
    components = local_ref.shape[0]
    tiles = local_ref.shape[3] // LANES
    even_x, even_y, _ = parities()
    sublane = lax.broadcasted_iota(jnp.int32, (8, LANES), 0)
    row_a = jnp.where(even_y, 7, 0)
    row_b = 7 - row_a
    is_a, is_b = sublane == row_a, sublane == row_b
    copies = []
    for c in range(components):
        for t in range(tiles):
            where = slice(t * LANES, t * LANES + LANES)
            spot = c * tiles + t
            below, above = ordered(even_x, xa_ref[spot], xb_ref[spot])
            for x in range(8):
                value = local_ref[c, x, :, where]
                if x in (0, 7):
                    value = value + (above if x else below)
                    at = 6 * t + 2 * c + x // 7
                    line = ea_ref[at : at + 1]
                else:
                    at = 18 * t + 6 * c + x - 1
                    line = ia_ref[at : at + 1]
                other = yb_ref[spot, x : x + 1]
                line = jnp.broadcast_to(line, (8, LANES))
                other = jnp.broadcast_to(other, (8, LANES))
                change = jnp.where(is_a, line, jnp.where(is_b, other, 0.0))
                out_ref[c, x, :, where] = value + change
        copies.append(pltpu.make_async_copy(out_ref.at[c], out_hbm.at[c], sems.at[c]))
        copies[-1].start()
    for copy in copies:
        copy.wait()


def pairs_from(start, count):
    found = []
    for i in range(start, count - 1, 2):
        found += [(i, i + 1), (i + 1, i)]
    return found


def exchange(array, axis, start):
    return lax.ppermute(array, axis, pairs_from(start, lax.axis_size(axis)))


def call(kernel, outs, scratch=(), flops=1000000, **specs):
    shapes = [out if hasattr(out, "dtype") else jax.ShapeDtypeStruct(out, F32) for out in outs]
    return pl.pallas_call(
        kernel,
        out_shape=shapes,
        scratch_shapes=list(scratch),
        compiler_params=pltpu.CompilerParams(vmem_limit_bytes=24 * 1024 * 1024),
        cost_estimate=pl.CostEstimate(flops=flops, bytes_accessed=1000000, transcendentals=0),
        **specs,
    )


def local(nodal, geometry):
    components, _, _, length = nodal.shape
    tiles = length // LANES
    blocks = length // BLOCK
    face = (components * tiles, 8, LANES)
    inner = (components * tiles * 6, LANES)
    edge = (components * tiles * 2, LANES)
    tile = (8, LANES)
    constants = [jnp.asarray(table) for table in tables()]
    operands = [
        pltpu.with_memory_space_constraint(operand, pltpu.HBM)
        for operand in [nodal, geometry] + constants
    ]
    hbm = pl.BlockSpec(memory_space=pltpu.HBM)
    kept = [jax.ShapeDtypeStruct(constants[k].shape, constants[k].dtype) for k in (0, 1, 2, 3, 6)]
    loaded = call(
        load_kernel,
        [nodal.shape, (8 * blocks, BLOCK)] + kept + [tile, tile],
        [pltpu.VMEM(operands[k].shape, operands[k].dtype) for k in (1, 6, 7)]
        + [pltpu.SemaphoreType.DMA((10 + components,))],
        in_specs=[hbm] * len(operands),
    )(*operands)
    za = exchange(loaded[-2], "gz", 0)
    zb = exchange(loaded[-1], "gz", 1)
    result, xa, xb, ia, ea, yb = call(
        stiffness_kernel, [nodal.shape, face, face, inner, edge, face]
    )(*loaded[:-2], za, zb)
    xa = exchange(xa, "gx", 0)
    xb = exchange(xb, "gx", 1)
    ia = exchange(ia, "gy", 0)
    ea, yb = call(edge_kernel, [edge, face])(ea, yb, xa, xb)
    yb = exchange(yb, "gy", 1)
    ea = exchange(ea, "gy", 0)
    (result,) = call(
        final_kernel,
        [nodal.shape],
        [pltpu.VMEM(nodal.shape, F32), pltpu.SemaphoreType.DMA((components,))],
        out_specs=[hbm],
    )(result, xa, xb, ia, ea, yb)
    return result


def solution(mesh):
    return jax.shard_map(
        local,
        mesh=mesh,
        in_specs=(P(None, "gx", "gy", "gz"), P(None, "gx", "gy", "gz")),
        out_specs=P(None, "gx", "gy", "gz"),
        check_vma=False,
    )
```

```python
import jax
import jax.numpy as jnp
import numpy as np
from jax import lax
from jax.experimental import pallas as pl
from jax.experimental.pallas import tpu as pltpu
from jax.sharding import PartitionSpec as P


interior_points = [
    -0.8717401485096066,
    -0.5917001814331423,
    -0.2092992179024789,
    0.2092992179024789,
    0.5917001814331423,
    0.8717401485096066,
]
LANES = 128
BLOCK = 256
F32 = jnp.float32
BF16 = jnp.bfloat16


def legendre_seven(point):
    previous = 1.0
    current = point
    for order in range(1, 7):
        following = ((2 * order + 1) * point * current - order * previous) / (order + 1)
        previous = current
        current = following
    return current


def gll_tables():
    degree = 7
    points = [-1.0] + interior_points + [1.0]
    values = [legendre_seven(point) for point in points]
    node_count = degree + 1
    weights = np.array([2.0 / (degree * (degree + 1) * value * value) for value in values])
    derivative = np.zeros((node_count, node_count))
    for row_index in range(node_count):
        for col_index in range(node_count):
            if row_index != col_index:
                derivative[row_index, col_index] = values[row_index] / (
                    values[col_index] * (points[row_index] - points[col_index])
                )
    derivative[0, 0] = -degree * (degree + 1) / 4.0
    derivative[node_count - 1, node_count - 1] = degree * (degree + 1) / 4.0
    return (derivative.astype(np.float32).astype(np.float64), weights)


def split_table(table):
    high = np.asarray(table, np.float32).astype(jnp.bfloat16)
    low = (np.asarray(table, np.float64) - high.astype(np.float64)).astype(jnp.bfloat16)
    return high, low


def tables():
    derivative, weights = gll_tables()
    eye = np.eye(8)

    high, low = split_table(np.concatenate([np.kron(derivative, eye), np.kron(eye, derivative)], 0))
    grad_y = np.concatenate([high, high, low], 1)
    back = (derivative * weights[:, None]).T
    high, low = split_table(np.concatenate([np.kron(back, np.diag(weights)), np.kron(np.diag(weights), back)], 1))
    back_y = np.concatenate([high, high, low], 1)
    many = np.eye(BLOCK // 8)
    grad_z = np.concatenate(split_table(np.kron(many, derivative.T)), 0)
    back_z = np.concatenate(split_table(np.kron(many, derivative)), 0)
    spread = np.kron(np.eye(LANES)[:, : BLOCK // 8], np.ones((1, 8))).astype(jnp.bfloat16)
    weight_z = np.tile(weights, BLOCK // 8)[None].astype(np.float32)
    plane = np.tile(np.kron(weights, weights)[:, None], (1, BLOCK)).astype(np.float32)
    return grad_y, back_y, grad_z, back_z, spread, weight_z, plane


def x_matrices():
    derivative, weights = gll_tables()
    scaled = (derivative * weights[:, None]).T / weights[:, None]
    return derivative, scaled


def split(values):
    high = values.astype(BF16)
    return high, (values - high.astype(F32)).astype(BF16)


def dot(left, right):
    return jnp.dot(left, right, preferred_element_type=F32)


def lane_iota():
    return lax.broadcasted_iota(jnp.int32, (8, LANES), 1)


def operator_block(field, factor, gy_ref, by_ref, gz_ref, bz_ref, plane):
    forward, backward = x_matrices()
    count = field.shape[0] // 64
    high, low = split(field)
    grad_z = dot(high, gz_ref[:BLOCK]) + dot(low, gz_ref[:BLOCK]) + dot(high, gz_ref[BLOCK:])
    g = [factor[k : k + 1] for k in range(6)]
    fluxes = []
    along_y = []
    for c in range(count):
        mine = slice(64 * c, 64 * c + 64)
        both = dot(gy_ref[...], jnp.concatenate([high[mine], low[mine], high[mine]], 0))
        gx, gy = both[:64], both[64:]
        gz = grad_z[mine]
        fx = g[0] * gx + g[3] * gy + g[4] * gz
        fy = g[3] * gx + g[1] * gy + g[5] * gz
        fz = g[4] * gx + g[5] * gy + g[2] * gz
        fluxes.append(fz)
        fh, fl = split(jnp.concatenate([fx, fy], 0))
        along_y.append(dot(by_ref[...], jnp.concatenate([fh, fl, fh], 0)))
    fh, fl = split(jnp.concatenate(fluxes, 0))
    back = dot(fh, bz_ref[:BLOCK]) + dot(fl, bz_ref[:BLOCK]) + dot(fh, bz_ref[BLOCK:])
    return [
        along_y[c] + plane * back[64 * c : 64 * c + 64] for c in range(count)
    ]


def spread_rows(rows, spread, weight):
    first = rows.astype(BF16)
    rest = rows - first.astype(F32)
    second = rest.astype(BF16)
    third = (rest - second.astype(F32)).astype(BF16)
    return (dot(first, spread) + dot(second, spread) + dot(third, spread)) * weight


def load_kernel(
    u_hbm, geo_hbm, gy_hbm, by_hbm, gz_hbm, bz_hbm, spread_hbm, wz_hbm, plane_hbm,
    u_ref, factor_ref, gy_ref, by_ref, gz_ref, bz_ref, plane_ref, za_ref, zb_ref,
    geo_ref, spread_ref, wz_ref, sems,
):
    components = u_ref.shape[0]
    length = u_ref.shape[3]
    blocks = length // BLOCK
    per_block = BLOCK // 8
    copies = []
    ends = (pl.ds(0, LANES), pl.ds(length - LANES, LANES))
    middle = pl.ds(LANES, length - 2 * LANES)
    pairs = [(geo_hbm, geo_ref), (spread_hbm, spread_ref), (wz_hbm, wz_ref)]
    pairs += [(u_hbm.at[:, :, :, where], u_ref.at[:, :, :, where]) for where in ends]
    pairs += [(gz_hbm, gz_ref), (gy_hbm, gy_ref), (by_hbm, by_ref), (bz_hbm, bz_ref)]
    pairs += [(plane_hbm, plane_ref)]
    pairs += [(u_hbm.at[c, :, :, middle], u_ref.at[c, :, :, middle]) for c in range(components)]
    for k, (source, target) in enumerate(pairs):
        copies.append(pltpu.make_async_copy(source, target, sems.at[k]))
        copies[-1].start()
    for copy in copies[:3]:
        copy.wait()
    geo = jnp.concatenate(
        [geo_ref[k, 0] for k in range(6)] + [jnp.zeros((2, length // 8), F32)], 0
    )
    rows = []
    for block in range(blocks):
        start = block * per_block
        tile = geo[:, start // LANES * LANES : start // LANES * LANES + LANES]
        shift = start % LANES
        rows.append(pltpu.roll(tile, LANES - shift, 1) if shift else tile)
    expanded = spread_rows(jnp.concatenate(rows, 0), spread_ref[...], wz_ref[...])
    factor_ref[...] = expanded
    for copy in copies[3:10]:
        copy.wait()
    factor = jnp.concatenate([expanded[:8, :LANES], expanded[8 * blocks - 8 :, LANES:]], 1)
    sides = []
    for c in range(components):
        sides.append(jnp.concatenate([u_ref[c, :, :, where].reshape(64, LANES) for where in ends], 1))
    totals = operator_block(
        jnp.concatenate(sides, 0), factor, gy_ref, by_ref, gz_ref, bz_ref, plane_ref[...]
    )
    even_z = lax.rem(lax.axis_index("gz"), 2) == 0
    lane = lane_iota()
    low_plane = jnp.zeros((8, LANES), F32)
    high_plane = jnp.zeros((8, LANES), F32)
    for c in range(components):
        for x in range(8):
            slot = 8 * c + x
            begin = totals[c][8 * x : 8 * x + 8, :LANES]
            end = totals[c][8 * x : 8 * x + 8, LANES:]
            begin = pltpu.roll(begin, slot, 1) if slot else begin
            end = pltpu.roll(end, slot + 1, 1)
            low_plane = jnp.where(lane == slot, begin, low_plane)
            high_plane = jnp.where(lane == slot, end, high_plane)
    za_ref[...] = jnp.where(even_z, high_plane, low_plane)
    zb_ref[...] = jnp.where(even_z, low_plane, high_plane)
    for copy in copies[10:]:
        copy.wait()


def stiffness_kernel(
    u_ref, factor_ref, gy_ref, by_ref, gz_ref, bz_ref, plane_ref, za_ref, zb_ref,
    out_ref, xa_ref, xb_ref, ia_ref, ea_ref, yb_ref,
):
    components = u_ref.shape[0]
    length = u_ref.shape[3]
    blocks = length // BLOCK
    tiles = length // LANES

    def body(block, carry):
        where = pl.ds(pl.multiple_of(block * BLOCK, BLOCK), BLOCK)
        field = jnp.concatenate(
            [u_ref[c, :, :, where].reshape(64, BLOCK) for c in range(components)], 0
        )
        factor = factor_ref[pl.ds(pl.multiple_of(block * 8, 8), 8), :]
        totals = operator_block(field, factor, gy_ref, by_ref, gz_ref, bz_ref, plane_ref[...])
        for c in range(components):
            out_ref[c, :, :, where] = totals[c].reshape(8, 8, BLOCK)
        return carry

    lax.fori_loop(0, blocks, body, 0, unroll=8)

    even_x, even_y, even_z = parities()
    low, high = ordered(even_z, za_ref[...], zb_ref[...])
    position = lax.broadcasted_iota(jnp.int32, (8, length), 1)
    last = (position % 8 == 7) & (position != length - 1)
    initial = (position % 8 == 0) & (position != 0)
    for c in range(components):
        for x in range(8):
            row = out_ref[c, x]
            after = pltpu.roll(row, length - 1, 1)
            before = pltpu.roll(row, 1, 1)
            row = row + jnp.where(last, after, 0.0) + jnp.where(initial, before, 0.0)
            slot = 8 * c + x
            out_ref[c, x] = row
            out_ref[c, x, :, :LANES] = row[:, :LANES] + at_lane(low, slot, 0)
            out_ref[c, x, :, length - LANES :] = row[:, length - LANES :] + at_lane(
                high, slot, LANES - 1
            )

    for c in range(components):
        for t in range(tiles):
            where = slice(t * LANES, t * LANES + LANES)
            spot = c * tiles + t
            first_plane = out_ref[c, 0, :, where]
            last_plane = out_ref[c, 7, :, where]
            xa_ref[spot] = jnp.where(even_x, last_plane, first_plane)
            xb_ref[spot] = jnp.where(even_x, first_plane, last_plane)
            for x in range(8):
                first_row = out_ref[c, x, 0:1, where]
                last_row = out_ref[c, x, 7:8, where]
                row_a = jnp.where(even_y, last_row, first_row)
                yb_ref[spot, x : x + 1] = jnp.where(even_y, first_row, last_row)
                if x in (0, 7):
                    at = 6 * t + 2 * c + x // 7
                    ea_ref[at : at + 1] = row_a
                else:
                    at = 18 * t + 6 * c + x - 1
                    ia_ref[at : at + 1] = row_a


def ordered(even, first, second):
    return jnp.where(even, second, first), jnp.where(even, first, second)


def parities():
    x, y, z = [lax.axis_index(axis) for axis in ("gx", "gy", "gz")]
    return [lax.rem(index, 2) == 0 for index in (x + z, y + z, z)]


def at_lane(packed, slot, lane_to):
    shift = (lane_to - slot) % LANES
    moved = pltpu.roll(packed, shift, 1) if shift else packed
    return jnp.where(lane_iota() == lane_to, moved, 0.0)


def copy_kernel(in_ref, out_ref):
    out_ref[...] = in_ref[...]


def edge_kernel(ea_ref, yb_ref, xa_ref, xb_ref, outa_ref, outb_ref):
    tiles = ea_ref.shape[0] // 6
    components = xa_ref.shape[0] // tiles
    even_x, even_y, _ = parities()
    for c in range(components):
        for t in range(tiles):
            spot = c * tiles + t
            sides = ordered(even_x, xa_ref[spot], xb_ref[spot])
            outb_ref[spot] = yb_ref[spot]
            for k in range(2):
                at = 6 * t + 2 * c + k
                at = slice(at, at + 1)
                first, last = sides[k][0:1], sides[k][7:8]
                outa_ref[at] = ea_ref[at] + jnp.where(even_y, last, first)
                x = slice(7 * k, 7 * k + 1)
                outb_ref[spot, x] = yb_ref[spot, x] + jnp.where(even_y, first, last)


def final_kernel(
    local_ref, xa_ref, xb_ref, ia_ref, ea_ref, yb_ref, out_hbm, out_ref, sems
):
    components = local_ref.shape[0]
    tiles = local_ref.shape[3] // LANES
    even_x, even_y, _ = parities()
    sublane = lax.broadcasted_iota(jnp.int32, (8, LANES), 0)
    row_a = jnp.where(even_y, 7, 0)
    row_b = 7 - row_a
    is_a, is_b = sublane == row_a, sublane == row_b
    copies = []
    for c in range(components):
        for t in range(tiles):
            where = slice(t * LANES, t * LANES + LANES)
            spot = c * tiles + t
            below, above = ordered(even_x, xa_ref[spot], xb_ref[spot])
            for x in range(8):
                value = local_ref[c, x, :, where]
                if x in (0, 7):
                    value = value + (above if x else below)
                    at = 6 * t + 2 * c + x // 7
                    line = ea_ref[at : at + 1]
                else:
                    at = 18 * t + 6 * c + x - 1
                    line = ia_ref[at : at + 1]
                other = yb_ref[spot, x : x + 1]
                line = jnp.broadcast_to(line, (8, LANES))
                other = jnp.broadcast_to(other, (8, LANES))
                change = jnp.where(is_a, line, jnp.where(is_b, other, 0.0))
                out_ref[c, x, :, where] = value + change
        copies.append(pltpu.make_async_copy(out_ref.at[c], out_hbm.at[c], sems.at[c]))
        copies[-1].start()
    for copy in copies:
        copy.wait()


def pairs_from(start, count):
    found = []
    for i in range(start, count - 1, 2):
        found += [(i, i + 1), (i + 1, i)]
    return found


def exchange(array, axis, start):
    return lax.ppermute(array, axis, pairs_from(start, lax.axis_size(axis)))


def mixed_exchange(array, axis, side):
    depth = lax.axis_size("gz")
    found = []
    for z in range(depth):
        for i, j in pairs_from((side + z) % 2, lax.axis_size(axis)):
            found.append((i * depth + z, j * depth + z))
    return lax.ppermute(array, (axis, "gz"), found)


def call(kernel, outs, scratch=(), flops=1000000, **specs):
    shapes = [out if hasattr(out, "dtype") else jax.ShapeDtypeStruct(out, F32) for out in outs]
    return pl.pallas_call(
        kernel,
        out_shape=shapes,
        scratch_shapes=list(scratch),
        compiler_params=pltpu.CompilerParams(vmem_limit_bytes=24 * 1024 * 1024),
        cost_estimate=pl.CostEstimate(flops=flops, bytes_accessed=1000000, transcendentals=0),
        **specs,
    )


def local(nodal, geometry):
    components, _, _, length = nodal.shape
    tiles = length // LANES
    blocks = length // BLOCK
    face = (components * tiles, 8, LANES)
    inner = (components * tiles * 6, LANES)
    edge = (components * tiles * 2, LANES)
    tile = (8, LANES)
    constants = [jnp.asarray(table) for table in tables()]
    operands = [
        pltpu.with_memory_space_constraint(operand, pltpu.HBM)
        for operand in [nodal, geometry] + constants
    ]
    hbm = pl.BlockSpec(memory_space=pltpu.HBM)
    kept = [jax.ShapeDtypeStruct(constants[k].shape, constants[k].dtype) for k in (0, 1, 2, 3, 6)]
    loaded = call(
        load_kernel,
        [nodal.shape, (8 * blocks, BLOCK)] + kept + [tile, tile],
        [pltpu.VMEM(operands[k].shape, operands[k].dtype) for k in (1, 6, 7)]
        + [pltpu.SemaphoreType.DMA((10 + components,))],
        in_specs=[hbm] * len(operands),
    )(*operands)
    za = exchange(loaded[-2], "gz", 0)
    zb = exchange(loaded[-1], "gz", 1)
    result, xa, xb, ia, ea, yb = call(
        stiffness_kernel, [nodal.shape, face, face, inner, edge, face]
    )(*loaded[:-2], za, zb)
    xa = mixed_exchange(xa, "gx", 0)
    xb = mixed_exchange(xb, "gx", 1)
    ia = mixed_exchange(ia, "gy", 0)
    (ea,) = call(copy_kernel, [edge])(ea)
    ea, yb = call(edge_kernel, [edge, face])(ea, yb, xa, xb)
    yb = mixed_exchange(yb, "gy", 1)
    ea = mixed_exchange(ea, "gy", 0)
    (result,) = call(
        final_kernel,
        [nodal.shape],
        [pltpu.VMEM(nodal.shape, F32), pltpu.SemaphoreType.DMA((components,))],
        out_specs=[hbm],
    )(result, xa, xb, ia, ea, yb)
    return result


def solution(mesh):
    return jax.shard_map(
        local,
        mesh=mesh,
        in_specs=(P(None, "gx", "gy", "gz"), P(None, "gx", "gy", "gz")),
        out_specs=P(None, "gx", "gy", "gz"),
        check_vma=False,
    )
```

```python
import jax
import jax.numpy as jnp
import numpy as np
from jax import lax
from jax.experimental import pallas as pl
from jax.experimental.pallas import tpu as pltpu
from jax.sharding import PartitionSpec as P


interior_points = [
    -0.8717401485096066,
    -0.5917001814331423,
    -0.2092992179024789,
    0.2092992179024789,
    0.5917001814331423,
    0.8717401485096066,
]
LANES = 128
BLOCK = 256
F32 = jnp.float32
BF16 = jnp.bfloat16


def legendre_seven(point):
    previous = 1.0
    current = point
    for order in range(1, 7):
        following = ((2 * order + 1) * point * current - order * previous) / (order + 1)
        previous = current
        current = following
    return current


def gll_tables():
    degree = 7
    points = [-1.0] + interior_points + [1.0]
    values = [legendre_seven(point) for point in points]
    node_count = degree + 1
    weights = np.array([2.0 / (degree * (degree + 1) * value * value) for value in values])
    derivative = np.zeros((node_count, node_count))
    for row_index in range(node_count):
        for col_index in range(node_count):
            if row_index != col_index:
                derivative[row_index, col_index] = values[row_index] / (
                    values[col_index] * (points[row_index] - points[col_index])
                )
    derivative[0, 0] = -degree * (degree + 1) / 4.0
    derivative[node_count - 1, node_count - 1] = degree * (degree + 1) / 4.0
    return (derivative.astype(np.float32).astype(np.float64), weights)


def split_table(table):
    high = np.asarray(table, np.float32).astype(jnp.bfloat16)
    low = (np.asarray(table, np.float64) - high.astype(np.float64)).astype(jnp.bfloat16)
    return high, low


def tables():
    derivative, weights = gll_tables()
    eye = np.eye(8)

    high, low = split_table(np.concatenate([np.kron(derivative, eye), np.kron(eye, derivative)], 0))
    grad_y = np.concatenate([high, high, low], 1)
    back = (derivative * weights[:, None]).T
    high, low = split_table(np.concatenate([np.kron(back, np.diag(weights)), np.kron(np.diag(weights), back)], 1))
    back_y = np.concatenate([high, high, low], 1)
    many = np.eye(BLOCK // 8)
    grad_z = np.concatenate(split_table(np.kron(many, derivative.T)), 0)
    back_z = np.concatenate(split_table(np.kron(many, derivative)), 0)
    spread = np.kron(np.eye(LANES)[:, : BLOCK // 8], np.ones((1, 8))).astype(jnp.bfloat16)
    weight_z = np.tile(weights, BLOCK // 8)[None].astype(np.float32)
    plane = np.tile(np.kron(weights, weights)[:, None], (1, BLOCK)).astype(np.float32)
    return grad_y, back_y, grad_z, back_z, spread, weight_z, plane


def x_matrices():
    derivative, weights = gll_tables()
    scaled = (derivative * weights[:, None]).T / weights[:, None]
    return derivative, scaled


def split(values):
    high = values.astype(BF16)
    return high, (values - high.astype(F32)).astype(BF16)


def dot(left, right):
    return jnp.dot(left, right, preferred_element_type=F32)


def lane_iota():
    return lax.broadcasted_iota(jnp.int32, (8, LANES), 1)


def operator_block(field, factor, gy_ref, by_ref, gz_ref, bz_ref, plane):
    forward, backward = x_matrices()
    count = field.shape[0] // 64
    high, low = split(field)
    grad_z = dot(high, gz_ref[:BLOCK]) + dot(low, gz_ref[:BLOCK]) + dot(high, gz_ref[BLOCK:])
    g = [factor[k : k + 1] for k in range(6)]
    fluxes = []
    along_y = []
    for c in range(count):
        mine = slice(64 * c, 64 * c + 64)
        both = dot(gy_ref[...], jnp.concatenate([high[mine], low[mine], high[mine]], 0))
        gx, gy = both[:64], both[64:]
        gz = grad_z[mine]
        fx = g[0] * gx + g[3] * gy + g[4] * gz
        fy = g[3] * gx + g[1] * gy + g[5] * gz
        fz = g[4] * gx + g[5] * gy + g[2] * gz
        fluxes.append(fz)
        fh, fl = split(jnp.concatenate([fx, fy], 0))
        along_y.append(dot(by_ref[...], jnp.concatenate([fh, fl, fh], 0)))
    fh, fl = split(jnp.concatenate(fluxes, 0))
    back = dot(fh, bz_ref[:BLOCK]) + dot(fl, bz_ref[:BLOCK]) + dot(fh, bz_ref[BLOCK:])
    return [
        along_y[c] + plane * back[64 * c : 64 * c + 64] for c in range(count)
    ]


def spread_rows(rows, spread, weight):
    first = rows.astype(BF16)
    rest = rows - first.astype(F32)
    second = rest.astype(BF16)
    third = (rest - second.astype(F32)).astype(BF16)
    return (dot(first, spread) + dot(second, spread) + dot(third, spread)) * weight


def load_kernel(
    u_hbm, geo_hbm, gy_hbm, by_hbm, gz_hbm, bz_hbm, spread_hbm, wz_hbm, plane_hbm,
    u_ref, factor_ref, gy_ref, by_ref, gz_ref, bz_ref, plane_ref, za_ref, zb_ref,
    geo_ref, spread_ref, wz_ref, sems,
):
    components = u_ref.shape[0]
    length = u_ref.shape[3]
    blocks = length // BLOCK
    per_block = BLOCK // 8
    copies = []
    ends = (pl.ds(0, LANES), pl.ds(length - LANES, LANES))
    middle = pl.ds(LANES, length - 2 * LANES)
    pairs = [(geo_hbm, geo_ref), (spread_hbm, spread_ref), (wz_hbm, wz_ref)]
    pairs += [(u_hbm.at[:, :, :, where], u_ref.at[:, :, :, where]) for where in ends]
    pairs += [(gz_hbm, gz_ref), (gy_hbm, gy_ref), (by_hbm, by_ref), (bz_hbm, bz_ref)]
    pairs += [(plane_hbm, plane_ref)]
    pairs += [(u_hbm.at[c, :, :, middle], u_ref.at[c, :, :, middle]) for c in range(components)]
    for k, (source, target) in enumerate(pairs):
        copies.append(pltpu.make_async_copy(source, target, sems.at[k]))
        copies[-1].start()
    for copy in copies[:3]:
        copy.wait()
    geo = jnp.concatenate(
        [geo_ref[k, 0] for k in range(6)] + [jnp.zeros((2, length // 8), F32)], 0
    )
    rows = []
    for block in range(blocks):
        start = block * per_block
        tile = geo[:, start // LANES * LANES : start // LANES * LANES + LANES]
        shift = start % LANES
        rows.append(pltpu.roll(tile, LANES - shift, 1) if shift else tile)
    expanded = spread_rows(jnp.concatenate(rows, 0), spread_ref[...], wz_ref[...])
    factor_ref[...] = expanded
    for copy in copies[3:10]:
        copy.wait()
    factor = jnp.concatenate([expanded[:8, :LANES], expanded[8 * blocks - 8 :, LANES:]], 1)
    sides = []
    for c in range(components):
        sides.append(jnp.concatenate([u_ref[c, :, :, where].reshape(64, LANES) for where in ends], 1))
    totals = operator_block(
        jnp.concatenate(sides, 0), factor, gy_ref, by_ref, gz_ref, bz_ref, plane_ref[...]
    )
    even_z = lax.rem(lax.axis_index("gz"), 2) == 0
    lane = lane_iota()
    low_plane = jnp.zeros((8, LANES), F32)
    high_plane = jnp.zeros((8, LANES), F32)
    for c in range(components):
        for x in range(8):
            slot = 8 * c + x
            begin = totals[c][8 * x : 8 * x + 8, :LANES]
            end = totals[c][8 * x : 8 * x + 8, LANES:]
            begin = pltpu.roll(begin, slot, 1) if slot else begin
            end = pltpu.roll(end, slot + 1, 1)
            low_plane = jnp.where(lane == slot, begin, low_plane)
            high_plane = jnp.where(lane == slot, end, high_plane)
    za_ref[...] = jnp.where(even_z, high_plane, low_plane)
    zb_ref[...] = jnp.where(even_z, low_plane, high_plane)
    for copy in copies[10:]:
        copy.wait()


def stiffness_kernel(
    u_ref, factor_ref, gy_ref, by_ref, gz_ref, bz_ref, plane_ref, out_ref
):
    components = u_ref.shape[0]
    blocks = u_ref.shape[3] // BLOCK

    def body(block, carry):
        where = pl.ds(pl.multiple_of(block * BLOCK, BLOCK), BLOCK)
        field = jnp.concatenate(
            [u_ref[c, :, :, where].reshape(64, BLOCK) for c in range(components)], 0
        )
        factor = factor_ref[pl.ds(pl.multiple_of(block * 8, 8), 8), :]
        totals = operator_block(field, factor, gy_ref, by_ref, gz_ref, bz_ref, plane_ref[...])
        for c in range(components):
            out_ref[c, :, :, where] = totals[c].reshape(8, 8, BLOCK)
        return carry

    lax.fori_loop(0, blocks, body, 0, unroll=8)


def face_kernel(
    in_ref, za_ref, zb_ref, out_ref, xa_ref, xb_ref, ia_ref, ea_ref, yb_ref
):
    components = in_ref.shape[0]
    length = in_ref.shape[3]
    tiles = length // LANES
    even_x, even_y, even_z = parities()
    low, high = ordered(even_z, za_ref[...], zb_ref[...])
    position = lax.broadcasted_iota(jnp.int32, (8, length), 1)
    last = (position % 8 == 7) & (position != length - 1)
    initial = (position % 8 == 0) & (position != 0)
    for c in range(components):
        for x in range(8):
            row = in_ref[c, x]
            after = pltpu.roll(row, length - 1, 1)
            before = pltpu.roll(row, 1, 1)
            row = row + jnp.where(last, after, 0.0) + jnp.where(initial, before, 0.0)
            slot = 8 * c + x
            out_ref[c, x] = row
            out_ref[c, x, :, :LANES] = row[:, :LANES] + at_lane(low, slot, 0)
            out_ref[c, x, :, length - LANES :] = row[:, length - LANES :] + at_lane(
                high, slot, LANES - 1
            )

    for c in range(components):
        for t in range(tiles):
            where = slice(t * LANES, t * LANES + LANES)
            spot = c * tiles + t
            first_plane = out_ref[c, 0, :, where]
            last_plane = out_ref[c, 7, :, where]
            xa_ref[spot] = jnp.where(even_x, last_plane, first_plane)
            xb_ref[spot] = jnp.where(even_x, first_plane, last_plane)
            for x in range(8):
                first_row = out_ref[c, x, 0:1, where]
                last_row = out_ref[c, x, 7:8, where]
                row_a = jnp.where(even_y, last_row, first_row)
                yb_ref[spot, x : x + 1] = jnp.where(even_y, first_row, last_row)
                if x in (0, 7):
                    at = 6 * t + 2 * c + x // 7
                    ea_ref[at : at + 1] = row_a
                else:
                    at = 18 * t + 6 * c + x - 1
                    ia_ref[at : at + 1] = row_a


def ordered(even, first, second):
    return jnp.where(even, second, first), jnp.where(even, first, second)


def parities():
    x, y, z = [lax.axis_index(axis) for axis in ("gx", "gy", "gz")]
    return [lax.rem(index, 2) == 0 for index in (x + y + z, y, z)]


def at_lane(packed, slot, lane_to):
    shift = (lane_to - slot) % LANES
    moved = pltpu.roll(packed, shift, 1) if shift else packed
    return jnp.where(lane_iota() == lane_to, moved, 0.0)


def copy_kernel(in_ref, out_ref):
    out_ref[...] = in_ref[...]


def edge_kernel(ea_ref, yb_ref, xa_ref, xb_ref, outa_ref, outb_ref):
    tiles = ea_ref.shape[0] // 6
    components = xa_ref.shape[0] // tiles
    even_x, even_y, _ = parities()
    for c in range(components):
        for t in range(tiles):
            spot = c * tiles + t
            sides = ordered(even_x, xa_ref[spot], xb_ref[spot])
            outb_ref[spot] = yb_ref[spot]
            for k in range(2):
                at = 6 * t + 2 * c + k
                at = slice(at, at + 1)
                first, last = sides[k][0:1], sides[k][7:8]
                outa_ref[at] = ea_ref[at] + jnp.where(even_y, last, first)
                x = slice(7 * k, 7 * k + 1)
                outb_ref[spot, x] = yb_ref[spot, x] + jnp.where(even_y, first, last)


def final_kernel(
    local_ref, xa_ref, xb_ref, ia_ref, ea_ref, yb_ref, out_hbm, out_ref, sems
):
    components = local_ref.shape[0]
    tiles = local_ref.shape[3] // LANES
    even_x, even_y, _ = parities()
    sublane = lax.broadcasted_iota(jnp.int32, (8, LANES), 0)
    row_a = jnp.where(even_y, 7, 0)
    row_b = 7 - row_a
    is_a, is_b = sublane == row_a, sublane == row_b
    copies = []
    for c in range(components):
        for t in range(tiles):
            where = slice(t * LANES, t * LANES + LANES)
            spot = c * tiles + t
            below, above = ordered(even_x, xa_ref[spot], xb_ref[spot])
            for x in range(8):
                value = local_ref[c, x, :, where]
                if x in (0, 7):
                    value = value + (above if x else below)
                    at = 6 * t + 2 * c + x // 7
                    line = ea_ref[at : at + 1]
                else:
                    at = 18 * t + 6 * c + x - 1
                    line = ia_ref[at : at + 1]
                other = yb_ref[spot, x : x + 1]
                line = jnp.broadcast_to(line, (8, LANES))
                other = jnp.broadcast_to(other, (8, LANES))
                change = jnp.where(is_a, line, jnp.where(is_b, other, 0.0))
                out_ref[c, x, :, where] = value + change
        copies.append(pltpu.make_async_copy(out_ref.at[c], out_hbm.at[c], sems.at[c]))
        copies[-1].start()
    for copy in copies:
        copy.wait()


def pairs_from(start, count):
    found = []
    for i in range(start, count - 1, 2):
        found += [(i, i + 1), (i + 1, i)]
    return found


def exchange(array, axis, start):
    return lax.ppermute(array, axis, pairs_from(start, lax.axis_size(axis)))


def mixed_exchange(array, side):
    width, height, depth = [lax.axis_size(axis) for axis in ("gx", "gy", "gz")]
    found = []
    for y in range(height):
        for z in range(depth):
            for i, j in pairs_from((side + y + z) % 2, width):
                found.append(((i * height + y) * depth + z, (j * height + y) * depth + z))
    return lax.ppermute(array, ("gx", "gy", "gz"), found)


def call(kernel, outs, scratch=(), flops=1000000, **specs):
    shapes = [out if hasattr(out, "dtype") else jax.ShapeDtypeStruct(out, F32) for out in outs]
    return pl.pallas_call(
        kernel,
        out_shape=shapes,
        scratch_shapes=list(scratch),
        compiler_params=pltpu.CompilerParams(vmem_limit_bytes=24 * 1024 * 1024),
        cost_estimate=pl.CostEstimate(flops=flops, bytes_accessed=1000000, transcendentals=0),
        **specs,
    )


def local(nodal, geometry):
    components, _, _, length = nodal.shape
    tiles = length // LANES
    blocks = length // BLOCK
    face = (components * tiles, 8, LANES)
    inner = (components * tiles * 6, LANES)
    edge = (components * tiles * 2, LANES)
    tile = (8, LANES)
    constants = [jnp.asarray(table) for table in tables()]
    operands = [
        pltpu.with_memory_space_constraint(operand, pltpu.HBM)
        for operand in [nodal, geometry] + constants
    ]
    hbm = pl.BlockSpec(memory_space=pltpu.HBM)
    kept = [jax.ShapeDtypeStruct(constants[k].shape, constants[k].dtype) for k in (0, 1, 2, 3, 6)]
    loaded = call(
        load_kernel,
        [nodal.shape, (8 * blocks, BLOCK)] + kept + [tile, tile],
        [pltpu.VMEM(operands[k].shape, operands[k].dtype) for k in (1, 6, 7)]
        + [pltpu.SemaphoreType.DMA((10 + components,))],
        in_specs=[hbm] * len(operands),
    )(*operands)
    za = exchange(loaded[-2], "gz", 0)
    zb = exchange(loaded[-1], "gz", 1)
    (result,) = call(stiffness_kernel, [nodal.shape])(*loaded[:-2])
    result, xa, xb, ia, ea, yb = call(
        face_kernel, [nodal.shape, face, face, inner, edge, face]
    )(result, za, zb)
    xa = mixed_exchange(xa, 0)
    xb = mixed_exchange(xb, 1)
    ia = exchange(ia, "gy", 0)
    (ea,) = call(copy_kernel, [edge])(ea)
    ea, yb = call(edge_kernel, [edge, face])(ea, yb, xa, xb)
    yb = exchange(yb, "gy", 1)
    ea = exchange(ea, "gy", 0)
    (result,) = call(
        final_kernel,
        [nodal.shape],
        [pltpu.VMEM(nodal.shape, F32), pltpu.SemaphoreType.DMA((components,))],
        out_specs=[hbm],
    )(result, xa, xb, ia, ea, yb)
    return result


def solution(mesh):
    return jax.shard_map(
        local,
        mesh=mesh,
        in_specs=(P(None, "gx", "gy", "gz"), P(None, "gx", "gy", "gz")),
        out_specs=P(None, "gx", "gy", "gz"),
        check_vma=False,
    )
```

```python
import jax
import jax.numpy as jnp
import numpy as np
from jax import lax
from jax.experimental import pallas as pl
from jax.experimental.pallas import tpu as pltpu
from jax.sharding import PartitionSpec as P


interior_points = [
    -0.8717401485096066,
    -0.5917001814331423,
    -0.2092992179024789,
    0.2092992179024789,
    0.5917001814331423,
    0.8717401485096066,
]
LANES = 128
COMPONENTS = 3
BLOCK = 256
F32 = jnp.float32
BF16 = jnp.bfloat16


def legendre_seven(point):
    previous = 1.0
    current = point
    for order in range(1, 7):
        following = ((2 * order + 1) * point * current - order * previous) / (order + 1)
        previous = current
        current = following
    return current


def gll_tables():
    degree = 7
    points = [-1.0] + interior_points + [1.0]
    values = [legendre_seven(point) for point in points]
    node_count = degree + 1
    weights = np.array([2.0 / (degree * (degree + 1) * value * value) for value in values])
    derivative = np.zeros((node_count, node_count))
    for row_index in range(node_count):
        for col_index in range(node_count):
            if row_index != col_index:
                derivative[row_index, col_index] = values[row_index] / (
                    values[col_index] * (points[row_index] - points[col_index])
                )
    derivative[0, 0] = -degree * (degree + 1) / 4.0
    derivative[node_count - 1, node_count - 1] = degree * (degree + 1) / 4.0
    return (derivative.astype(np.float32).astype(np.float64), weights)


def split_table(table):
    high = np.asarray(table, np.float32).astype(jnp.bfloat16)
    low = (np.asarray(table, np.float64) - high.astype(np.float64)).astype(jnp.bfloat16)
    return high, low


def tables():
    derivative, weights = gll_tables()
    eye = np.eye(8)

    def doubled(table):
        high, low = split_table(table)
        top = np.concatenate([high, high], 1)
        return np.concatenate([top, np.concatenate([low, np.zeros_like(low)], 1)], 0)

    high, low = split_table(np.concatenate([np.kron(derivative, eye), np.kron(eye, derivative)], 0))
    grad_y = np.concatenate([high, high, low], 1)
    back = (derivative * weights[:, None]).T
    both = np.concatenate([np.kron(back, np.diag(weights)), np.kron(np.diag(weights), back)], 1)
    back_y = doubled(both)
    many = np.eye(LANES // 8)

    def stacked(table):
        high, low = split_table(table)
        bottom = np.concatenate([high, np.zeros_like(low)], 1)
        return np.concatenate([np.concatenate([high, low], 1), bottom], 0)

    grad_z = stacked(np.kron(many, derivative.T))
    back_z = stacked(np.kron(many, derivative))
    spread = np.kron(np.eye(LANES)[:, : BLOCK // 8], np.ones((1, 8))).astype(jnp.bfloat16)
    weight_z = np.tile(weights, BLOCK // 8)[None].astype(np.float32)
    plane = np.tile(np.kron(weights, weights)[:, None], (1, BLOCK)).astype(np.float32)
    return grad_y, back_y, grad_z, back_z, spread, weight_z, plane


def split(values):
    high = values.astype(BF16)
    return high, (values - high.astype(F32)).astype(BF16)


def dot(left, right):
    return jnp.dot(left, right, preferred_element_type=F32)


def lane_iota():
    return lax.broadcasted_iota(jnp.int32, (8, LANES), 1)


def along_z(high, low, table):
    rows = high.shape[0]
    halves = []
    for k in range(BLOCK // LANES):
        lanes = slice(k * LANES, k * LANES + LANES)
        halves.append(jnp.concatenate([high[:, lanes], low[:, lanes]], 1))
    both = dot(jnp.concatenate(halves, 0), table)
    both = both[:, :LANES] + both[:, LANES:]
    return jnp.concatenate([both[:rows], both[rows:]], 1)


def operator_block(field, factor, gxy_ref, bxy_ref, gz_ref, bz_ref, plane):
    count = field.shape[0] // 64
    high, low = split(field)
    grad_z = along_z(high, low, gz_ref[...])
    g = [factor[k : k + 1] for k in range(6)]
    fluxes = []
    sums = []
    for c in range(count):
        mine = slice(64 * c, 64 * c + 64)
        both = dot(gxy_ref[...], jnp.concatenate([high[mine], low[mine], high[mine]], 0))
        gx, gy = both[:64], both[64:]
        gz = grad_z[mine]
        fx = g[0] * gx + g[3] * gy + g[4] * gz
        fy = g[3] * gx + g[1] * gy + g[5] * gz
        fz = g[4] * gx + g[5] * gy + g[2] * gz
        fluxes.append(fz)
        fh, fl = split(jnp.concatenate([fx, fy], 0))
        both = dot(bxy_ref[...], jnp.concatenate([fh, fl], 0))
        sums.append(both[:64] + both[64:])
    fh, fl = split(jnp.concatenate(fluxes, 0))
    back = along_z(fh, fl, bz_ref[...])
    return [sums[c] + plane * back[64 * c : 64 * c + 64] for c in range(count)]


def spread_rows(rows, spread, weight):
    first = rows.astype(BF16)
    rest = rows - first.astype(F32)
    second = rest.astype(BF16)
    third = (rest - second.astype(F32)).astype(BF16)
    return (dot(first, spread) + dot(second, spread) + dot(third, spread)) * weight


def load_kernel(
    u_hbm, geo_hbm, gy_hbm, by_hbm, gz_hbm, bz_hbm, spread_hbm, wz_hbm, plane_hbm,
    u_ref, factor_ref, gy_ref, by_ref, gz_ref, bz_ref, plane_ref, za_ref, zb_ref,
    geo_ref, spread_ref, wz_ref, sems,
):
    components = u_ref.shape[0]
    length = u_ref.shape[3]
    blocks = length // BLOCK
    per_block = BLOCK // 8
    copies = []
    ends = (pl.ds(0, LANES), pl.ds(length - LANES, LANES))
    middle = pl.ds(LANES, length - 2 * LANES)
    pairs = [(geo_hbm, geo_ref), (spread_hbm, spread_ref), (wz_hbm, wz_ref)]
    pairs += [(u_hbm.at[:, :, :, where], u_ref.at[:, :, :, where]) for where in ends]
    pairs += [(gz_hbm, gz_ref), (gy_hbm, gy_ref), (by_hbm, by_ref), (bz_hbm, bz_ref)]
    pairs += [(plane_hbm, plane_ref)]
    pairs += [(u_hbm.at[c, :, :, middle], u_ref.at[c, :, :, middle]) for c in range(components)]
    for k, (source, target) in enumerate(pairs):
        copies.append(pltpu.make_async_copy(source, target, sems.at[k]))
        copies[-1].start()
    for copy in copies[:3]:
        copy.wait()
    geo = jnp.concatenate(
        [geo_ref[k, 0] for k in range(6)] + [jnp.zeros((2, length // 8), F32)], 0
    )
    rows = []
    for block in range(blocks):
        start = block * per_block
        tile = geo[:, start // LANES * LANES : start // LANES * LANES + LANES]
        shift = start % LANES
        rows.append(pltpu.roll(tile, LANES - shift, 1) if shift else tile)
    expanded = spread_rows(jnp.concatenate(rows, 0), spread_ref[...], wz_ref[...])
    factor_ref[...] = expanded
    for copy in copies[3:10]:
        copy.wait()
    factor = jnp.concatenate([expanded[:8, :LANES], expanded[8 * blocks - 8 :, LANES:]], 1)
    sides = []
    for c in range(components):
        sides.append(jnp.concatenate([u_ref[c, :, :, where].reshape(64, LANES) for where in ends], 1))
    totals = operator_block(
        jnp.concatenate(sides, 0), factor, gy_ref, by_ref, gz_ref, bz_ref, plane_ref[...]
    )
    even_z = lax.rem(lax.axis_index("gz"), 2) == 0
    lane = lane_iota()
    low_plane = jnp.zeros((8, LANES), F32)
    high_plane = jnp.zeros((8, LANES), F32)
    for c in range(components):
        for x in range(8):
            slot = 8 * c + x
            begin = totals[c][8 * x : 8 * x + 8, :LANES]
            end = totals[c][8 * x : 8 * x + 8, LANES:]
            begin = pltpu.roll(begin, slot, 1) if slot else begin
            end = pltpu.roll(end, slot + 1, 1)
            low_plane = jnp.where(lane == slot, begin, low_plane)
            high_plane = jnp.where(lane == slot, end, high_plane)
    za_ref[...] = jnp.where(even_z, high_plane, low_plane)
    zb_ref[...] = jnp.where(even_z, low_plane, high_plane)
    for copy in copies[10:]:
        copy.wait()


def stiffness_kernel(
    u_ref, factor_ref, gy_ref, by_ref, gz_ref, bz_ref, plane_ref, out_ref
):
    components = u_ref.shape[0]
    blocks = u_ref.shape[3] // BLOCK
    tiles = blocks * (BLOCK // LANES)
    lane = lax.broadcasted_iota(jnp.int32, (64, LANES), 1)
    last, initial = lane % 8 == 7, lane % 8 == 0
    final_lane, first_lane = lane == LANES - 1, lane == 0
    zero = jnp.zeros((64, LANES), F32)
    plane = plane_ref[...]
    pending = [None] * components
    edge = [zero] * components

    def finish(c, tile, following):
        value, after, before, previous = pending[c]
        after = jnp.where(final_lane, following, after)
        before = jnp.where(first_lane, previous, before)
        change = jnp.where(last, after, jnp.where(initial, before, 0.0))
        out_ref[c * tiles + tile] = value + change

    for block in range(blocks):
        where = slice(block * BLOCK, block * BLOCK + BLOCK)
        field = jnp.concatenate(
            [u_ref[c, :, :, where].reshape(64, BLOCK) for c in range(components)], 0
        )
        factor = factor_ref[8 * block : 8 * block + 8, :]
        totals = operator_block(field, factor, gy_ref, by_ref, gz_ref, bz_ref, plane)
        for c in range(components):
            for k in range(BLOCK // LANES):
                value = totals[c][:, k * LANES : k * LANES + LANES]
                after = pltpu.roll(value, LANES - 1, 1)
                before = pltpu.roll(value, 1, 1)
                tile = block * (BLOCK // LANES) + k
                if tile:
                    finish(c, tile - 1, after)
                pending[c] = (value, after, before, edge[c])
                edge[c] = before
    for c in range(components):
        finish(c, tiles - 1, zero)


def ordered(even, first, second):
    return jnp.where(even, second, first), jnp.where(even, first, second)


def parities():
    x, y, z = [lax.axis_index(axis) for axis in ("gx", "gy", "gz")]
    return [lax.rem(index, 2) == 0 for index in (x + y + z, y, z)]


def at_lane(packed, slot, lane_to):
    shift = (lane_to - slot) % LANES
    moved = pltpu.roll(packed, shift, 1) if shift else packed
    return jnp.where(lane_iota() == lane_to, moved, 0.0)


def face_kernel(
    local_ref, za_ref, zb_ref, xa_ref, xb_ref, ia_ref, ea_ref, yb_ref, ends_ref
):
    tiles = local_ref.shape[0] // COMPONENTS
    even_x, even_y, even_z = parities()
    low, high = ordered(even_z, za_ref[...], zb_ref[...])
    for c in range(COMPONENTS):
        for k, (t, packed, lane_to) in enumerate(((0, low, 0), (tiles - 1, high, LANES - 1))):
            for x in range(8):
                rows = slice(8 * x, 8 * x + 8)
                halo = at_lane(packed, 8 * c + x, lane_to)
                ends_ref[2 * c + k, rows] = local_ref[c * tiles + t, rows] + halo

    for c in range(COMPONENTS):
        for t in range(tiles):
            spot = c * tiles + t
            ref, at = local_ref, spot
            if t in (0, tiles - 1):
                ref, at = ends_ref, 2 * c + (t > 0)
            first_plane = ref[at, 0:8]
            last_plane = ref[at, 56:64]
            xa_ref[spot] = jnp.where(even_x, last_plane, first_plane)
            xb_ref[spot] = jnp.where(even_x, first_plane, last_plane)
            first_rows = ref[at, pl.ds(0, 8, stride=8)]
            last_rows = ref[at, pl.ds(7, 8, stride=8)]
            rows_a = jnp.where(even_y, last_rows, first_rows)
            yb_ref[spot] = jnp.where(even_y, first_rows, last_rows)
            ia_ref[18 * t + 6 * c : 18 * t + 6 * c + 6] = rows_a[1:7]
            ea_ref[6 * t + 2 * c : 6 * t + 2 * c + 1] = rows_a[0:1]
            ea_ref[6 * t + 2 * c + 1 : 6 * t + 2 * c + 2] = rows_a[7:8]


def copy_kernel(in_ref, out_ref):
    out_ref[...] = in_ref[...]


def edge_kernel(ea_ref, yb_ref, xa_ref, xb_ref, outa_ref, outb_ref):
    tiles = ea_ref.shape[0] // 6
    components = xa_ref.shape[0] // tiles
    even_x, even_y, _ = parities()
    for c in range(components):
        for t in range(tiles):
            spot = c * tiles + t
            sides = ordered(even_x, xa_ref[spot], xb_ref[spot])
            outb_ref[spot] = yb_ref[spot]
            for k in range(2):
                at = 6 * t + 2 * c + k
                at = slice(at, at + 1)
                first, last = sides[k][0:1], sides[k][7:8]
                outa_ref[at] = ea_ref[at] + jnp.where(even_y, last, first)
                x = slice(7 * k, 7 * k + 1)
                outb_ref[spot, x] = yb_ref[spot, x] + jnp.where(even_y, first, last)


def final_kernel(
    local_ref, za_ref, zb_ref, xa_ref, xb_ref, ia_ref, ea_ref, yb_ref, out_hbm, out_ref, sems
):
    components = out_ref.shape[0]
    tiles = local_ref.shape[0] // components
    even_x, even_y, even_z = parities()
    low, high = ordered(even_z, za_ref[...], zb_ref[...])
    sublane = lax.broadcasted_iota(jnp.int32, (8, LANES), 0)
    row_a = jnp.where(even_y, 7, 0)
    row_b = 7 - row_a
    is_a, is_b = sublane == row_a, sublane == row_b
    copies = []
    for c in range(components):
        for t in range(tiles):
            where = slice(t * LANES, t * LANES + LANES)
            spot = c * tiles + t
            below, above = ordered(even_x, xa_ref[spot], xb_ref[spot])
            for x in range(8):
                value = local_ref[spot, 8 * x : 8 * x + 8]
                if t == 0:
                    value = value + at_lane(low, 8 * c + x, 0)
                if t == tiles - 1:
                    value = value + at_lane(high, 8 * c + x, LANES - 1)
                if x in (0, 7):
                    value = value + (above if x else below)
                    at = 6 * t + 2 * c + x // 7
                    line = ea_ref[at : at + 1]
                else:
                    at = 18 * t + 6 * c + x - 1
                    line = ia_ref[at : at + 1]
                other = yb_ref[spot, x : x + 1]
                line = jnp.broadcast_to(line, (8, LANES))
                other = jnp.broadcast_to(other, (8, LANES))
                change = jnp.where(is_a, line, jnp.where(is_b, other, 0.0))
                out_ref[c, x, :, where] = value + change
        copies.append(pltpu.make_async_copy(out_ref.at[c], out_hbm.at[c], sems.at[c]))
        copies[-1].start()
    for copy in copies:
        copy.wait()


def pairs_from(start, count):
    found = []
    for i in range(start, count - 1, 2):
        found += [(i, i + 1), (i + 1, i)]
    return found


def exchange(array, axis, start):
    return lax.ppermute(array, axis, pairs_from(start, lax.axis_size(axis)))


def mixed_exchange(array, side):
    width, height, depth = [lax.axis_size(axis) for axis in ("gx", "gy", "gz")]
    found = []
    for y in range(height):
        for z in range(depth):
            for i, j in pairs_from((side + y + z) % 2, width):
                found.append(((i * height + y) * depth + z, (j * height + y) * depth + z))
    return lax.ppermute(array, ("gx", "gy", "gz"), found)


def call(kernel, outs, scratch=(), flops=1000000, **specs):
    shapes = [out if hasattr(out, "dtype") else jax.ShapeDtypeStruct(out, F32) for out in outs]
    return pl.pallas_call(
        kernel,
        out_shape=shapes,
        scratch_shapes=list(scratch),
        compiler_params=pltpu.CompilerParams(vmem_limit_bytes=24 * 1024 * 1024),
        cost_estimate=pl.CostEstimate(flops=flops, bytes_accessed=1000000, transcendentals=0),
        **specs,
    )


def local(nodal, geometry):
    components, _, _, length = nodal.shape
    tiles = length // LANES
    blocks = length // BLOCK
    face = (components * tiles, 8, LANES)
    inner = (components * tiles * 6, LANES)
    edge = (components * tiles * 2, LANES)
    tile = (8, LANES)
    flat = (components * tiles, 64, LANES)
    constants = [jnp.asarray(table) for table in tables()]
    operands = [
        pltpu.with_memory_space_constraint(operand, pltpu.HBM)
        for operand in [nodal, geometry] + constants
    ]
    hbm = pl.BlockSpec(memory_space=pltpu.HBM)
    kept = [jax.ShapeDtypeStruct(constants[k].shape, constants[k].dtype) for k in (0, 1, 2, 3, 6)]
    loaded = call(
        load_kernel,
        [nodal.shape, (8 * blocks, BLOCK)] + kept + [tile, tile],
        [pltpu.VMEM(operands[k].shape, operands[k].dtype) for k in (1, 6, 7)]
        + [pltpu.SemaphoreType.DMA((10 + components,))],
        in_specs=[hbm] * len(operands),
    )(*operands)
    za = exchange(loaded[-2], "gz", 0)
    zb = exchange(loaded[-1], "gz", 1)
    (result,) = call(stiffness_kernel, [flat])(*loaded[:-2])
    xa, xb, ia, ea, yb = call(
        face_kernel,
        [face, face, inner, edge, face],
        [pltpu.VMEM((2 * components, 64, LANES), F32)],
    )(result, za, zb)
    xa = mixed_exchange(xa, 0)
    xb = mixed_exchange(xb, 1)
    ia = exchange(ia, "gy", 0)
    (ea,) = call(copy_kernel, [edge])(ea)
    ea, yb = call(edge_kernel, [edge, face])(ea, yb, xa, xb)
    yb = exchange(yb, "gy", 1)
    ea = exchange(ea, "gy", 0)
    (result,) = call(
        final_kernel,
        [nodal.shape],
        [pltpu.VMEM(nodal.shape, F32), pltpu.SemaphoreType.DMA((components,))],
        out_specs=[hbm],
    )(result, za, zb, xa, xb, ia, ea, yb)
    return result


def solution(mesh):
    return jax.shard_map(
        local,
        mesh=mesh,
        in_specs=(P(None, "gx", "gy", "gz"), P(None, "gx", "gy", "gz")),
        out_specs=P(None, "gx", "gy", "gz"),
        check_vma=False,
    )
```

```python
import jax
import jax.numpy as jnp
import numpy as np
from jax import lax
from jax.experimental import pallas as pl
from jax.experimental.pallas import tpu as pltpu
from jax.sharding import PartitionSpec as P


interior_points = [
    -0.8717401485096066,
    -0.5917001814331423,
    -0.2092992179024789,
    0.2092992179024789,
    0.5917001814331423,
    0.8717401485096066,
]
LANES = 128
COMPONENTS = 3
BLOCK = 256
F32 = jnp.float32
BF16 = jnp.bfloat16


def legendre_seven(point):
    previous = 1.0
    current = point
    for order in range(1, 7):
        following = ((2 * order + 1) * point * current - order * previous) / (order + 1)
        previous = current
        current = following
    return current


def gll_tables():
    degree = 7
    points = [-1.0] + interior_points + [1.0]
    values = [legendre_seven(point) for point in points]
    node_count = degree + 1
    weights = np.array([2.0 / (degree * (degree + 1) * value * value) for value in values])
    derivative = np.zeros((node_count, node_count))
    for row_index in range(node_count):
        for col_index in range(node_count):
            if row_index != col_index:
                derivative[row_index, col_index] = values[row_index] / (
                    values[col_index] * (points[row_index] - points[col_index])
                )
    derivative[0, 0] = -degree * (degree + 1) / 4.0
    derivative[node_count - 1, node_count - 1] = degree * (degree + 1) / 4.0
    return (derivative.astype(np.float32).astype(np.float64), weights)


def split_table(table):
    high = np.asarray(table, np.float32).astype(jnp.bfloat16)
    low = (np.asarray(table, np.float64) - high.astype(np.float64)).astype(jnp.bfloat16)
    return high, low


def tables():
    derivative, weights = gll_tables()
    eye = np.eye(8)

    def doubled(table):
        high, low = split_table(table)
        top = np.concatenate([high, high], 1)
        return np.concatenate([top, np.concatenate([low, np.zeros_like(low)], 1)], 0)

    high, low = split_table(np.concatenate([np.kron(derivative, eye), np.kron(eye, derivative)], 0))
    grad_y = np.concatenate([high, high, low], 1)
    back = (derivative * weights[:, None]).T
    both = np.concatenate([np.kron(back, np.diag(weights)), np.kron(np.diag(weights), back)], 1)
    back_y = doubled(both)
    many = np.eye(LANES // 8)

    def stacked(table):
        high, low = split_table(table)
        bottom = np.concatenate([high, np.zeros_like(low)], 1)
        return np.concatenate([np.concatenate([high, low], 1), bottom], 0)

    grad_z = stacked(np.kron(many, derivative.T))
    back_z = stacked(np.kron(many, derivative))
    spread = np.kron(np.eye(LANES)[:, : BLOCK // 8], np.ones((1, 8))).astype(jnp.bfloat16)
    weight_z = np.tile(weights, BLOCK // 8)[None].astype(np.float32)
    plane = np.tile(np.kron(weights, weights)[:, None], (1, BLOCK)).astype(np.float32)
    return grad_y, back_y, grad_z, back_z, spread, weight_z, plane


def split(values):
    high = values.astype(BF16)
    return high, (values - high.astype(F32)).astype(BF16)


def dot(left, right):
    return jnp.dot(left, right, preferred_element_type=F32)


def lane_iota():
    return lax.broadcasted_iota(jnp.int32, (8, LANES), 1)


def along_z(high, low, table):
    rows = high.shape[0]
    halves = []
    for k in range(BLOCK // LANES):
        lanes = slice(k * LANES, k * LANES + LANES)
        halves.append(jnp.concatenate([high[:, lanes], low[:, lanes]], 1))
    both = dot(jnp.concatenate(halves, 0), table)
    both = both[:, :LANES] + both[:, LANES:]
    return jnp.concatenate([both[:rows], both[rows:]], 1)


def operator_block(field, factor, gxy_ref, bxy_ref, gz_ref, bz_ref, plane):
    count = field.shape[0] // 64
    high, low = split(field)
    grad_z = along_z(high, low, gz_ref[...])
    g = [factor[k : k + 1] for k in range(6)]
    fluxes = []
    sums = []
    for c in range(count):
        mine = slice(64 * c, 64 * c + 64)
        both = dot(gxy_ref[...], jnp.concatenate([high[mine], low[mine], high[mine]], 0))
        gx, gy = both[:64], both[64:]
        gz = grad_z[mine]
        fx = g[0] * gx + g[3] * gy + g[4] * gz
        fy = g[3] * gx + g[1] * gy + g[5] * gz
        fz = g[4] * gx + g[5] * gy + g[2] * gz
        fluxes.append(fz)
        fh, fl = split(jnp.concatenate([fx, fy], 0))
        both = dot(bxy_ref[...], jnp.concatenate([fh, fl], 0))
        sums.append(both[:64] + both[64:])
    fh, fl = split(jnp.concatenate(fluxes, 0))
    back = along_z(fh, fl, bz_ref[...])
    return [sums[c] + plane * back[64 * c : 64 * c + 64] for c in range(count)]


def spread_rows(rows, spread, weight):
    first = rows.astype(BF16)
    rest = rows - first.astype(F32)
    second = rest.astype(BF16)
    third = (rest - second.astype(F32)).astype(BF16)
    return (dot(first, spread) + dot(second, spread) + dot(third, spread)) * weight


def load_kernel(
    u_hbm, geo_hbm, gy_hbm, by_hbm, gz_hbm, bz_hbm, spread_hbm, wz_hbm, plane_hbm,
    u_ref, factor_ref, gy_ref, by_ref, gz_ref, bz_ref, plane_ref, za_ref, zb_ref,
    geo_ref, spread_ref, wz_ref, sems,
):
    components = u_ref.shape[0]
    length = u_ref.shape[3]
    blocks = length // BLOCK
    per_block = BLOCK // 8
    copies = []
    ends = (pl.ds(0, LANES), pl.ds(length - LANES, LANES))
    middle = pl.ds(LANES, length - 2 * LANES)
    pairs = [(geo_hbm, geo_ref), (spread_hbm, spread_ref), (wz_hbm, wz_ref)]
    pairs += [(u_hbm.at[:, :, :, where], u_ref.at[:, :, :, where]) for where in ends]
    pairs += [(gz_hbm, gz_ref), (gy_hbm, gy_ref), (by_hbm, by_ref), (bz_hbm, bz_ref)]
    pairs += [(plane_hbm, plane_ref)]
    pairs += [(u_hbm.at[c, :, :, middle], u_ref.at[c, :, :, middle]) for c in range(components)]
    for k, (source, target) in enumerate(pairs):
        copies.append(pltpu.make_async_copy(source, target, sems.at[k]))
        copies[-1].start()
    for copy in copies[:3]:
        copy.wait()
    geo = jnp.concatenate(
        [geo_ref[k, 0] for k in range(6)] + [jnp.zeros((2, length // 8), F32)], 0
    )
    rows = []
    for block in range(blocks):
        start = block * per_block
        tile = geo[:, start // LANES * LANES : start // LANES * LANES + LANES]
        shift = start % LANES
        rows.append(pltpu.roll(tile, LANES - shift, 1) if shift else tile)
    expanded = spread_rows(jnp.concatenate(rows, 0), spread_ref[...], wz_ref[...])
    factor_ref[...] = expanded
    for copy in copies[3:10]:
        copy.wait()
    factor = jnp.concatenate([expanded[:8, :LANES], expanded[8 * blocks - 8 :, LANES:]], 1)
    sides = []
    for c in range(components):
        sides.append(jnp.concatenate([u_ref[c, :, :, where].reshape(64, LANES) for where in ends], 1))
    totals = operator_block(
        jnp.concatenate(sides, 0), factor, gy_ref, by_ref, gz_ref, bz_ref, plane_ref[...]
    )
    even_z = lax.rem(lax.axis_index("gz"), 2) == 0
    lane = lane_iota()
    low_plane = jnp.zeros((8, LANES), F32)
    high_plane = jnp.zeros((8, LANES), F32)
    for c in range(components):
        for x in range(8):
            slot = 8 * c + x
            begin = totals[c][8 * x : 8 * x + 8, :LANES]
            end = totals[c][8 * x : 8 * x + 8, LANES:]
            begin = pltpu.roll(begin, slot, 1) if slot else begin
            end = pltpu.roll(end, slot + 1, 1)
            low_plane = jnp.where(lane == slot, begin, low_plane)
            high_plane = jnp.where(lane == slot, end, high_plane)
    za_ref[...] = jnp.where(even_z, high_plane, low_plane)
    zb_ref[...] = jnp.where(even_z, low_plane, high_plane)
    for copy in copies[10:]:
        copy.wait()


def stiffness_kernel(
    u_ref, factor_ref, gy_ref, by_ref, gz_ref, bz_ref, plane_ref, out_ref
):
    components = u_ref.shape[0]
    blocks = u_ref.shape[3] // BLOCK
    tiles = blocks * (BLOCK // LANES)
    lane = lax.broadcasted_iota(jnp.int32, (64, LANES), 1)
    last, initial = lane % 8 == 7, lane % 8 == 0
    final_lane, first_lane = lane == LANES - 1, lane == 0
    zero = jnp.zeros((64, LANES), F32)
    plane = plane_ref[...]
    pending = [None] * components
    edge = [zero] * components

    def finish(c, tile, following):
        value, after, before, previous = pending[c]
        after = jnp.where(final_lane, following, after)
        before = jnp.where(first_lane, previous, before)
        change = jnp.where(last, after, jnp.where(initial, before, 0.0))
        out_ref[c * tiles + tile] = value + change

    for block in range(blocks):
        where = slice(block * BLOCK, block * BLOCK + BLOCK)
        field = jnp.concatenate(
            [u_ref[c, :, :, where].reshape(64, BLOCK) for c in range(components)], 0
        )
        factor = factor_ref[8 * block : 8 * block + 8, :]
        totals = operator_block(field, factor, gy_ref, by_ref, gz_ref, bz_ref, plane)
        for c in range(components):
            for k in range(BLOCK // LANES):
                value = totals[c][:, k * LANES : k * LANES + LANES]
                after = pltpu.roll(value, LANES - 1, 1)
                before = pltpu.roll(value, 1, 1)
                tile = block * (BLOCK // LANES) + k
                if tile:
                    finish(c, tile - 1, after)
                pending[c] = (value, after, before, edge[c])
                edge[c] = before
    for c in range(components):
        finish(c, tiles - 1, zero)


def ordered(even, first, second):
    return jnp.where(even, second, first), jnp.where(even, first, second)


def parities():
    x, y, z = [lax.axis_index(axis) for axis in ("gx", "gy", "gz")]
    odd = lax.rem(z, 2)
    y = y + z + 1
    first = lax.rem(x * (1 - odd) + y * odd, 2) == 0
    second = lax.rem(y * (1 - odd) + x * odd, 2) == 0
    return first, second, odd == 0


def at_lane(packed, slot, lane_to):
    shift = (lane_to - slot) % LANES
    moved = pltpu.roll(packed, shift, 1) if shift else packed
    return jnp.where(lane_iota() == lane_to, moved, 0.0)


def face_kernel(
    local_ref, za_ref, zb_ref, fa_ref, fb_ref, ia_ref, ea_ref, sb_ref, ends_ref
):
    tiles = local_ref.shape[0] // COMPONENTS
    even_first, even_second, even_z = parities()
    low, high = ordered(even_z, za_ref[...], zb_ref[...])
    for c in range(COMPONENTS):
        for k, (t, packed, lane_to) in enumerate(((0, low, 0), (tiles - 1, high, LANES - 1))):
            for x in range(8):
                rows = slice(8 * x, 8 * x + 8)
                halo = at_lane(packed, 8 * c + x, lane_to)
                ends_ref[2 * c + k, rows] = local_ref[c * tiles + t, rows] + halo

    for c in range(COMPONENTS):
        for t in range(tiles):
            spot = c * tiles + t
            ref, at = local_ref, spot
            if t in (0, tiles - 1):
                ref, at = ends_ref, 2 * c + (t > 0)
            planes = (ref[at, 0:8], ref[at, 56:64])
            lines = (ref[at, pl.ds(0, 8, stride=8)], ref[at, pl.ds(7, 8, stride=8)])
            near = [jnp.where(even_z, planes[k], lines[k]) for k in range(2)]
            far = [jnp.where(even_z, lines[k], planes[k]) for k in range(2)]
            fa_ref[spot], fb_ref[spot] = ordered(even_first, *near)
            rows, sb_ref[spot] = ordered(even_second, *far)
            ia_ref[18 * t + 6 * c : 18 * t + 6 * c + 6] = rows[1:7]
            ea_ref[6 * t + 2 * c : 6 * t + 2 * c + 1] = rows[0:1]
            ea_ref[6 * t + 2 * c + 1 : 6 * t + 2 * c + 2] = rows[7:8]


def copy_kernel(in_ref, out_ref):
    out_ref[...] = in_ref[...]


def edge_kernel(ea_ref, sb_ref, fa_ref, fb_ref, outa_ref, outb_ref):
    tiles = ea_ref.shape[0] // (2 * COMPONENTS)
    even_first, even_second, _ = parities()
    for c in range(COMPONENTS):
        for t in range(tiles):
            spot = c * tiles + t
            sides = ordered(even_first, fa_ref[spot], fb_ref[spot])
            outb_ref[spot] = sb_ref[spot]
            for k in range(2):
                at = 6 * t + 2 * c + k
                at = slice(at, at + 1)
                row_a, row_b = ordered(even_second, sides[k][0:1], sides[k][7:8])
                outa_ref[at] = ea_ref[at] + row_a
                end = slice(7 * k, 7 * k + 1)
                outb_ref[spot, end] = sb_ref[spot, end] + row_b


def final_kernel(
    local_ref, za_ref, zb_ref, fa_ref, fb_ref, ia_ref, ea_ref, sb_ref, out_hbm, out_ref, sems
):
    tiles = local_ref.shape[0] // COMPONENTS
    even_first, even_second, even_z = parities()
    low, high = ordered(even_z, za_ref[...], zb_ref[...])
    sublane = lax.broadcasted_iota(jnp.int32, (8, LANES), 0)
    copies = []
    for c in range(COMPONENTS):
        for t in range(tiles):
            where = slice(t * LANES, t * LANES + LANES)
            spot = c * tiles + t
            near = ordered(even_first, fa_ref[spot], fb_ref[spot])
            outer = ea_ref[6 * t + 2 * c : 6 * t + 2 * c + 2]
            inner = ia_ref[18 * t + 6 * c : 18 * t + 6 * c + 6]
            side = jnp.concatenate([outer[0:1], inner, outer[1:2]], 0)
            far = ordered(even_second, side, sb_ref[spot])
            planes = [jnp.where(even_z, near[k], far[k]) for k in range(2)]
            lines = [jnp.where(even_z, far[k], near[k]) for k in range(2)]
            for x in range(8):
                value = local_ref[spot, 8 * x : 8 * x + 8]
                if t == 0:
                    value = value + at_lane(low, 8 * c + x, 0)
                if t == tiles - 1:
                    value = value + at_lane(high, 8 * c + x, LANES - 1)
                if x in (0, 7):
                    value = value + planes[x // 7]
                first, last = [
                    jnp.broadcast_to(lines[k][x : x + 1], (8, LANES)) for k in range(2)
                ]
                change = jnp.where(sublane == 0, first, jnp.where(sublane == 7, last, 0.0))
                out_ref[c, x, :, where] = value + change
        copies.append(pltpu.make_async_copy(out_ref.at[c], out_hbm.at[c], sems.at[c]))
        copies[-1].start()
    for copy in copies:
        copy.wait()


def pairs_from(start, count):
    found = []
    for i in range(start, count - 1, 2):
        found += [(i, i + 1), (i + 1, i)]
    return found


def exchange(array, axis, start):
    return lax.ppermute(array, axis, pairs_from(start, lax.axis_size(axis)))


def mixed_exchange(array, phase, side):
    width, height, depth = [lax.axis_size(axis) for axis in ("gx", "gy", "gz")]
    found = []
    for z in range(depth):
        if (phase == 0) == (z % 2 == 0):
            for y in range(height):
                for i, j in pairs_from(side, width):
                    found.append(((i * height + y) * depth + z, (j * height + y) * depth + z))
        else:
            for x in range(width):
                for i, j in pairs_from((side + z + 1) % 2, height):
                    found.append(((x * height + i) * depth + z, (x * height + j) * depth + z))
    return lax.ppermute(array, ("gx", "gy", "gz"), found)


def call(kernel, outs, scratch=(), flops=1000000, **specs):
    shapes = [out if hasattr(out, "dtype") else jax.ShapeDtypeStruct(out, F32) for out in outs]
    return pl.pallas_call(
        kernel,
        out_shape=shapes,
        scratch_shapes=list(scratch),
        compiler_params=pltpu.CompilerParams(vmem_limit_bytes=24 * 1024 * 1024),
        cost_estimate=pl.CostEstimate(flops=flops, bytes_accessed=1000000, transcendentals=0),
        **specs,
    )


def local(nodal, geometry):
    components, _, _, length = nodal.shape
    tiles = length // LANES
    blocks = length // BLOCK
    face = (components * tiles, 8, LANES)
    inner = (components * tiles * 6, LANES)
    edge = (components * tiles * 2, LANES)
    tile = (8, LANES)
    flat = (components * tiles, 64, LANES)
    constants = [jnp.asarray(table) for table in tables()]
    operands = [
        pltpu.with_memory_space_constraint(operand, pltpu.HBM)
        for operand in [nodal, geometry] + constants
    ]
    hbm = pl.BlockSpec(memory_space=pltpu.HBM)
    kept = [jax.ShapeDtypeStruct(constants[k].shape, constants[k].dtype) for k in (0, 1, 2, 3, 6)]
    loaded = call(
        load_kernel,
        [nodal.shape, (8 * blocks, BLOCK)] + kept + [tile, tile],
        [pltpu.VMEM(operands[k].shape, operands[k].dtype) for k in (1, 6, 7)]
        + [pltpu.SemaphoreType.DMA((10 + components,))],
        in_specs=[hbm] * len(operands),
    )(*operands)
    za = exchange(loaded[-2], "gz", 0)
    zb = exchange(loaded[-1], "gz", 1)
    (result,) = call(stiffness_kernel, [flat])(*loaded[:-2])
    fa, fb, ia, ea, sb = call(
        face_kernel,
        [face, face, inner, edge, face],
        [pltpu.VMEM((2 * components, 64, LANES), F32)],
    )(result, za, zb)
    fa = mixed_exchange(fa, 0, 0)
    fb = mixed_exchange(fb, 0, 1)
    ia = mixed_exchange(ia, 1, 0)
    (ea,) = call(copy_kernel, [edge])(ea)
    ea, sb = call(edge_kernel, [edge, face])(ea, sb, fa, fb)
    sb = mixed_exchange(sb, 1, 1)
    ea = mixed_exchange(ea, 1, 0)
    (result,) = call(
        final_kernel,
        [nodal.shape],
        [pltpu.VMEM(nodal.shape, F32), pltpu.SemaphoreType.DMA((components,))],
        out_specs=[hbm],
    )(result, za, zb, fa, fb, ia, ea, sb)
    return result


def solution(mesh):
    return jax.shard_map(
        local,
        mesh=mesh,
        in_specs=(P(None, "gx", "gy", "gz"), P(None, "gx", "gy", "gz")),
        out_specs=P(None, "gx", "gy", "gz"),
        check_vma=False,
    )
```

```python
import jax
import jax.numpy as jnp
import numpy as np
from jax import lax
from jax.experimental import pallas as pl
from jax.experimental.pallas import tpu as pltpu
from jax.sharding import PartitionSpec as P


interior_points = [
    -0.8717401485096066,
    -0.5917001814331423,
    -0.2092992179024789,
    0.2092992179024789,
    0.5917001814331423,
    0.8717401485096066,
]
LANES = 128
COMPONENTS = 3
BLOCK = 256
F32 = jnp.float32
BF16 = jnp.bfloat16


def legendre_seven(point):
    previous = 1.0
    current = point
    for order in range(1, 7):
        following = ((2 * order + 1) * point * current - order * previous) / (order + 1)
        previous = current
        current = following
    return current


def gll_tables():
    degree = 7
    points = [-1.0] + interior_points + [1.0]
    values = [legendre_seven(point) for point in points]
    node_count = degree + 1
    weights = np.array([2.0 / (degree * (degree + 1) * value * value) for value in values])
    derivative = np.zeros((node_count, node_count))
    for row_index in range(node_count):
        for col_index in range(node_count):
            if row_index != col_index:
                derivative[row_index, col_index] = values[row_index] / (
                    values[col_index] * (points[row_index] - points[col_index])
                )
    derivative[0, 0] = -degree * (degree + 1) / 4.0
    derivative[node_count - 1, node_count - 1] = degree * (degree + 1) / 4.0
    return (derivative.astype(np.float32).astype(np.float64), weights)


def split_table(table):
    high = np.asarray(table, np.float32).astype(jnp.bfloat16)
    low = (np.asarray(table, np.float64) - high.astype(np.float64)).astype(jnp.bfloat16)
    return high, low


def tables():
    derivative, weights = gll_tables()
    eye = np.eye(8)

    def doubled(table):
        high, low = split_table(table)
        top = np.concatenate([high, high], 1)
        return np.concatenate([top, np.concatenate([low, np.zeros_like(low)], 1)], 0)

    high, low = split_table(np.concatenate([np.kron(derivative, eye), np.kron(eye, derivative)], 0))
    grad_y = np.concatenate([high, high, low], 1)
    back = (derivative * weights[:, None]).T
    both = np.concatenate([np.kron(back, np.diag(weights)), np.kron(np.diag(weights), back)], 1)
    back_y = doubled(both)
    many = np.eye(LANES // 8)

    def stacked(table):
        high, low = split_table(table)
        bottom = np.concatenate([high, np.zeros_like(low)], 1)
        return np.concatenate([np.concatenate([high, low], 1), bottom], 0)

    grad_z = stacked(np.kron(many, derivative.T))
    back_z = stacked(np.kron(many, derivative))
    spread = np.kron(np.eye(LANES)[:, : BLOCK // 8], np.ones((1, 8))).astype(jnp.bfloat16)
    weight_z = np.tile(weights, BLOCK // 8)[None].astype(np.float32)
    plane = np.tile(np.kron(weights, weights)[:, None], (1, BLOCK)).astype(np.float32)
    return grad_y, back_y, grad_z, back_z, spread, weight_z, plane


def split(values):
    high = values.astype(BF16)
    return high, (values - high.astype(F32)).astype(BF16)


def dot(left, right):
    return jnp.dot(left, right, preferred_element_type=F32)


def lane_iota():
    return lax.broadcasted_iota(jnp.int32, (8, LANES), 1)


def along_z(high, low, table):
    rows, width = high.shape
    halves = []
    for k in range(width // LANES):
        lanes = slice(k * LANES, k * LANES + LANES)
        halves.append(jnp.concatenate([high[:, lanes], low[:, lanes]], 1))
    both = dot(jnp.concatenate(halves, 0), table)
    both = both[:, :LANES] + both[:, LANES:]
    return jnp.concatenate([both[k * rows : k * rows + rows] for k in range(width // LANES)], 1)


def operator_block(field, factor, gxy_ref, bxy_ref, gz_ref, bz_ref, plane):
    count = field.shape[0] // 64
    high, low = split(field)
    grad_z = along_z(high, low, gz_ref[...])
    g = [factor[k : k + 1] for k in range(6)]
    fluxes = []
    sums = []
    for c in range(count):
        mine = slice(64 * c, 64 * c + 64)
        both = dot(gxy_ref[...], jnp.concatenate([high[mine], low[mine], high[mine]], 0))
        gx, gy = both[:64], both[64:]
        gz = grad_z[mine]
        fx = g[0] * gx + g[3] * gy + g[4] * gz
        fy = g[3] * gx + g[1] * gy + g[5] * gz
        fz = g[4] * gx + g[5] * gy + g[2] * gz
        fluxes.append(fz)
        fh, fl = split(jnp.concatenate([fx, fy], 0))
        both = dot(bxy_ref[...], jnp.concatenate([fh, fl], 0))
        sums.append(both[:64] + both[64:])
    fh, fl = split(jnp.concatenate(fluxes, 0))
    back = along_z(fh, fl, bz_ref[...])
    return [sums[c] + plane * back[64 * c : 64 * c + 64] for c in range(count)]


def spread_rows(rows, spread, weight):
    first = rows.astype(BF16)
    rest = rows - first.astype(F32)
    second = rest.astype(BF16)
    third = (rest - second.astype(F32)).astype(BF16)
    return (dot(first, spread) + dot(second, spread) + dot(third, spread)) * weight


def load_kernel(
    u_hbm, geo_hbm, gy_hbm, by_hbm, gz_hbm, bz_hbm, spread_hbm, wz_hbm, plane_hbm,
    u_ref, factor_ref, gy_ref, by_ref, gz_ref, bz_ref, plane_ref, za_ref, zb_ref,
    geo_ref, spread_ref, wz_ref, sems,
):
    components = u_ref.shape[0]
    length = u_ref.shape[3]
    blocks = length // BLOCK
    per_block = BLOCK // 8
    copies = []
    ends = (pl.ds(0, LANES), pl.ds(length - LANES, LANES))
    middle = pl.ds(LANES, length - 2 * LANES)
    pairs = [(geo_hbm, geo_ref), (spread_hbm, spread_ref), (wz_hbm, wz_ref)]
    pairs += [(u_hbm.at[:, :, :, where], u_ref.at[:, :, :, where]) for where in ends]
    pairs += [(gz_hbm, gz_ref), (gy_hbm, gy_ref), (by_hbm, by_ref), (bz_hbm, bz_ref)]
    pairs += [(plane_hbm, plane_ref)]
    pairs += [(u_hbm.at[c, :, :, middle], u_ref.at[c, :, :, middle]) for c in range(components)]
    for k, (source, target) in enumerate(pairs):
        copies.append(pltpu.make_async_copy(source, target, sems.at[k]))
        copies[-1].start()
    for copy in copies[:3]:
        copy.wait()
    geo = jnp.concatenate(
        [geo_ref[k, 0] for k in range(6)] + [jnp.zeros((2, length // 8), F32)], 0
    )
    rows = []
    for block in range(blocks):
        start = block * per_block
        tile = geo[:, start // LANES * LANES : start // LANES * LANES + LANES]
        shift = start % LANES
        rows.append(pltpu.roll(tile, LANES - shift, 1) if shift else tile)
    expanded = spread_rows(jnp.concatenate(rows, 0), spread_ref[...], wz_ref[...])
    factor_ref[...] = expanded
    for copy in copies[3:10]:
        copy.wait()
    lower = lane_iota() < LANES // 2
    factor = jnp.where(lower, expanded[:8, :LANES], expanded[8 * blocks - 8 :, LANES:])
    lower = lax.broadcasted_iota(jnp.int32, (64, LANES), 1) < LANES // 2
    sides = []
    for c in range(components):
        begin, end = [u_ref[c, :, :, where].reshape(64, LANES) for where in ends]
        sides.append(jnp.where(lower, begin, end))
    totals = operator_block(
        jnp.concatenate(sides, 0), factor, gy_ref, by_ref, gz_ref, bz_ref, plane_ref[:, :LANES]
    )
    even_z = lax.rem(lax.axis_index("gz"), 2) == 0
    lane = lane_iota()
    low_plane = jnp.zeros((8, LANES), F32)
    high_plane = jnp.zeros((8, LANES), F32)
    for c in range(components):
        for x in range(8):
            slot = 8 * c + x
            both = totals[c][8 * x : 8 * x + 8]
            begin = pltpu.roll(both, slot, 1) if slot else both
            end = pltpu.roll(both, slot + 1, 1)
            low_plane = jnp.where(lane == slot, begin, low_plane)
            high_plane = jnp.where(lane == slot, end, high_plane)
    za_ref[...] = jnp.where(even_z, high_plane, low_plane)
    zb_ref[...] = jnp.where(even_z, low_plane, high_plane)
    for copy in copies[10:]:
        copy.wait()


def stiffness_kernel(
    u_ref, factor_ref, gy_ref, by_ref, gz_ref, bz_ref, plane_ref, out_ref
):
    components = u_ref.shape[0]
    blocks = u_ref.shape[3] // BLOCK
    tiles = blocks * (BLOCK // LANES)
    lane = lax.broadcasted_iota(jnp.int32, (64, LANES), 1)
    last, initial = lane % 8 == 7, lane % 8 == 0
    final_lane, first_lane = lane == LANES - 1, lane == 0
    zero = jnp.zeros((64, LANES), F32)
    plane = plane_ref[...]
    pending = [None] * components
    edge = [zero] * components

    def finish(c, tile, following):
        value, after, before, previous = pending[c]
        after = jnp.where(final_lane, following, after)
        before = jnp.where(first_lane, previous, before)
        change = jnp.where(last, after, jnp.where(initial, before, 0.0))
        out_ref[c * tiles + tile] = value + change

    for block in range(blocks):
        where = slice(block * BLOCK, block * BLOCK + BLOCK)
        field = jnp.concatenate(
            [u_ref[c, :, :, where].reshape(64, BLOCK) for c in range(components)], 0
        )
        factor = factor_ref[8 * block : 8 * block + 8, :]
        totals = operator_block(field, factor, gy_ref, by_ref, gz_ref, bz_ref, plane)
        for c in range(components):
            for k in range(BLOCK // LANES):
                value = totals[c][:, k * LANES : k * LANES + LANES]
                after = pltpu.roll(value, LANES - 1, 1)
                before = pltpu.roll(value, 1, 1)
                tile = block * (BLOCK // LANES) + k
                if tile:
                    finish(c, tile - 1, after)
                pending[c] = (value, after, before, edge[c])
                edge[c] = before
    for c in range(components):
        finish(c, tiles - 1, zero)


def ordered(even, first, second):
    return jnp.where(even, second, first), jnp.where(even, first, second)


def parities():
    x, y, z = [lax.axis_index(axis) for axis in ("gx", "gy", "gz")]
    return [lax.rem(index, 2) == 0 for index in (x + z, y + z, z)]


def at_lane(packed, slot, lane_to):
    shift = (lane_to - slot) % LANES
    moved = pltpu.roll(packed, shift, 1) if shift else packed
    return jnp.where(lane_iota() == lane_to, moved, 0.0)


def face_kernel(
    local_ref, za_ref, zb_ref, fa_ref, fb_ref, ia_ref, ea_ref, sb_ref, ends_ref
):
    tiles = local_ref.shape[0] // COMPONENTS
    even_x, even_y, even_z = parities()
    low, high = ordered(even_z, za_ref[...], zb_ref[...])
    for c in range(COMPONENTS):
        for k, (t, packed, lane_to) in enumerate(((0, low, 0), (tiles - 1, high, LANES - 1))):
            for x in range(8):
                rows = slice(8 * x, 8 * x + 8)
                halo = at_lane(packed, 8 * c + x, lane_to)
                ends_ref[2 * c + k, rows] = local_ref[c * tiles + t, rows] + halo

    for c in range(COMPONENTS):
        for t in range(tiles):
            spot = c * tiles + t
            ref, at = local_ref, spot
            if t in (0, tiles - 1):
                ref, at = ends_ref, 2 * c + (t > 0)
            lines = (ref[at, pl.ds(0, 8, stride=8)], ref[at, pl.ds(7, 8, stride=8)])
            fa_ref[spot], fb_ref[spot] = ordered(even_y, *lines)
            plane, sb_ref[spot] = ordered(even_x, ref[at, 0:8], ref[at, 56:64])
            ia_ref[18 * t + 6 * c : 18 * t + 6 * c + 6] = plane[1:7]
            ea_ref[6 * t + 2 * c : 6 * t + 2 * c + 1] = plane[0:1]
            ea_ref[6 * t + 2 * c + 1 : 6 * t + 2 * c + 2] = plane[7:8]


def copy_kernel(in_ref, out_ref):
    out_ref[...] = in_ref[...]


def edge_kernel(ea_ref, sb_ref, fa_ref, fb_ref, outa_ref, outb_ref):
    tiles = ea_ref.shape[0] // (2 * COMPONENTS)
    even_x, even_y, _ = parities()
    for c in range(COMPONENTS):
        for t in range(tiles):
            spot = c * tiles + t
            sides = ordered(even_y, fa_ref[spot], fb_ref[spot])
            outb_ref[spot] = sb_ref[spot]
            for k in range(2):
                at = 6 * t + 2 * c + k
                at = slice(at, at + 1)
                row_a, row_b = ordered(even_x, sides[k][0:1], sides[k][7:8])
                outa_ref[at] = ea_ref[at] + row_a
                end = slice(7 * k, 7 * k + 1)
                outb_ref[spot, end] = sb_ref[spot, end] + row_b


def base_kernel(
    local_ref, za_ref, zb_ref, fa_ref, fb_ref, out_hbm, first_ref, last_ref, out_ref, sems
):
    tiles = local_ref.shape[0] // COMPONENTS
    _, even_y, even_z = parities()
    low, high = ordered(even_z, za_ref[...], zb_ref[...])
    sublane = lax.broadcasted_iota(jnp.int32, (8, LANES), 0)
    copies = []
    for c in range(COMPONENTS):
        for t in range(tiles):
            where = slice(t * LANES, t * LANES + LANES)
            spot = c * tiles + t
            lines = ordered(even_y, fa_ref[spot], fb_ref[spot])
            for x in range(8):
                value = local_ref[spot, 8 * x : 8 * x + 8]
                if t == 0:
                    value = value + at_lane(low, 8 * c + x, 0)
                if t == tiles - 1:
                    value = value + at_lane(high, 8 * c + x, LANES - 1)
                first, last = [
                    jnp.broadcast_to(lines[k][x : x + 1], (8, LANES)) for k in range(2)
                ]
                change = jnp.where(sublane == 0, first, jnp.where(sublane == 7, last, 0.0))
                if x == 0:
                    first_ref[spot] = value + change
                elif x == 7:
                    last_ref[spot] = value + change
                else:
                    out_ref[c, x - 1, :, where] = value + change
        copies.append(pltpu.make_async_copy(out_ref.at[c], out_hbm.at[c, 1:7], sems.at[c]))
        copies[-1].start()
    for copy in copies:
        copy.wait()


def late_kernel(
    base_hbm, first_ref, last_ref, ia_ref, ea_ref, sb_ref, out_hbm, planes_ref, sems
):
    del base_hbm
    tiles = first_ref.shape[0] // COMPONENTS
    even_x, _, _ = parities()
    copies = []
    for c in range(COMPONENTS):
        for t in range(tiles):
            where = slice(t * LANES, t * LANES + LANES)
            spot = c * tiles + t
            outer = ea_ref[6 * t + 2 * c : 6 * t + 2 * c + 2]
            inner = ia_ref[18 * t + 6 * c : 18 * t + 6 * c + 6]
            side = jnp.concatenate([outer[0:1], inner, outer[1:2]], 0)
            below, above = ordered(even_x, side, sb_ref[spot])
            planes_ref[c, 0, :, where] = first_ref[spot] + below
            planes_ref[c, 1, :, where] = last_ref[spot] + above
        for k in range(2):
            copies.append(
                pltpu.make_async_copy(
                    planes_ref.at[c, k], out_hbm.at[c, 7 * k], sems.at[2 * c + k]
                )
            )
            copies[-1].start()
    for copy in copies:
        copy.wait()


def pairs_from(start, count):
    found = []
    for i in range(start, count - 1, 2):
        found += [(i, i + 1), (i + 1, i)]
    return found


def exchange(array, axis, start):
    return lax.ppermute(array, axis, pairs_from(start, lax.axis_size(axis)))


def mixed_exchange(array, axis, side):
    depth = lax.axis_size("gz")
    found = []
    for z in range(depth):
        for i, j in pairs_from((side + z) % 2, lax.axis_size(axis)):
            found.append((i * depth + z, j * depth + z))
    return lax.ppermute(array, (axis, "gz"), found)


def call(kernel, outs, scratch=(), flops=1000000, **specs):
    shapes = [out if hasattr(out, "dtype") else jax.ShapeDtypeStruct(out, F32) for out in outs]
    return pl.pallas_call(
        kernel,
        out_shape=shapes,
        scratch_shapes=list(scratch),
        compiler_params=pltpu.CompilerParams(vmem_limit_bytes=24 * 1024 * 1024),
        cost_estimate=pl.CostEstimate(flops=flops, bytes_accessed=1000000, transcendentals=0),
        **specs,
    )


def local(nodal, geometry):
    components, _, _, length = nodal.shape
    tiles = length // LANES
    blocks = length // BLOCK
    face = (components * tiles, 8, LANES)
    inner = (components * tiles * 6, LANES)
    edge = (components * tiles * 2, LANES)
    tile = (8, LANES)
    flat = (components * tiles, 64, LANES)
    constants = [jnp.asarray(table) for table in tables()]
    operands = [
        pltpu.with_memory_space_constraint(operand, pltpu.HBM)
        for operand in [nodal, geometry] + constants
    ]
    hbm = pl.BlockSpec(memory_space=pltpu.HBM)
    kept = [jax.ShapeDtypeStruct(constants[k].shape, constants[k].dtype) for k in (0, 1, 2, 3, 6)]
    loaded = call(
        load_kernel,
        [nodal.shape, (8 * blocks, BLOCK)] + kept + [tile, tile],
        [pltpu.VMEM(operands[k].shape, operands[k].dtype) for k in (1, 6, 7)]
        + [pltpu.SemaphoreType.DMA((10 + components,))],
        in_specs=[hbm] * len(operands),
    )(*operands)
    za = exchange(loaded[-2], "gz", 0)
    zb = exchange(loaded[-1], "gz", 1)
    (result,) = call(stiffness_kernel, [flat])(*loaded[:-2])
    fa, fb, ia, ea, sb = call(
        face_kernel,
        [face, face, inner, edge, face],
        [pltpu.VMEM((2 * components, 64, LANES), F32)],
    )(result, za, zb)
    fa = mixed_exchange(fa, "gy", 0)
    fb = mixed_exchange(fb, "gy", 1)
    ia = mixed_exchange(ia, "gx", 0)
    (ea,) = call(copy_kernel, [edge])(ea)
    ea, sb = call(edge_kernel, [edge, face])(ea, sb, fa, fb)
    sb = mixed_exchange(sb, "gx", 1)
    ea = mixed_exchange(ea, "gx", 0)
    vmem = pl.BlockSpec(memory_space=pltpu.VMEM)
    result, first, last = call(
        base_kernel,
        [nodal.shape, face, face],
        [pltpu.VMEM((components, 6, 8, length), F32), pltpu.SemaphoreType.DMA((3,))],
        out_specs=[hbm, vmem, vmem],
    )(result, za, zb, fa, fb)
    (result,) = call(
        late_kernel,
        [nodal.shape],
        [pltpu.VMEM((components, 2, 8, length), F32), pltpu.SemaphoreType.DMA((6,))],
        in_specs=[hbm] + [vmem] * 5,
        out_specs=[hbm],
        input_output_aliases={0: 0},
    )(result, first, last, ia, ea, sb)
    return result


def solution(mesh):
    return jax.shard_map(
        local,
        mesh=mesh,
        in_specs=(P(None, "gx", "gy", "gz"), P(None, "gx", "gy", "gz")),
        out_specs=P(None, "gx", "gy", "gz"),
        check_vma=False,
    )
```

```python
import jax
import jax.numpy as jnp
import numpy as np
from jax import lax
from jax.experimental import pallas as pl
from jax.experimental.pallas import tpu as pltpu
from jax.sharding import PartitionSpec as P


interior_points = [
    -0.8717401485096066,
    -0.5917001814331423,
    -0.2092992179024789,
    0.2092992179024789,
    0.5917001814331423,
    0.8717401485096066,
]
LANES = 128
COMPONENTS = 3
BLOCK = 256
F32 = jnp.float32
BF16 = jnp.bfloat16


def legendre_seven(point):
    previous = 1.0
    current = point
    for order in range(1, 7):
        following = ((2 * order + 1) * point * current - order * previous) / (order + 1)
        previous = current
        current = following
    return current


def gll_tables():
    degree = 7
    points = [-1.0] + interior_points + [1.0]
    values = [legendre_seven(point) for point in points]
    node_count = degree + 1
    weights = np.array([2.0 / (degree * (degree + 1) * value * value) for value in values])
    derivative = np.zeros((node_count, node_count))
    for row_index in range(node_count):
        for col_index in range(node_count):
            if row_index != col_index:
                derivative[row_index, col_index] = values[row_index] / (
                    values[col_index] * (points[row_index] - points[col_index])
                )
    derivative[0, 0] = -degree * (degree + 1) / 4.0
    derivative[node_count - 1, node_count - 1] = degree * (degree + 1) / 4.0
    return (derivative.astype(np.float32).astype(np.float64), weights)


def split_table(table):
    high = np.asarray(table, np.float32).astype(jnp.bfloat16)
    low = (np.asarray(table, np.float64) - high.astype(np.float64)).astype(jnp.bfloat16)
    return high, low


def tables():
    derivative, weights = gll_tables()
    eye = np.eye(8)

    def doubled(table):
        high, low = split_table(table)
        top = np.concatenate([high, high], 1)
        return np.concatenate([top, np.concatenate([low, np.zeros_like(low)], 1)], 0)

    high, low = split_table(np.concatenate([np.kron(derivative, eye), np.kron(eye, derivative)], 0))
    grad_y = np.concatenate([high, high, low], 1)
    back = (derivative * weights[:, None]).T
    both = np.concatenate([np.kron(back, np.diag(weights)), np.kron(np.diag(weights), back)], 1)
    back_y = doubled(both)
    many = np.eye(LANES // 8)

    def stacked(table):
        high, low = split_table(table)
        bottom = np.concatenate([high, np.zeros_like(low)], 1)
        return np.concatenate([np.concatenate([high, low], 1), bottom], 0)

    grad_z = stacked(np.kron(many, derivative.T))
    back_z = stacked(np.kron(many, derivative))
    spread = np.kron(np.eye(LANES)[:, : BLOCK // 8], np.ones((1, 8))).astype(jnp.bfloat16)
    weight_z = np.tile(weights, BLOCK // 8)[None].astype(np.float32)
    plane = np.tile(np.kron(weights, weights)[:, None], (1, BLOCK)).astype(np.float32)
    return grad_y, back_y, grad_z, back_z, spread, weight_z, plane


def split(values):
    high = values.astype(BF16)
    return high, (values - high.astype(F32)).astype(BF16)


def dot(left, right):
    return jnp.dot(left, right, preferred_element_type=F32)


def lane_iota():
    return lax.broadcasted_iota(jnp.int32, (8, LANES), 1)


def along_z(high, low, table):
    rows, width = high.shape
    halves = []
    for k in range(width // LANES):
        lanes = slice(k * LANES, k * LANES + LANES)
        halves.append(jnp.concatenate([high[:, lanes], low[:, lanes]], 1))
    both = dot(jnp.concatenate(halves, 0), table)
    both = both[:, :LANES] + both[:, LANES:]
    return jnp.concatenate([both[k * rows : k * rows + rows] for k in range(width // LANES)], 1)


def operator_block(field, factor, gxy_ref, bxy_ref, gz_ref, bz_ref, plane):
    count = field.shape[0] // 64
    high, low = split(field)
    grad_z = along_z(high, low, gz_ref[...])
    g = [factor[k : k + 1] for k in range(6)]
    fluxes = []
    sums = []
    for c in range(count):
        mine = slice(64 * c, 64 * c + 64)
        both = dot(gxy_ref[...], jnp.concatenate([high[mine], low[mine], high[mine]], 0))
        gx, gy = both[:64], both[64:]
        gz = grad_z[mine]
        fx = g[0] * gx + g[3] * gy + g[4] * gz
        fy = g[3] * gx + g[1] * gy + g[5] * gz
        fz = g[4] * gx + g[5] * gy + g[2] * gz
        fluxes.append(fz)
        fh, fl = split(jnp.concatenate([fx, fy], 0))
        both = dot(bxy_ref[...], jnp.concatenate([fh, fl], 0))
        sums.append(both[:64] + both[64:])
    fh, fl = split(jnp.concatenate(fluxes, 0))
    back = along_z(fh, fl, bz_ref[...])
    return [sums[c] + plane * back[64 * c : 64 * c + 64] for c in range(count)]


def spread_rows(rows, spread, weight):
    first = rows.astype(BF16)
    rest = rows - first.astype(F32)
    second = rest.astype(BF16)
    third = (rest - second.astype(F32)).astype(BF16)
    return (dot(first, spread) + dot(second, spread) + dot(third, spread)) * weight


def load_kernel(
    u_hbm, geo_hbm, gy_hbm, by_hbm, gz_hbm, bz_hbm, spread_hbm, wz_hbm, plane_hbm,
    u_ref, factor_ref, gy_ref, by_ref, gz_ref, bz_ref, plane_ref, za_ref, zb_ref,
    geo_ref, spread_ref, wz_ref, sems,
):
    components = u_ref.shape[0]
    length = u_ref.shape[3]
    blocks = length // BLOCK
    per_block = BLOCK // 8
    copies = []
    ends = (pl.ds(0, LANES), pl.ds(length - LANES, LANES))
    middle = pl.ds(LANES, length - 2 * LANES)
    pairs = [(geo_hbm, geo_ref), (spread_hbm, spread_ref), (wz_hbm, wz_ref)]
    pairs += [(u_hbm.at[:, :, :, where], u_ref.at[:, :, :, where]) for where in ends]
    pairs += [(gz_hbm, gz_ref), (gy_hbm, gy_ref), (by_hbm, by_ref), (bz_hbm, bz_ref)]
    pairs += [(plane_hbm, plane_ref)]
    pairs += [(u_hbm.at[c, :, :, middle], u_ref.at[c, :, :, middle]) for c in range(components)]
    for k, (source, target) in enumerate(pairs):
        copies.append(pltpu.make_async_copy(source, target, sems.at[k]))
        copies[-1].start()
    for copy in copies[:3]:
        copy.wait()
    geo = jnp.concatenate(
        [geo_ref[k, 0] for k in range(6)] + [jnp.zeros((2, length // 8), F32)], 0
    )
    rows = []
    for block in range(blocks):
        start = block * per_block
        tile = geo[:, start // LANES * LANES : start // LANES * LANES + LANES]
        shift = start % LANES
        rows.append(pltpu.roll(tile, LANES - shift, 1) if shift else tile)
    expanded = spread_rows(jnp.concatenate(rows, 0), spread_ref[...], wz_ref[...])
    factor_ref[...] = expanded
    for copy in copies[3:10]:
        copy.wait()
    lower = lane_iota() < LANES // 2
    factor = jnp.where(lower, expanded[:8, :LANES], expanded[8 * blocks - 8 :, LANES:])
    lower = lax.broadcasted_iota(jnp.int32, (64, LANES), 1) < LANES // 2
    sides = []
    for c in range(components):
        begin, end = [u_ref[c, :, :, where].reshape(64, LANES) for where in ends]
        sides.append(jnp.where(lower, begin, end))
    totals = operator_block(
        jnp.concatenate(sides, 0), factor, gy_ref, by_ref, gz_ref, bz_ref, plane_ref[:, :LANES]
    )
    even_z = lax.rem(lax.axis_index("gz"), 2) == 0
    lane = lane_iota()
    low_plane = jnp.zeros((8, LANES), F32)
    high_plane = jnp.zeros((8, LANES), F32)
    for c in range(components):
        for x in range(8):
            slot = 8 * c + x
            both = totals[c][8 * x : 8 * x + 8]
            begin = pltpu.roll(both, slot, 1) if slot else both
            end = pltpu.roll(both, slot + 1, 1)
            low_plane = jnp.where(lane == slot, begin, low_plane)
            high_plane = jnp.where(lane == slot, end, high_plane)
    za_ref[...] = jnp.where(even_z, high_plane, low_plane)
    zb_ref[...] = jnp.where(even_z, low_plane, high_plane)
    for copy in copies[10:]:
        copy.wait()


def stiffness_kernel(
    u_ref, factor_ref, gy_ref, by_ref, gz_ref, bz_ref, plane_ref, out_ref
):
    components = u_ref.shape[0]
    blocks = u_ref.shape[3] // BLOCK
    tiles = blocks * (BLOCK // LANES)
    lane = lax.broadcasted_iota(jnp.int32, (64, LANES), 1)
    last, initial = lane % 8 == 7, lane % 8 == 0
    final_lane, first_lane = lane == LANES - 1, lane == 0
    zero = jnp.zeros((64, LANES), F32)
    plane = plane_ref[...]
    pending = [None] * components
    edge = [zero] * components

    def finish(c, tile, following):
        value, after, before, previous = pending[c]
        after = jnp.where(final_lane, following, after)
        before = jnp.where(first_lane, previous, before)
        change = jnp.where(last, after, jnp.where(initial, before, 0.0))
        out_ref[c * tiles + tile] = value + change

    for block in range(blocks):
        where = slice(block * BLOCK, block * BLOCK + BLOCK)
        field = jnp.concatenate(
            [u_ref[c, :, :, where].reshape(64, BLOCK) for c in range(components)], 0
        )
        factor = factor_ref[8 * block : 8 * block + 8, :]
        totals = operator_block(field, factor, gy_ref, by_ref, gz_ref, bz_ref, plane)
        for c in range(components):
            for k in range(BLOCK // LANES):
                value = totals[c][:, k * LANES : k * LANES + LANES]
                after = pltpu.roll(value, LANES - 1, 1)
                before = pltpu.roll(value, 1, 1)
                tile = block * (BLOCK // LANES) + k
                if tile:
                    finish(c, tile - 1, after)
                pending[c] = (value, after, before, edge[c])
                edge[c] = before
    for c in range(components):
        finish(c, tiles - 1, zero)


def ordered(even, first, second):
    return jnp.where(even, second, first), jnp.where(even, first, second)


def parities():
    x, y, z = [lax.axis_index(axis) for axis in ("gx", "gy", "gz")]
    return [lax.rem(index, 2) == 0 for index in (x + z, y + z, z)]


def at_lane(packed, slot, lane_to):
    shift = (lane_to - slot) % LANES
    moved = pltpu.roll(packed, shift, 1) if shift else packed
    return jnp.where(lane_iota() == lane_to, moved, 0.0)


def face_kernel(
    local_ref, za_ref, zb_ref, xa_ref, xb_ref, ya_ref, yb_ref, ends_ref
):
    tiles = local_ref.shape[0] // COMPONENTS
    even_x, even_y, even_z = parities()
    low, high = ordered(even_z, za_ref[...], zb_ref[...])
    for c in range(COMPONENTS):
        for k, (t, packed, lane_to) in enumerate(((0, low, 0), (tiles - 1, high, LANES - 1))):
            for x in range(8):
                rows = slice(8 * x, 8 * x + 8)
                halo = at_lane(packed, 8 * c + x, lane_to)
                ends_ref[2 * c + k, rows] = local_ref[c * tiles + t, rows] + halo

    for c in range(COMPONENTS):
        for t in range(tiles):
            spot = c * tiles + t
            ref, at = local_ref, spot
            if t in (0, tiles - 1):
                ref, at = ends_ref, 2 * c + (t > 0)
            xa_ref[spot], xb_ref[spot] = ordered(even_x, ref[at, 0:8], ref[at, 56:64])
            lines = (ref[at, pl.ds(0, 8, stride=8)], ref[at, pl.ds(7, 8, stride=8)])
            ya_ref[spot], yb_ref[spot] = ordered(even_y, *lines)


def edge_kernel(ya_ref, yb_ref, xa_ref, xb_ref, outa_ref, outb_ref):
    even_x, even_y, _ = parities()
    for spot in range(xa_ref.shape[0]):
        sides = ordered(even_x, xa_ref[spot], xb_ref[spot])
        outa_ref[spot] = ya_ref[spot]
        outb_ref[spot] = yb_ref[spot]
        for k in range(2):
            row_a, row_b = ordered(even_y, sides[k][0:1], sides[k][7:8])
            end = slice(7 * k, 7 * k + 1)
            outa_ref[spot, end] = ya_ref[spot, end] + row_a
            outb_ref[spot, end] = yb_ref[spot, end] + row_b


def final_kernel(
    local_ref, za_ref, zb_ref, xa_ref, xb_ref, ya_ref, yb_ref, out_hbm, out_ref, sems
):
    tiles = local_ref.shape[0] // COMPONENTS
    even_x, even_y, even_z = parities()
    low, high = ordered(even_z, za_ref[...], zb_ref[...])
    sublane = lax.broadcasted_iota(jnp.int32, (8, LANES), 0)
    copies = []
    for c in range(COMPONENTS):
        for t in range(tiles):
            where = slice(t * LANES, t * LANES + LANES)
            spot = c * tiles + t
            planes = ordered(even_x, xa_ref[spot], xb_ref[spot])
            lines = ordered(even_y, ya_ref[spot], yb_ref[spot])
            for x in range(8):
                value = local_ref[spot, 8 * x : 8 * x + 8]
                if t == 0:
                    value = value + at_lane(low, 8 * c + x, 0)
                if t == tiles - 1:
                    value = value + at_lane(high, 8 * c + x, LANES - 1)
                if x in (0, 7):
                    value = value + planes[x // 7]
                first, last = [
                    jnp.broadcast_to(lines[k][x : x + 1], (8, LANES)) for k in range(2)
                ]
                change = jnp.where(sublane == 0, first, jnp.where(sublane == 7, last, 0.0))
                out_ref[c, x, :, where] = value + change
        copies.append(pltpu.make_async_copy(out_ref.at[c], out_hbm.at[c], sems.at[c]))
        copies[-1].start()
    for copy in copies:
        copy.wait()


def pairs_from(start, count):
    found = []
    for i in range(start, count - 1, 2):
        found += [(i, i + 1), (i + 1, i)]
    return found


def exchange(array, axis, start):
    return lax.ppermute(array, axis, pairs_from(start, lax.axis_size(axis)))


def mixed_exchange(array, axis, side):
    depth = lax.axis_size("gz")
    found = []
    for z in range(depth):
        for i, j in pairs_from((side + z) % 2, lax.axis_size(axis)):
            found.append((i * depth + z, j * depth + z))
    return lax.ppermute(array, (axis, "gz"), found)


def call(kernel, outs, scratch=(), flops=1000000, **specs):
    shapes = [out if hasattr(out, "dtype") else jax.ShapeDtypeStruct(out, F32) for out in outs]
    return pl.pallas_call(
        kernel,
        out_shape=shapes,
        scratch_shapes=list(scratch),
        compiler_params=pltpu.CompilerParams(vmem_limit_bytes=24 * 1024 * 1024),
        cost_estimate=pl.CostEstimate(flops=flops, bytes_accessed=1000000, transcendentals=0),
        **specs,
    )


def local(nodal, geometry):
    components, _, _, length = nodal.shape
    tiles = length // LANES
    blocks = length // BLOCK
    face = (components * tiles, 8, LANES)
    tile = (8, LANES)
    flat = (components * tiles, 64, LANES)
    constants = [jnp.asarray(table) for table in tables()]
    operands = [
        pltpu.with_memory_space_constraint(operand, pltpu.HBM)
        for operand in [nodal, geometry] + constants
    ]
    hbm = pl.BlockSpec(memory_space=pltpu.HBM)
    kept = [jax.ShapeDtypeStruct(constants[k].shape, constants[k].dtype) for k in (0, 1, 2, 3, 6)]
    loaded = call(
        load_kernel,
        [nodal.shape, (8 * blocks, BLOCK)] + kept + [tile, tile],
        [pltpu.VMEM(operands[k].shape, operands[k].dtype) for k in (1, 6, 7)]
        + [pltpu.SemaphoreType.DMA((10 + components,))],
        in_specs=[hbm] * len(operands),
    )(*operands)
    za = exchange(loaded[-2], "gz", 0)
    zb = exchange(loaded[-1], "gz", 1)
    (result,) = call(stiffness_kernel, [flat])(*loaded[:-2])
    xa, xb, ya, yb = call(
        face_kernel, [face] * 4, [pltpu.VMEM((2 * components, 64, LANES), F32)]
    )(result, za, zb)
    xa = mixed_exchange(xa, "gx", 0)
    xb = mixed_exchange(xb, "gx", 1)
    ya, yb = call(edge_kernel, [face, face])(ya, yb, xa, xb)
    ya = mixed_exchange(ya, "gy", 0)
    yb = mixed_exchange(yb, "gy", 1)
    (result,) = call(
        final_kernel,
        [nodal.shape],
        [pltpu.VMEM(nodal.shape, F32), pltpu.SemaphoreType.DMA((components,))],
        out_specs=[hbm],
    )(result, za, zb, xa, xb, ya, yb)
    return result


def solution(mesh):
    return jax.shard_map(
        local,
        mesh=mesh,
        in_specs=(P(None, "gx", "gy", "gz"), P(None, "gx", "gy", "gz")),
        out_specs=P(None, "gx", "gy", "gz"),
        check_vma=False,
    )
```

```python
import jax
import jax.numpy as jnp
import numpy as np
from jax import lax
from jax.experimental import pallas as pl
from jax.experimental.pallas import tpu as pltpu
from jax.sharding import PartitionSpec as P


interior_points = [
    -0.8717401485096066,
    -0.5917001814331423,
    -0.2092992179024789,
    0.2092992179024789,
    0.5917001814331423,
    0.8717401485096066,
]
LANES = 128
COMPONENTS = 3
BLOCK = 256
F32 = jnp.float32
BF16 = jnp.bfloat16


def legendre_seven(point):
    previous = 1.0
    current = point
    for order in range(1, 7):
        following = ((2 * order + 1) * point * current - order * previous) / (order + 1)
        previous = current
        current = following
    return current


def gll_tables():
    degree = 7
    points = [-1.0] + interior_points + [1.0]
    values = [legendre_seven(point) for point in points]
    node_count = degree + 1
    weights = np.array([2.0 / (degree * (degree + 1) * value * value) for value in values])
    derivative = np.zeros((node_count, node_count))
    for row_index in range(node_count):
        for col_index in range(node_count):
            if row_index != col_index:
                derivative[row_index, col_index] = values[row_index] / (
                    values[col_index] * (points[row_index] - points[col_index])
                )
    derivative[0, 0] = -degree * (degree + 1) / 4.0
    derivative[node_count - 1, node_count - 1] = degree * (degree + 1) / 4.0
    return (derivative.astype(np.float32).astype(np.float64), weights)


def split_table(table):
    high = np.asarray(table, np.float32).astype(jnp.bfloat16)
    low = (np.asarray(table, np.float64) - high.astype(np.float64)).astype(jnp.bfloat16)
    return high, low


def tables():
    derivative, weights = gll_tables()
    eye = np.eye(8)

    def doubled(table):
        high, low = split_table(table)
        top = np.concatenate([high, high], 1)
        return np.concatenate([top, np.concatenate([low, np.zeros_like(low)], 1)], 0)

    high, low = split_table(np.concatenate([np.kron(derivative, eye), np.kron(eye, derivative)], 0))
    grad_y = np.concatenate([high, high, low], 1)
    back = (derivative * weights[:, None]).T
    both = np.concatenate([np.kron(back, np.diag(weights)), np.kron(np.diag(weights), back)], 1)
    back_y = doubled(both)
    many = np.eye(LANES // 8)

    def stacked(table):
        high, low = split_table(table)
        bottom = np.concatenate([high, np.zeros_like(low)], 1)
        return np.concatenate([np.concatenate([high, low], 1), bottom], 0)

    grad_z = stacked(np.kron(many, derivative.T))
    back_z = stacked(np.kron(many, derivative))
    spread = np.kron(np.eye(LANES)[:, : BLOCK // 8], np.ones((1, 8))).astype(jnp.bfloat16)
    weight_z = np.tile(weights, BLOCK // 8)[None].astype(np.float32)
    plane = np.tile(np.kron(weights, weights)[:, None], (1, BLOCK)).astype(np.float32)
    return grad_y, back_y, grad_z, back_z, spread, weight_z, plane


def split(values):
    high = values.astype(BF16)
    return high, (values - high.astype(F32)).astype(BF16)


def dot(left, right):
    return jnp.dot(left, right, preferred_element_type=F32)


def lane_iota():
    return lax.broadcasted_iota(jnp.int32, (8, LANES), 1)


def along_z(high, low, table):
    rows, width = high.shape
    halves = []
    for k in range(width // LANES):
        lanes = slice(k * LANES, k * LANES + LANES)
        halves.append(jnp.concatenate([high[:, lanes], low[:, lanes]], 1))
    both = dot(jnp.concatenate(halves, 0), table)
    both = both[:, :LANES] + both[:, LANES:]
    return jnp.concatenate([both[k * rows : k * rows + rows] for k in range(width // LANES)], 1)


def operator_block(field, factor, gxy_ref, bxy_ref, gz_ref, bz_ref, plane):
    count = field.shape[0] // 64
    high, low = split(field)
    grad_z = along_z(high, low, gz_ref[...])
    g = [factor[k : k + 1] for k in range(6)]
    fluxes = []
    sums = []
    for c in range(count):
        mine = slice(64 * c, 64 * c + 64)
        both = dot(gxy_ref[...], jnp.concatenate([high[mine], low[mine], high[mine]], 0))
        gx, gy = both[:64], both[64:]
        gz = grad_z[mine]
        fx = g[0] * gx + g[3] * gy + g[4] * gz
        fy = g[3] * gx + g[1] * gy + g[5] * gz
        fz = g[4] * gx + g[5] * gy + g[2] * gz
        fluxes.append(fz)
        fh, fl = split(jnp.concatenate([fx, fy], 0))
        both = dot(bxy_ref[...], jnp.concatenate([fh, fl], 0))
        sums.append(both[:64] + both[64:])
    fh, fl = split(jnp.concatenate(fluxes, 0))
    back = along_z(fh, fl, bz_ref[...])
    return [sums[c] + plane * back[64 * c : 64 * c + 64] for c in range(count)]


def spread_rows(rows, spread, weight):
    first = rows.astype(BF16)
    rest = rows - first.astype(F32)
    second = rest.astype(BF16)
    third = (rest - second.astype(F32)).astype(BF16)
    return (dot(first, spread) + dot(second, spread) + dot(third, spread)) * weight


def load_kernel(
    u_hbm, geo_hbm, gy_hbm, by_hbm, gz_hbm, bz_hbm, spread_hbm, wz_hbm, plane_hbm,
    u_ref, factor_ref, gy_ref, by_ref, gz_ref, bz_ref, plane_ref, za_ref, zb_ref,
    geo_ref, spread_ref, wz_ref, sems,
):
    components = u_ref.shape[0]
    length = u_ref.shape[3]
    blocks = length // BLOCK
    per_block = BLOCK // 8
    copies = []
    ends = (pl.ds(0, LANES), pl.ds(length - LANES, LANES))
    middle = pl.ds(LANES, length - 2 * LANES)
    pairs = [(geo_hbm, geo_ref), (spread_hbm, spread_ref), (wz_hbm, wz_ref)]
    pairs += [(u_hbm.at[:, :, :, where], u_ref.at[:, :, :, where]) for where in ends]
    pairs += [(gz_hbm, gz_ref), (gy_hbm, gy_ref), (by_hbm, by_ref), (bz_hbm, bz_ref)]
    pairs += [(plane_hbm, plane_ref)]
    pairs += [(u_hbm.at[c, :, :, middle], u_ref.at[c, :, :, middle]) for c in range(components)]
    for k, (source, target) in enumerate(pairs):
        copies.append(pltpu.make_async_copy(source, target, sems.at[k]))
        copies[-1].start()
    for copy in copies[:3]:
        copy.wait()
    geo = jnp.concatenate(
        [geo_ref[k, 0] for k in range(6)] + [jnp.zeros((2, length // 8), F32)], 0
    )
    rows = []
    for block in range(blocks):
        start = block * per_block
        tile = geo[:, start // LANES * LANES : start // LANES * LANES + LANES]
        shift = start % LANES
        rows.append(pltpu.roll(tile, LANES - shift, 1) if shift else tile)
    expanded = spread_rows(jnp.concatenate(rows, 0), spread_ref[...], wz_ref[...])
    factor_ref[...] = expanded
    for copy in copies[3:10]:
        copy.wait()
    lower = lane_iota() < LANES // 2
    factor = jnp.where(lower, expanded[:8, :LANES], expanded[8 * blocks - 8 :, LANES:])
    lower = lax.broadcasted_iota(jnp.int32, (64, LANES), 1) < LANES // 2
    sides = []
    for c in range(components):
        begin, end = [u_ref[c, :, :, where].reshape(64, LANES) for where in ends]
        sides.append(jnp.where(lower, begin, end))
    totals = operator_block(
        jnp.concatenate(sides, 0), factor, gy_ref, by_ref, gz_ref, bz_ref, plane_ref[:, :LANES]
    )
    even_z = lax.rem(lax.axis_index("gz"), 2) == 0
    lane = lane_iota()
    low_plane = jnp.zeros((8, LANES), F32)
    high_plane = jnp.zeros((8, LANES), F32)
    for c in range(components):
        for x in range(8):
            slot = 8 * c + x
            both = totals[c][8 * x : 8 * x + 8]
            begin = pltpu.roll(both, slot, 1) if slot else both
            end = pltpu.roll(both, slot + 1, 1)
            low_plane = jnp.where(lane == slot, begin, low_plane)
            high_plane = jnp.where(lane == slot, end, high_plane)
    za_ref[...] = jnp.where(even_z, high_plane, low_plane)
    zb_ref[...] = jnp.where(even_z, low_plane, high_plane)
    for copy in copies[10:]:
        copy.wait()


def stiffness_kernel(
    u_ref, factor_ref, gy_ref, by_ref, gz_ref, bz_ref, plane_ref, out_ref
):
    components = u_ref.shape[0]
    blocks = u_ref.shape[3] // BLOCK
    tiles = blocks * (BLOCK // LANES)
    lane = lax.broadcasted_iota(jnp.int32, (64, LANES), 1)
    last, initial = lane % 8 == 7, lane % 8 == 0
    final_lane, first_lane = lane == LANES - 1, lane == 0
    zero = jnp.zeros((64, LANES), F32)
    plane = plane_ref[...]
    pending = [None] * components
    edge = [zero] * components

    def finish(c, tile, following):
        value, after, before, previous = pending[c]
        after = jnp.where(final_lane, following, after)
        before = jnp.where(first_lane, previous, before)
        change = jnp.where(last, after, jnp.where(initial, before, 0.0))
        out_ref[c * tiles + tile] = value + change

    for block in range(blocks):
        where = slice(block * BLOCK, block * BLOCK + BLOCK)
        field = jnp.concatenate(
            [u_ref[c, :, :, where].reshape(64, BLOCK) for c in range(components)], 0
        )
        factor = factor_ref[8 * block : 8 * block + 8, :]
        totals = operator_block(field, factor, gy_ref, by_ref, gz_ref, bz_ref, plane)
        for c in range(components):
            for k in range(BLOCK // LANES):
                value = totals[c][:, k * LANES : k * LANES + LANES]
                after = pltpu.roll(value, LANES - 1, 1)
                before = pltpu.roll(value, 1, 1)
                tile = block * (BLOCK // LANES) + k
                if tile:
                    finish(c, tile - 1, after)
                pending[c] = (value, after, before, edge[c])
                edge[c] = before
    for c in range(components):
        finish(c, tiles - 1, zero)


def ordered(even, first, second):
    return jnp.where(even, second, first), jnp.where(even, first, second)


def parities():
    x, y, z = [lax.axis_index(axis) for axis in ("gx", "gy", "gz")]
    return [lax.rem(index, 2) == 0 for index in (x + z, y, z)]


def at_lane(packed, slot, lane_to):
    shift = (lane_to - slot) % LANES
    moved = pltpu.roll(packed, shift, 1) if shift else packed
    return jnp.where(lane_iota() == lane_to, moved, 0.0)


def face_kernel(
    local_ref, za_ref, zb_ref, xa_ref, xb_ref, ia_ref, ea_ref, yb_ref, ends_ref
):
    tiles = local_ref.shape[0] // COMPONENTS
    even_x, even_y, even_z = parities()
    low, high = ordered(even_z, za_ref[...], zb_ref[...])
    for c in range(COMPONENTS):
        for k, (t, packed, lane_to) in enumerate(((0, low, 0), (tiles - 1, high, LANES - 1))):
            for x in range(8):
                rows = slice(8 * x, 8 * x + 8)
                halo = at_lane(packed, 8 * c + x, lane_to)
                ends_ref[2 * c + k, rows] = local_ref[c * tiles + t, rows] + halo

    for c in range(COMPONENTS):
        for t in range(tiles):
            spot = c * tiles + t
            ref, at = local_ref, spot
            if t in (0, tiles - 1):
                ref, at = ends_ref, 2 * c + (t > 0)
            first_plane = ref[at, 0:8]
            last_plane = ref[at, 56:64]
            xa_ref[spot] = jnp.where(even_x, last_plane, first_plane)
            xb_ref[spot] = jnp.where(even_x, first_plane, last_plane)
            first_rows = ref[at, pl.ds(0, 8, stride=8)]
            last_rows = ref[at, pl.ds(7, 8, stride=8)]
            rows_a = jnp.where(even_y, last_rows, first_rows)
            yb_ref[spot] = jnp.where(even_y, first_rows, last_rows)
            ia_ref[18 * t + 6 * c : 18 * t + 6 * c + 6] = rows_a[1:7]
            ea_ref[6 * t + 2 * c : 6 * t + 2 * c + 1] = rows_a[0:1]
            ea_ref[6 * t + 2 * c + 1 : 6 * t + 2 * c + 2] = rows_a[7:8]


def copy_kernel(in_ref, out_ref):
    out_ref[...] = in_ref[...]


def edge_kernel(ea_ref, yb_ref, xa_ref, xb_ref, outa_ref, outb_ref):
    tiles = ea_ref.shape[0] // 6
    components = xa_ref.shape[0] // tiles
    even_x, even_y, _ = parities()
    for c in range(components):
        for t in range(tiles):
            spot = c * tiles + t
            sides = ordered(even_x, xa_ref[spot], xb_ref[spot])
            outb_ref[spot] = yb_ref[spot]
            for k in range(2):
                at = 6 * t + 2 * c + k
                at = slice(at, at + 1)
                first, last = sides[k][0:1], sides[k][7:8]
                outa_ref[at] = ea_ref[at] + jnp.where(even_y, last, first)
                x = slice(7 * k, 7 * k + 1)
                outb_ref[spot, x] = yb_ref[spot, x] + jnp.where(even_y, first, last)


def base_kernel(
    local_ref, za_ref, zb_ref, xa_ref, xb_ref, out_hbm, first_ref, last_ref, out_ref, tile_ref, sems
):
    tiles = local_ref.shape[0] // COMPONENTS
    even_x, _, even_z = parities()
    low, high = ordered(even_z, za_ref[...], zb_ref[...])
    copies = []
    for c in range(COMPONENTS):
        for t in range(tiles):
            where = slice(t * LANES, t * LANES + LANES)
            spot = c * tiles + t
            planes = ordered(even_x, xa_ref[spot], xb_ref[spot])
            for x in range(8):
                value = local_ref[spot, 8 * x : 8 * x + 8]
                if t == 0:
                    value = value + at_lane(low, 8 * c + x, 0)
                if t == tiles - 1:
                    value = value + at_lane(high, 8 * c + x, LANES - 1)
                if x in (0, 7):
                    value = value + planes[x // 7]
                out_ref[c, x, :, where] = value
                tile_ref[spot, 8 * x : 8 * x + 8] = value
            first_ref[spot] = tile_ref[spot, pl.ds(0, 8, stride=8)]
            last_ref[spot] = tile_ref[spot, pl.ds(7, 8, stride=8)]
        copies.append(pltpu.make_async_copy(out_ref.at[c], out_hbm.at[c], sems.at[c]))
        copies[-1].start()
    for copy in copies:
        copy.wait()


def late_kernel(
    base_hbm, first_ref, last_ref, ia_ref, ea_ref, yb_ref, out_hbm, rows_ref, sems
):
    del base_hbm
    tiles = first_ref.shape[0] // COMPONENTS
    _, even_y, _ = parities()
    copies = []
    for c in range(COMPONENTS):
        for t in range(tiles):
            where = slice(t * LANES, t * LANES + LANES)
            spot = c * tiles + t
            outer = ea_ref[6 * t + 2 * c : 6 * t + 2 * c + 2]
            inner = ia_ref[18 * t + 6 * c : 18 * t + 6 * c + 6]
            side = jnp.concatenate([outer[0:1], inner, outer[1:2]], 0)
            front, behind = ordered(even_y, side, yb_ref[spot])
            rows_ref[c, 0, :, where] = first_ref[spot] + front
            rows_ref[c, 1, :, where] = last_ref[spot] + behind
        for k in range(2):
            copies.append(
                pltpu.make_async_copy(
                    rows_ref.at[c, k], out_hbm.at[c, :, 7 * k, :], sems.at[2 * c + k]
                )
            )
            copies[-1].start()
    for copy in copies:
        copy.wait()


def pairs_from(start, count):
    found = []
    for i in range(start, count - 1, 2):
        found += [(i, i + 1), (i + 1, i)]
    return found


def exchange(array, axis, start):
    return lax.ppermute(array, axis, pairs_from(start, lax.axis_size(axis)))


def mixed_exchange(array, side):
    width, height, depth = [lax.axis_size(axis) for axis in ("gx", "gy", "gz")]
    found = []
    for y in range(height):
        for z in range(depth):
            for i, j in pairs_from((side + z) % 2, width):
                found.append(((i * height + y) * depth + z, (j * height + y) * depth + z))
    return lax.ppermute(array, ("gx", "gy", "gz"), found)


def call(kernel, outs, scratch=(), flops=1000000, **specs):
    shapes = [out if hasattr(out, "dtype") else jax.ShapeDtypeStruct(out, F32) for out in outs]
    return pl.pallas_call(
        kernel,
        out_shape=shapes,
        scratch_shapes=list(scratch),
        compiler_params=pltpu.CompilerParams(vmem_limit_bytes=24 * 1024 * 1024),
        cost_estimate=pl.CostEstimate(flops=flops, bytes_accessed=1000000, transcendentals=0),
        **specs,
    )


def local(nodal, geometry):
    components, _, _, length = nodal.shape
    tiles = length // LANES
    blocks = length // BLOCK
    face = (components * tiles, 8, LANES)
    inner = (components * tiles * 6, LANES)
    edge = (components * tiles * 2, LANES)
    tile = (8, LANES)
    flat = (components * tiles, 64, LANES)
    constants = [jnp.asarray(table) for table in tables()]
    operands = [
        pltpu.with_memory_space_constraint(operand, pltpu.HBM)
        for operand in [nodal, geometry] + constants
    ]
    hbm = pl.BlockSpec(memory_space=pltpu.HBM)
    kept = [jax.ShapeDtypeStruct(constants[k].shape, constants[k].dtype) for k in (0, 1, 2, 3, 6)]
    loaded = call(
        load_kernel,
        [nodal.shape, (8 * blocks, BLOCK)] + kept + [tile, tile],
        [pltpu.VMEM(operands[k].shape, operands[k].dtype) for k in (1, 6, 7)]
        + [pltpu.SemaphoreType.DMA((10 + components,))],
        in_specs=[hbm] * len(operands),
    )(*operands)
    za = exchange(loaded[-2], "gz", 0)
    zb = exchange(loaded[-1], "gz", 1)
    (result,) = call(stiffness_kernel, [flat])(*loaded[:-2])
    xa, xb, ia, ea, yb = call(
        face_kernel,
        [face, face, inner, edge, face],
        [pltpu.VMEM((2 * components, 64, LANES), F32)],
    )(result, za, zb)
    xa = mixed_exchange(xa, 0)
    xb = mixed_exchange(xb, 1)
    ia = exchange(ia, "gy", 0)
    (ea,) = call(copy_kernel, [edge])(ea)
    ea, yb = call(edge_kernel, [edge, face])(ea, yb, xa, xb)
    yb = exchange(yb, "gy", 1)
    ea = exchange(ea, "gy", 0)
    vmem = pl.BlockSpec(memory_space=pltpu.VMEM)
    result, first, last = call(
        base_kernel,
        [nodal.shape, face, face],
        [
            pltpu.VMEM(nodal.shape, F32),
            pltpu.VMEM(flat, F32),
            pltpu.SemaphoreType.DMA((components,)),
        ],
        out_specs=[hbm, vmem, vmem],
    )(result, za, zb, xa, xb)
    (result,) = call(
        late_kernel,
        [nodal.shape],
        [pltpu.VMEM((components, 2, 8, length), F32), pltpu.SemaphoreType.DMA((2 * components,))],
        in_specs=[hbm] + [vmem] * 5,
        out_specs=[hbm],
        input_output_aliases={0: 0},
    )(result, first, last, ia, ea, yb)
    return result


def solution(mesh):
    return jax.shard_map(
        local,
        mesh=mesh,
        in_specs=(P(None, "gx", "gy", "gz"), P(None, "gx", "gy", "gz")),
        out_specs=P(None, "gx", "gy", "gz"),
        check_vma=False,
    )
```

```python
import jax
import jax.numpy as jnp
import numpy as np
from jax import lax
from jax.experimental import pallas as pl
from jax.experimental.pallas import tpu as pltpu
from jax.sharding import PartitionSpec as P


interior_points = [
    -0.8717401485096066,
    -0.5917001814331423,
    -0.2092992179024789,
    0.2092992179024789,
    0.5917001814331423,
    0.8717401485096066,
]
LANES = 128
COMPONENTS = 3
BLOCK = 256
F32 = jnp.float32
BF16 = jnp.bfloat16


def legendre_seven(point):
    previous = 1.0
    current = point
    for order in range(1, 7):
        following = ((2 * order + 1) * point * current - order * previous) / (order + 1)
        previous = current
        current = following
    return current


def gll_tables():
    degree = 7
    points = [-1.0] + interior_points + [1.0]
    values = [legendre_seven(point) for point in points]
    node_count = degree + 1
    weights = np.array([2.0 / (degree * (degree + 1) * value * value) for value in values])
    derivative = np.zeros((node_count, node_count))
    for row_index in range(node_count):
        for col_index in range(node_count):
            if row_index != col_index:
                derivative[row_index, col_index] = values[row_index] / (
                    values[col_index] * (points[row_index] - points[col_index])
                )
    derivative[0, 0] = -degree * (degree + 1) / 4.0
    derivative[node_count - 1, node_count - 1] = degree * (degree + 1) / 4.0
    return (derivative.astype(np.float32).astype(np.float64), weights)


def split_table(table):
    high = np.asarray(table, np.float32).astype(jnp.bfloat16)
    low = (np.asarray(table, np.float64) - high.astype(np.float64)).astype(jnp.bfloat16)
    return high, low


def tables():
    derivative, weights = gll_tables()
    eye = np.eye(8)

    def doubled(table):
        high, low = split_table(table)
        top = np.concatenate([high, high], 1)
        return np.concatenate([top, np.concatenate([low, np.zeros_like(low)], 1)], 0)

    high, low = split_table(np.concatenate([np.kron(derivative, eye), np.kron(eye, derivative)], 0))
    grad_y = np.concatenate([high, high, low], 1)
    back = (derivative * weights[:, None]).T
    both = np.concatenate([np.kron(back, np.diag(weights)), np.kron(np.diag(weights), back)], 1)
    back_y = doubled(both)
    many = np.eye(LANES // 8)

    def stacked(table):
        high, low = split_table(table)
        bottom = np.concatenate([high, np.zeros_like(low)], 1)
        return np.concatenate([np.concatenate([high, low], 1), bottom], 0)

    grad_z = stacked(np.kron(many, derivative.T))
    back_z = stacked(np.kron(many, derivative))
    spread = np.kron(np.eye(LANES)[:, : BLOCK // 8], np.ones((1, 8))).astype(jnp.bfloat16)
    weight_z = np.tile(weights, BLOCK // 8)[None].astype(np.float32)
    plane = np.tile(np.kron(weights, weights)[:, None], (1, BLOCK)).astype(np.float32)
    return grad_y, back_y, grad_z, back_z, spread, weight_z, plane


def split(values):
    high = values.astype(BF16)
    return high, (values - high.astype(F32)).astype(BF16)


def dot(left, right):
    return jnp.dot(left, right, preferred_element_type=F32)


def lane_iota():
    return lax.broadcasted_iota(jnp.int32, (8, LANES), 1)


def along_z(high, low, table):
    rows, width = high.shape
    halves = []
    for k in range(width // LANES):
        lanes = slice(k * LANES, k * LANES + LANES)
        halves.append(jnp.concatenate([high[:, lanes], low[:, lanes]], 1))
    both = dot(jnp.concatenate(halves, 0), table)
    both = both[:, :LANES] + both[:, LANES:]
    return jnp.concatenate([both[k * rows : k * rows + rows] for k in range(width // LANES)], 1)


def operator_block(field, factor, gxy_ref, bxy_ref, gz_ref, bz_ref, plane):
    count = field.shape[0] // 64
    high, low = split(field)
    grad_z = along_z(high, low, gz_ref[...])
    g = [factor[k : k + 1] for k in range(6)]
    fluxes = []
    sums = []
    for c in range(count):
        mine = slice(64 * c, 64 * c + 64)
        both = dot(gxy_ref[...], jnp.concatenate([high[mine], low[mine], high[mine]], 0))
        gx, gy = both[:64], both[64:]
        gz = grad_z[mine]
        fx = g[0] * gx + g[3] * gy + g[4] * gz
        fy = g[3] * gx + g[1] * gy + g[5] * gz
        fz = g[4] * gx + g[5] * gy + g[2] * gz
        fluxes.append(fz)
        fh, fl = split(jnp.concatenate([fx, fy], 0))
        both = dot(bxy_ref[...], jnp.concatenate([fh, fl], 0))
        sums.append(both[:64] + both[64:])
    fh, fl = split(jnp.concatenate(fluxes, 0))
    back = along_z(fh, fl, bz_ref[...])
    return [sums[c] + plane * back[64 * c : 64 * c + 64] for c in range(count)]


def spread_rows(rows, spread, weight):
    first = rows.astype(BF16)
    rest = rows - first.astype(F32)
    second = rest.astype(BF16)
    third = (rest - second.astype(F32)).astype(BF16)
    return (dot(first, spread) + dot(second, spread) + dot(third, spread)) * weight


def load_kernel(
    u_hbm, geo_hbm, gy_hbm, by_hbm, gz_hbm, bz_hbm, spread_hbm, wz_hbm, plane_hbm,
    u_ref, factor_ref, gy_ref, by_ref, gz_ref, bz_ref, plane_ref, za_ref, zb_ref,
    geo_ref, spread_ref, wz_ref, sems,
):
    components = u_ref.shape[0]
    length = u_ref.shape[3]
    blocks = length // BLOCK
    per_block = BLOCK // 8
    copies = []
    ends = (pl.ds(0, LANES), pl.ds(length - LANES, LANES))
    middle = pl.ds(LANES, length - 2 * LANES)
    pairs = [(geo_hbm, geo_ref), (spread_hbm, spread_ref), (wz_hbm, wz_ref)]
    pairs += [(u_hbm.at[:, :, :, where], u_ref.at[:, :, :, where]) for where in ends]
    pairs += [(gz_hbm, gz_ref), (gy_hbm, gy_ref), (by_hbm, by_ref), (bz_hbm, bz_ref)]
    pairs += [(plane_hbm, plane_ref)]
    pairs += [(u_hbm.at[c, :, :, middle], u_ref.at[c, :, :, middle]) for c in range(components)]
    for k, (source, target) in enumerate(pairs):
        copies.append(pltpu.make_async_copy(source, target, sems.at[k]))
        copies[-1].start()
    for copy in copies[:3]:
        copy.wait()
    geo = jnp.concatenate(
        [geo_ref[k, 0] for k in range(6)] + [jnp.zeros((2, length // 8), F32)], 0
    )
    rows = []
    for block in range(blocks):
        start = block * per_block
        tile = geo[:, start // LANES * LANES : start // LANES * LANES + LANES]
        shift = start % LANES
        rows.append(pltpu.roll(tile, LANES - shift, 1) if shift else tile)
    expanded = spread_rows(jnp.concatenate(rows, 0), spread_ref[...], wz_ref[...])
    factor_ref[...] = expanded
    for copy in copies[3:10]:
        copy.wait()
    lower = lane_iota() < LANES // 2
    factor = jnp.where(lower, expanded[:8, :LANES], expanded[8 * blocks - 8 :, LANES:])
    lower = lax.broadcasted_iota(jnp.int32, (64, LANES), 1) < LANES // 2
    sides = []
    for c in range(components):
        begin, end = [u_ref[c, :, :, where].reshape(64, LANES) for where in ends]
        sides.append(jnp.where(lower, begin, end))
    totals = operator_block(
        jnp.concatenate(sides, 0), factor, gy_ref, by_ref, gz_ref, bz_ref, plane_ref[:, :LANES]
    )
    even_z = lax.rem(lax.axis_index("gz"), 2) == 0
    lane = lane_iota()
    low_plane = jnp.zeros((8, LANES), F32)
    high_plane = jnp.zeros((8, LANES), F32)
    for c in range(components):
        for x in range(8):
            slot = 8 * c + x
            both = totals[c][8 * x : 8 * x + 8]
            begin = pltpu.roll(both, slot, 1) if slot else both
            end = pltpu.roll(both, slot + 1, 1)
            low_plane = jnp.where(lane == slot, begin, low_plane)
            high_plane = jnp.where(lane == slot, end, high_plane)
    za_ref[...] = jnp.where(even_z, high_plane, low_plane)
    zb_ref[...] = jnp.where(even_z, low_plane, high_plane)
    for copy in copies[10:]:
        copy.wait()


def stiffness_kernel(
    u_ref, factor_ref, gy_ref, by_ref, gz_ref, bz_ref, plane_ref, out_ref
):
    components = u_ref.shape[0]
    blocks = u_ref.shape[3] // BLOCK
    tiles = blocks * (BLOCK // LANES)
    lane = lax.broadcasted_iota(jnp.int32, (64, LANES), 1)
    last, initial = lane % 8 == 7, lane % 8 == 0
    final_lane, first_lane = lane == LANES - 1, lane == 0
    zero = jnp.zeros((64, LANES), F32)
    plane = plane_ref[...]
    pending = [None] * components
    edge = [zero] * components

    def finish(c, tile, following):
        value, after, before, previous = pending[c]
        after = jnp.where(final_lane, following, after)
        before = jnp.where(first_lane, previous, before)
        change = jnp.where(last, after, jnp.where(initial, before, 0.0))
        out_ref[c * tiles + tile] = value + change

    for block in range(blocks):
        where = slice(block * BLOCK, block * BLOCK + BLOCK)
        field = jnp.concatenate(
            [u_ref[c, :, :, where].reshape(64, BLOCK) for c in range(components)], 0
        )
        factor = factor_ref[8 * block : 8 * block + 8, :]
        totals = operator_block(field, factor, gy_ref, by_ref, gz_ref, bz_ref, plane)
        for c in range(components):
            for k in range(BLOCK // LANES):
                value = totals[c][:, k * LANES : k * LANES + LANES]
                after = pltpu.roll(value, LANES - 1, 1)
                before = pltpu.roll(value, 1, 1)
                tile = block * (BLOCK // LANES) + k
                if tile:
                    finish(c, tile - 1, after)
                pending[c] = (value, after, before, edge[c])
                edge[c] = before
    for c in range(components):
        finish(c, tiles - 1, zero)


def ordered(even, first, second):
    return jnp.where(even, second, first), jnp.where(even, first, second)


def parities():
    x, y, z = [lax.axis_index(axis) for axis in ("gx", "gy", "gz")]
    return [lax.rem(index, 2) == 0 for index in (x + z, y + z, z)]


def at_lane(packed, slot, lane_to):
    shift = (lane_to - slot) % LANES
    moved = pltpu.roll(packed, shift, 1) if shift else packed
    return jnp.where(lane_iota() == lane_to, moved, 0.0)


def face_kernel(
    local_ref, za_ref, zb_ref, xa_ref, xb_ref, ia_ref, ea_ref, yb_ref, ends_ref
):
    tiles = local_ref.shape[0] // COMPONENTS
    even_x, even_y, even_z = parities()
    low, high = ordered(even_z, za_ref[...], zb_ref[...])
    for c in range(COMPONENTS):
        for k, (t, packed, lane_to) in enumerate(((0, low, 0), (tiles - 1, high, LANES - 1))):
            for x in range(8):
                rows = slice(8 * x, 8 * x + 8)
                halo = at_lane(packed, 8 * c + x, lane_to)
                ends_ref[2 * c + k, rows] = local_ref[c * tiles + t, rows] + halo

    for c in range(COMPONENTS):
        for t in range(tiles):
            spot = c * tiles + t
            ref, at = local_ref, spot
            if t in (0, tiles - 1):
                ref, at = ends_ref, 2 * c + (t > 0)
            first_plane = ref[at, 0:8]
            last_plane = ref[at, 56:64]
            xa_ref[spot] = jnp.where(even_x, last_plane, first_plane)
            xb_ref[spot] = jnp.where(even_x, first_plane, last_plane)
            first_rows = ref[at, pl.ds(0, 8, stride=8)]
            last_rows = ref[at, pl.ds(7, 8, stride=8)]
            rows_a = jnp.where(even_y, last_rows, first_rows)
            yb_ref[spot] = jnp.where(even_y, first_rows, last_rows)
            ia_ref[18 * t + 6 * c : 18 * t + 6 * c + 6] = rows_a[1:7]
            ea_ref[6 * t + 2 * c : 6 * t + 2 * c + 1] = rows_a[0:1]
            ea_ref[6 * t + 2 * c + 1 : 6 * t + 2 * c + 2] = rows_a[7:8]


def copy_kernel(in_ref, out_ref):
    out_ref[...] = in_ref[...]


def edge_kernel(ea_ref, yb_ref, xa_ref, xb_ref, outa_ref, outb_ref):
    tiles = ea_ref.shape[0] // 6
    components = xa_ref.shape[0] // tiles
    even_x, even_y, _ = parities()
    for c in range(components):
        for t in range(tiles):
            spot = c * tiles + t
            sides = ordered(even_x, xa_ref[spot], xb_ref[spot])
            outb_ref[spot] = yb_ref[spot]
            for k in range(2):
                at = 6 * t + 2 * c + k
                at = slice(at, at + 1)
                first, last = sides[k][0:1], sides[k][7:8]
                outa_ref[at] = ea_ref[at] + jnp.where(even_y, last, first)
                x = slice(7 * k, 7 * k + 1)
                outb_ref[spot, x] = yb_ref[spot, x] + jnp.where(even_y, first, last)


def base_kernel(
    local_ref, za_ref, zb_ref, xa_ref, xb_ref, out_hbm, first_ref, last_ref, out_ref, tile_ref, sems
):
    tiles = local_ref.shape[0] // COMPONENTS
    even_x, _, even_z = parities()
    low, high = ordered(even_z, za_ref[...], zb_ref[...])
    copies = []
    for c in range(COMPONENTS):
        for t in range(tiles):
            where = slice(t * LANES, t * LANES + LANES)
            spot = c * tiles + t
            planes = ordered(even_x, xa_ref[spot], xb_ref[spot])
            for x in range(8):
                value = local_ref[spot, 8 * x : 8 * x + 8]
                if t == 0:
                    value = value + at_lane(low, 8 * c + x, 0)
                if t == tiles - 1:
                    value = value + at_lane(high, 8 * c + x, LANES - 1)
                if x in (0, 7):
                    value = value + planes[x // 7]
                out_ref[c, x, :, where] = value
                tile_ref[spot, 8 * x : 8 * x + 8] = value
            first_ref[spot] = tile_ref[spot, pl.ds(0, 8, stride=8)]
            last_ref[spot] = tile_ref[spot, pl.ds(7, 8, stride=8)]
        copies.append(pltpu.make_async_copy(out_ref.at[c], out_hbm.at[c], sems.at[c]))
        copies[-1].start()
    for copy in copies:
        copy.wait()


def late_kernel(
    base_hbm, first_ref, last_ref, ia_ref, ea_ref, yb_ref, out_hbm, rows_ref, sems
):
    del base_hbm
    tiles = first_ref.shape[0] // COMPONENTS
    _, even_y, _ = parities()
    copies = []
    for c in range(COMPONENTS):
        for t in range(tiles):
            where = slice(t * LANES, t * LANES + LANES)
            spot = c * tiles + t
            outer = ea_ref[6 * t + 2 * c : 6 * t + 2 * c + 2]
            inner = ia_ref[18 * t + 6 * c : 18 * t + 6 * c + 6]
            side = jnp.concatenate([outer[0:1], inner, outer[1:2]], 0)
            front, behind = ordered(even_y, side, yb_ref[spot])
            rows_ref[c, 0, :, where] = first_ref[spot] + front
            rows_ref[c, 1, :, where] = last_ref[spot] + behind
        for k in range(2):
            copies.append(
                pltpu.make_async_copy(
                    rows_ref.at[c, k], out_hbm.at[c, :, 7 * k, :], sems.at[2 * c + k]
                )
            )
            copies[-1].start()
    for copy in copies:
        copy.wait()


def pairs_from(start, count):
    found = []
    for i in range(start, count - 1, 2):
        found += [(i, i + 1), (i + 1, i)]
    return found


def exchange(array, axis, start):
    return lax.ppermute(array, axis, pairs_from(start, lax.axis_size(axis)))


def mixed_exchange(array, axis, side):
    depth = lax.axis_size("gz")
    found = []
    for z in range(depth):
        for i, j in pairs_from((side + z) % 2, lax.axis_size(axis)):
            found.append((i * depth + z, j * depth + z))
    return lax.ppermute(array, (axis, "gz"), found)


def call(kernel, outs, scratch=(), flops=1000000, **specs):
    shapes = [out if hasattr(out, "dtype") else jax.ShapeDtypeStruct(out, F32) for out in outs]
    return pl.pallas_call(
        kernel,
        out_shape=shapes,
        scratch_shapes=list(scratch),
        compiler_params=pltpu.CompilerParams(vmem_limit_bytes=24 * 1024 * 1024),
        cost_estimate=pl.CostEstimate(flops=flops, bytes_accessed=1000000, transcendentals=0),
        **specs,
    )


def local(nodal, geometry):
    components, _, _, length = nodal.shape
    tiles = length // LANES
    blocks = length // BLOCK
    face = (components * tiles, 8, LANES)
    inner = (components * tiles * 6, LANES)
    edge = (components * tiles * 2, LANES)
    tile = (8, LANES)
    flat = (components * tiles, 64, LANES)
    constants = [jnp.asarray(table) for table in tables()]
    operands = [
        pltpu.with_memory_space_constraint(operand, pltpu.HBM)
        for operand in [nodal, geometry] + constants
    ]
    hbm = pl.BlockSpec(memory_space=pltpu.HBM)
    kept = [jax.ShapeDtypeStruct(constants[k].shape, constants[k].dtype) for k in (0, 1, 2, 3, 6)]
    loaded = call(
        load_kernel,
        [nodal.shape, (8 * blocks, BLOCK)] + kept + [tile, tile],
        [pltpu.VMEM(operands[k].shape, operands[k].dtype) for k in (1, 6, 7)]
        + [pltpu.SemaphoreType.DMA((10 + components,))],
        in_specs=[hbm] * len(operands),
    )(*operands)
    za = exchange(loaded[-2], "gz", 0)
    zb = exchange(loaded[-1], "gz", 1)
    (result,) = call(stiffness_kernel, [flat])(*loaded[:-2])
    xa, xb, ia, ea, yb = call(
        face_kernel,
        [face, face, inner, edge, face],
        [pltpu.VMEM((2 * components, 64, LANES), F32)],
    )(result, za, zb)
    xa = mixed_exchange(xa, "gx", 0)
    xb = mixed_exchange(xb, "gx", 1)
    ia = mixed_exchange(ia, "gy", 0)
    (ea,) = call(copy_kernel, [edge])(ea)
    ea, yb = call(edge_kernel, [edge, face])(ea, yb, xa, xb)
    yb = mixed_exchange(yb, "gy", 1)
    ea = mixed_exchange(ea, "gy", 0)
    vmem = pl.BlockSpec(memory_space=pltpu.VMEM)
    result, first, last = call(
        base_kernel,
        [nodal.shape, face, face],
        [
            pltpu.VMEM(nodal.shape, F32),
            pltpu.VMEM(flat, F32),
            pltpu.SemaphoreType.DMA((components,)),
        ],
        out_specs=[hbm, vmem, vmem],
    )(result, za, zb, xa, xb)
    (result,) = call(
        late_kernel,
        [nodal.shape],
        [pltpu.VMEM((components, 2, 8, length), F32), pltpu.SemaphoreType.DMA((2 * components,))],
        in_specs=[hbm] + [vmem] * 5,
        out_specs=[hbm],
        input_output_aliases={0: 0},
    )(result, first, last, ia, ea, yb)
    return result


def solution(mesh):
    return jax.shard_map(
        local,
        mesh=mesh,
        in_specs=(P(None, "gx", "gy", "gz"), P(None, "gx", "gy", "gz")),
        out_specs=P(None, "gx", "gy", "gz"),
        check_vma=False,
    )
```
